8 devices in a mesh: dp: 2 (over z, y), sp: 4 (over x, core).
Axes of the slice: x: 2, y: 2, z: 1, core: 2. Of those that a mesh axis runs over, the one named last changes fastest.
Arguments:
- hidden: bfloat16 [24576, 896], P(('dp', 'sp')), parts along dimension 0
- tok_perm: int32 [24576], P(('dp', 'sp')), parts along dimension 0
- send_off: int32 [32], P(('dp', 'sp')), parts along dimension 0
- send_len: int32 [32], P(('dp', 'sp')), parts along dimension 0
- recv_off: int32 [32], P(('dp', 'sp')), parts along dimension 0
- recv_len: int32 [32], P(('dp', 'sp')), parts along dimension 0
- recv_doc: int32 [12288], P(('dp', 'sp')), parts along dimension 0
- recv_pos: int32 [12288], P(('dp', 'sp')), parts along dimension 0
- g_attn: bfloat16 [896], replicated
- w_q: bfloat16 [896, 14, 64], replicated
- w_k: bfloat16 [896, 2, 64], replicated
- w_v: bfloat16 [896, 2, 64], replicated
- w_o: bfloat16 [14, 64, 896], replicated
- g_mlp: bfloat16 [896], replicated
- w_gate: bfloat16 [896, 4864], replicated
- w_up: bfloat16 [896, 4864], replicated
- w_down: bfloat16 [4864, 896], replicated
Outputs:
- output: bfloat16 [24576, 896], P(('dp', 'sp')), parts along dimension 0
There are 2 independent parts. The reference program is written for one: setup_inputs(seed, part) draws one part's arguments, and reference() takes and returns one part's arrays. A program takes and returns all parts, laid end to end along the dimension named above; an argument that names none is the same for every part.
All inputs are finite; a program needn't handle non-finite values.
Results may differ from the reference program's by a relative error of at most 0.0108911.
Values are sent between devices in bfloat16 or wider.
A program may use at most 1 GiB of HBM per device.

```python
import jax
import jax.numpy as jnp
from jax import lax

GROUP_SIZE = 4
TOKENS_DEV = 3072
D = 896
HEADS = 14
KV_HEADS = 2
HEAD = 64
FF = 4864
PIECES = 4
Q_BLOCK = 128
ROPE_BASE = 500000
RECV_CAP = TOKENS_DEV // 2
Q_PER_KV = HEADS // KV_HEADS
NORM_EPS = 1e-5


def draw_plan(plan_key):
    key_src, key_shift, key_long = jax.random.split(plan_key, 3)
    src_of = jax.vmap(lambda sub_key: jax.random.permutation(sub_key, GROUP_SIZE))(jax.random.split(key_src, PIECES)).astype(jnp.int32)
    dev_ids = jnp.arange(GROUP_SIZE, dtype=jnp.int32)
    len_shift = jax.random.randint(key_shift, (GROUP_SIZE,), 0, 6, dtype=jnp.int32)
    long_dev = jax.random.randint(key_long, (), 0, GROUP_SIZE, dtype=jnp.int32)
    len_shift = jnp.where(dev_ids == long_dev, 0, len_shift).astype(jnp.int32)
    first_len = jnp.right_shift(jnp.full((GROUP_SIZE,), RECV_CAP, jnp.int32), len_shift)
    rest_len = RECV_CAP - first_len
    piece_len = jnp.stack([first_len, rest_len // 3, (rest_len + 1) // 3, (rest_len + 2) // 3]).astype(jnp.int32)
    held_dest = jnp.argsort(src_of, axis=1).astype(jnp.int32)
    held_len = jnp.take_along_axis(piece_len, held_dest, axis=1)
    held_end = jnp.cumsum(held_len, axis=0)
    tok_idx = jnp.arange(TOKENS_DEV, dtype=jnp.int32)
    piece_idx = jnp.sum((tok_idx[None, None, :] >= held_end[:, :, None]).astype(jnp.int32), axis=0)
    dest_pad = jnp.concatenate([held_dest, jnp.full((1, GROUP_SIZE), GROUP_SIZE, jnp.int32)], axis=0)
    tok_dest = jnp.take_along_axis(dest_pad.T, piece_idx, axis=1)
    tok_perm = jnp.argsort(tok_dest * TOKENS_DEV + tok_idx[None, :], axis=1)
    to_dest = (held_dest[:, :, None] == dev_ids[None, None, :]).astype(jnp.int32)
    send_len = jnp.sum(to_dest * held_len[:, :, None], axis=0)
    send_off = jnp.cumsum(send_len, axis=1) - send_len
    recv_len = send_len.T
    recv_off = jnp.cumsum(recv_len, axis=1) - recv_len
    order_key = src_of * PIECES + jnp.arange(PIECES, dtype=jnp.int32)[:, None]
    earlier = (order_key[None, :, :] < order_key[:, None, :]).astype(jnp.int32)
    dest_start = jnp.sum(earlier * piece_len[None, :, :], axis=1)
    slot_idx = jnp.arange(RECV_CAP, dtype=jnp.int32)
    in_piece = ((slot_idx[None, None, :] >= dest_start[:, :, None]) & (slot_idx[None, None, :] < (dest_start + piece_len)[:, :, None])).astype(jnp.int32)
    recv_doc = jnp.sum(in_piece * order_key[:, :, None], axis=0)
    recv_pos = jnp.sum(in_piece * (slot_idx[None, None, :] - dest_start[:, :, None]), axis=0)
    return {
        "tok_perm": tok_perm.reshape(-1).astype(jnp.int32),
        "send_off": send_off.reshape(-1).astype(jnp.int32),
        "send_len": send_len.reshape(-1).astype(jnp.int32),
        "recv_off": recv_off.reshape(-1).astype(jnp.int32),
        "recv_len": recv_len.reshape(-1).astype(jnp.int32),
        "recv_doc": recv_doc.reshape(-1).astype(jnp.int32),
        "recv_pos": recv_pos.reshape(-1).astype(jnp.int32),
    }


def setup_inputs(seed: int = 0, part: int = 0) -> dict:
    base_key = jax.random.key(seed)
    part_key = jax.random.fold_in(base_key, part)
    key_hidden, key_plan = jax.random.split(part_key)
    weight_keys = jax.random.split(base_key, 9)
    plan_ints = draw_plan(key_plan)
    qk_std = 1.7 * D ** -0.5

    def normal_w(index, shape, std):
        return (jax.random.normal(weight_keys[index], shape, jnp.float32) * std).astype(jnp.bfloat16)

    def draw_gain(index):
        return jax.random.uniform(weight_keys[index], (D,), jnp.float32, 0.5, 1.5).astype(jnp.bfloat16)

    return {
        "hidden": jax.random.normal(key_hidden, (GROUP_SIZE * TOKENS_DEV, D), jnp.float32).astype(jnp.bfloat16),
        "tok_perm": plan_ints["tok_perm"],
        "send_off": plan_ints["send_off"],
        "send_len": plan_ints["send_len"],
        "recv_off": plan_ints["recv_off"],
        "recv_len": plan_ints["recv_len"],
        "recv_doc": plan_ints["recv_doc"],
        "recv_pos": plan_ints["recv_pos"],
        "g_attn": draw_gain(0),
        "w_q": normal_w(1, (D, HEADS, HEAD), qk_std),
        "w_k": normal_w(2, (D, KV_HEADS, HEAD), qk_std),
        "w_v": normal_w(3, (D, KV_HEADS, HEAD), D ** -0.5),
        "w_o": normal_w(4, (HEADS, HEAD, D), (HEADS * HEAD) ** -0.5),
        "g_mlp": draw_gain(5),
        "w_gate": normal_w(6, (D, FF), D ** -0.5),
        "w_up": normal_w(7, (D, FF), D ** -0.5),
        "w_down": normal_w(8, (FF, D), FF ** -0.5),
    }


def rms_norm(rows_in, gain_vec):
    rows_f = rows_in.astype(jnp.float32)
    inv_rms = lax.rsqrt(jnp.mean(rows_f * rows_f, axis=-1, keepdims=True) + NORM_EPS)
    return (rows_f * inv_rms * gain_vec.astype(jnp.float32)).astype(jnp.bfloat16)


def rope(proj, positions):
    half_dim = HEAD // 2
    inv_freq = jnp.power(jnp.float32(ROPE_BASE), -2.0 * jnp.arange(half_dim, dtype=jnp.float32) / HEAD)
    angles = positions.astype(jnp.float32)[:, None, None] * inv_freq[None, None, :]
    cos_t = jnp.cos(angles)
    sin_t = jnp.sin(angles)
    lo_half = proj[..., :half_dim]
    hi_half = proj[..., half_dim:]
    return jnp.concatenate([lo_half * cos_t - hi_half * sin_t, hi_half * cos_t + lo_half * sin_t], axis=-1)


def attend(q_rot, k_rot, v_proj, doc_ids, positions):
    k_f = k_rot.astype(jnp.float32)
    v_f = v_proj.astype(jnp.float32)
    n_blocks = RECV_CAP // Q_BLOCK

    def one_block(blk_args):
        q_blk, doc_q, pos_q = blk_args
        scores = jnp.einsum("qkgd,skd->kgqs", q_blk.astype(jnp.float32), k_f) * (HEAD ** -0.5)
        allowed = (doc_q[:, None] == doc_ids[None, :]) & (positions[None, :] <= pos_q[:, None])
        probs_bf = jax.nn.softmax(jnp.where(allowed, scores, -1e30), axis=-1).astype(jnp.bfloat16)
        return jnp.einsum("kgqs,skd->qkgd", probs_bf.astype(jnp.float32), v_f).astype(jnp.bfloat16)

    blocks_out = lax.map(one_block, (q_rot.reshape(n_blocks, Q_BLOCK, KV_HEADS, Q_PER_KV, HEAD), doc_ids.reshape(n_blocks, Q_BLOCK), positions.reshape(n_blocks, Q_BLOCK)))
    return blocks_out.reshape(RECV_CAP, HEADS * HEAD)


def layer(dest_rows, doc_ids, positions, g_attn, w_q, w_k, w_v, w_o, g_mlp, w_gate, w_up, w_down):
    normed = rms_norm(dest_rows, g_attn)
    q_proj = jnp.dot(normed, w_q.reshape(D, HEADS * HEAD), preferred_element_type=jnp.float32).reshape(RECV_CAP, HEADS, HEAD)
    k_proj = jnp.dot(normed, w_k.reshape(D, KV_HEADS * HEAD), preferred_element_type=jnp.float32).reshape(RECV_CAP, KV_HEADS, HEAD)
    v_proj = jnp.dot(normed, w_v.reshape(D, KV_HEADS * HEAD), preferred_element_type=jnp.float32).astype(jnp.bfloat16).reshape(RECV_CAP, KV_HEADS, HEAD)
    q_rot = rope(q_proj, positions).astype(jnp.bfloat16).reshape(RECV_CAP, KV_HEADS, Q_PER_KV, HEAD)
    k_rot = rope(k_proj, positions).astype(jnp.bfloat16)
    attn_heads = attend(q_rot, k_rot, v_proj, doc_ids, positions)
    attn_out = jnp.dot(attn_heads, w_o.reshape(HEADS * HEAD, D), preferred_element_type=jnp.float32).astype(jnp.bfloat16)
    resid_mid = (dest_rows.astype(jnp.float32) + attn_out.astype(jnp.float32)).astype(jnp.bfloat16)
    normed_mlp = rms_norm(resid_mid, g_mlp)
    gate_proj = jnp.dot(normed_mlp, w_gate, preferred_element_type=jnp.float32)
    up_proj = jnp.dot(normed_mlp, w_up, preferred_element_type=jnp.float32)
    hidden_act = (jax.nn.silu(gate_proj) * up_proj).astype(jnp.bfloat16)
    down_proj = jnp.dot(hidden_act, w_down, preferred_element_type=jnp.float32).astype(jnp.bfloat16)
    return (resid_mid.astype(jnp.float32) + down_proj.astype(jnp.float32)).astype(jnp.bfloat16)


def reference(hidden, tok_perm, send_off, send_len, recv_off, recv_len, recv_doc, recv_pos, g_attn, w_q, w_k, w_v, w_o, g_mlp, w_gate, w_up, w_down):
    perm_rows = tok_perm.reshape(GROUP_SIZE, TOKENS_DEV)
    send_off_m = send_off.reshape(GROUP_SIZE, GROUP_SIZE)
    send_len_m = send_len.reshape(GROUP_SIZE, GROUP_SIZE)
    recv_off_m = recv_off.reshape(GROUP_SIZE, GROUP_SIZE)
    recv_len_m = recv_len.reshape(GROUP_SIZE, GROUP_SIZE)
    doc_rows = recv_doc.reshape(GROUP_SIZE, RECV_CAP)
    pos_rows = recv_pos.reshape(GROUP_SIZE, RECV_CAP)
    dev_ids = jnp.arange(GROUP_SIZE)
    slot_idx = jnp.arange(RECV_CAP)
    sorted_idx = jnp.arange(TOKENS_DEV)

    def one_dest(dest_dev):
        run_start = recv_off_m[dest_dev]
        in_run = (slot_idx[:, None] >= run_start[None, :]) & (slot_idx[:, None] < (run_start + recv_len_m[dest_dev])[None, :])
        src_dev = jnp.clip(jnp.sum(jnp.where(in_run, dev_ids[None, :], 0), axis=1), 0, GROUP_SIZE - 1)
        src_pos = jnp.sum(jnp.where(in_run, send_off_m[:, dest_dev][None, :] + slot_idx[:, None] - run_start[None, :], 0), axis=1)
        src_pos = jnp.clip(src_pos, 0, TOKENS_DEV - 1)
        filled = jnp.any(in_run, axis=1)
        src_row = src_dev * TOKENS_DEV + perm_rows[src_dev, src_pos]
        dest_rows = jnp.where(filled[:, None], hidden[src_row], jnp.zeros((), jnp.bfloat16))
        return layer(dest_rows, doc_rows[dest_dev], pos_rows[dest_dev], g_attn, w_q, w_k, w_v, w_o, g_mlp, w_gate, w_up, w_down)

    layer_rows = lax.map(one_dest, dev_ids).reshape(GROUP_SIZE * RECV_CAP, D)

    def one_source(src_dev):
        run_start = send_off_m[src_dev]
        in_run = (sorted_idx[:, None] >= run_start[None, :]) & (sorted_idx[:, None] < (run_start + send_len_m[src_dev])[None, :])
        dest_dev = jnp.clip(jnp.sum(jnp.where(in_run, dev_ids[None, :], 0), axis=1), 0, GROUP_SIZE - 1)
        dest_slot = jnp.sum(jnp.where(in_run, recv_off_m[:, src_dev][None, :] + sorted_idx[:, None] - run_start[None, :], 0), axis=1)
        dest_slot = jnp.clip(dest_slot, 0, RECV_CAP - 1)
        was_sent = jnp.any(in_run, axis=1)
        back_rows = jnp.where(was_sent[:, None], layer_rows[dest_dev * RECV_CAP + dest_slot], jnp.zeros((), jnp.bfloat16))
        inv_perm = jnp.argsort(perm_rows[src_dev])
        return back_rows[inv_perm]

    return lax.map(one_source, dev_ids).reshape(GROUP_SIZE * TOKENS_DEV, D)
```

```python
import functools

import jax
import jax.numpy as jnp
from jax import lax
from jax.experimental import pallas as pl
from jax.experimental.pallas import tpu as pltpu
from jax.sharding import PartitionSpec as P

ROPE_BASE = 500000.0
NORM_EPS = 1e-5
ROWS = 512
QB = 256
FT = 256


def norm_rows(rows_f, gain):
    inv = lax.rsqrt(jnp.mean(rows_f * rows_f, axis=-1, keepdims=True) + NORM_EPS)
    return (rows_f * inv * gain).astype(jnp.bfloat16)


def rope_pair(x, cos_t, sin_t, first_half):
    swapped = jnp.where(first_half, pltpu.roll(x, 96, 1), pltpu.roll(x, 32, 1))
    return x * cos_t + swapped * sin_t


def dot_t(a, b):
    return lax.dot_general(a, b, (((1,), (1,)), ((), ())), preferred_element_type=jnp.float32)


def dot_n(a, b):
    return jnp.dot(a, b, preferred_element_type=jnp.float32)


def layer_kernel(maxs_ref, r_ref, start_ref, cos_ref, sin_ref, ga_ref, gm_ref, wq_h, wk_h, wv_h, wo_h, wg_h, wu_h, wd_h, out_ref,
                 q_s, k_s, v_s, o_s, h_s, m_s, wq_s, wk_s, wv_s, wo_s, wg_s, wu_s, wd_s, sems):
    n_rows, dim = r_ref.shape
    n_pairs = dim // 128
    ff = wg_s.shape[1]
    loads = [pltpu.make_async_copy(a, b, sems.at[i]) for i, (a, b) in enumerate(
        [(wq_h, wq_s), (wk_h, wk_s), (wv_h, wv_s), (wo_h, wo_s), (wg_h, wg_s), (wu_h, wu_s), (wd_h, wd_s)])]
    for c in loads:
        c.start()
    for c in loads[:3]:
        c.wait()
    gain_a = ga_ref[...].astype(jnp.float32)
    gain_m = gm_ref[...].astype(jnp.float32)

    @pl.loop(0, n_rows // QB)
    def _qkv(b):
        rows = pl.ds(pl.multiple_of(b * QB, QB), QB)
        lane = lax.broadcasted_iota(jnp.int32, (QB, 128), 1)
        first_half = lane % 64 < 32
        low = lane < 64
        h = norm_rows(r_ref[rows, :].astype(jnp.float32), gain_a)
        cos_t = cos_ref[rows, :]
        sin_t = sin_ref[rows, :]
        q = dot_t(h, wq_s[...])
        for p in range(n_pairs):
            qp = rope_pair(q[:, 128 * p:128 * (p + 1)], cos_t, sin_t, first_half)
            q_s[p, rows, :] = (qp.astype(jnp.bfloat16) * 0.125).astype(jnp.bfloat16)
        k = rope_pair(dot_t(h, wk_s[...]), cos_t, sin_t, first_half)
        v = dot_t(h, wv_s[...])
        for s, x in ((k_s, k), (v_s, v)):
            other = pltpu.roll(x, 64, 1)
            s[0, rows, :] = jnp.where(low, x, other).astype(jnp.bfloat16)
            s[1, rows, :] = jnp.where(low, other, x).astype(jnp.bfloat16)

    for c in range(n_rows // QB):
        length = (c + 1) * QB
        row = c * QB + lax.broadcasted_iota(jnp.int32, (QB, QB), 0)
        col = c * QB + lax.broadcasted_iota(jnp.int32, (QB, QB), 1)
        start = start_ref[c * QB:(c + 1) * QB, :]
        low_q = lax.broadcasted_iota(jnp.int32, (QB, 128), 1) < 64

        def heads(p, masked):
            outs = []
            qp = q_s[p, c * QB:(c + 1) * QB, :]
            for half in range(2):
                g = (2 * p + half) // 7
                qh = jnp.where(low_q if half == 0 else ~low_q, qp, jnp.zeros_like(qp))
                s = dot_t(qh, k_s[g, :length, :])
                diag = jnp.where((col >= start) & (col <= row), s[:, c * QB:], -1e30)
                if c == 0:
                    s = diag
                else:
                    body = s[:, :c * QB]
                    if masked:
                        body_col = lax.broadcasted_iota(jnp.int32, (QB, c * QB), 1)
                        body = jnp.where(body_col >= start, body, -1e30)
                    s = jnp.concatenate([body, diag], axis=1)
                top = jnp.max(s, axis=1, keepdims=True)
                e = jnp.exp(s - top)
                total = jnp.sum(e, axis=1, keepdims=True)
                outs.append(dot_n(e.astype(jnp.bfloat16), v_s[g, :length, :]) / total)
            o_s[c * QB:(c + 1) * QB, pl.ds(pl.multiple_of(p * 128, 128), 128)] = jnp.where(low_q, outs[0], outs[1]).astype(jnp.bfloat16)

        if c == 0:
            @pl.loop(0, n_pairs)
            def _pair(p):
                heads(p, False)
        else:
            has_start = maxs_ref[c] > 0

            @pl.when(has_start)
            def _masked():
                @pl.loop(0, n_pairs)
                def _pair(p):
                    heads(p, True)

            @pl.when(jnp.logical_not(has_start))
            def _plain():
                @pl.loop(0, n_pairs)
                def _pair(p):
                    heads(p, False)

    for c in loads[3:]:
        c.wait()

    @pl.loop(0, n_rows // ROWS)
    def _mlp(b):
        rows = pl.ds(pl.multiple_of(b * ROWS, ROWS), ROWS)
        attn = dot_n(o_s[rows, :], wo_s[...]).astype(jnp.bfloat16)
        z = (r_ref[rows, :].astype(jnp.float32) + attn.astype(jnp.float32)).astype(jnp.bfloat16)
        out_ref[rows, :] = z
        h_s[...] = norm_rows(z.astype(jnp.float32), gain_m)
        for t in range(ff // FT):
            cols = slice(t * FT, (t + 1) * FT)
            gate = dot_n(h_s[...], wg_s[:, cols])
            up = dot_n(h_s[...], wu_s[:, cols])
            m_s[:, cols] = (gate / (1.0 + jnp.exp(-gate)) * up).astype(jnp.bfloat16)
        down = dot_n(m_s[...], wd_s[...]).astype(jnp.bfloat16)
        out_ref[rows, :] = (out_ref[rows, :].astype(jnp.float32) + down.astype(jnp.float32)).astype(jnp.bfloat16)


def layer(dest_rows, positions, g_attn, w_q, w_k, w_v, w_o, g_mlp, w_gate, w_up, w_down):
    n_rows, dim = dest_rows.shape
    head_dim = w_q.shape[2]
    half_dim = head_dim // 2
    ff = w_gate.shape[1]
    inv_freq = jnp.power(jnp.float32(ROPE_BASE), -2.0 * jnp.arange(half_dim, dtype=jnp.float32) / head_dim)
    angles = positions.astype(jnp.float32)[:, None] * inv_freq[None, :]
    cos_t = jnp.cos(angles)
    sin_t = jnp.sin(angles)
    cos_t = jnp.concatenate([cos_t, cos_t, cos_t, cos_t], axis=1)
    sin_t = jnp.concatenate([-sin_t, sin_t, -sin_t, sin_t], axis=1)
    start = jnp.arange(n_rows, dtype=jnp.int32) - positions
    max_start = jnp.max(start.reshape(n_rows // QB, QB), axis=1)
    wq_t = jnp.transpose(w_q, (1, 2, 0)).reshape(dim, dim)
    wk_t = jnp.transpose(w_k, (1, 2, 0)).reshape(128, dim)
    wv_t = jnp.transpose(w_v, (1, 2, 0)).reshape(128, dim)
    wo_t = w_o.reshape(dim, dim)
    vm = pl.BlockSpec(memory_space=pltpu.VMEM)
    hb = pl.BlockSpec(memory_space=pl.ANY)
    bf = jnp.bfloat16
    return pl.pallas_call(
        layer_kernel,
        out_shape=jax.ShapeDtypeStruct((n_rows, dim), bf),
        in_specs=[pl.BlockSpec(memory_space=pltpu.SMEM)] + [vm] * 6 + [hb] * 7,
        out_specs=vm,
        scratch_shapes=[
            pltpu.VMEM((dim // 128, n_rows, 128), bf), pltpu.VMEM((2, n_rows, 128), bf), pltpu.VMEM((2, n_rows, 128), bf),
            pltpu.VMEM((n_rows, dim), bf), pltpu.VMEM((ROWS, dim), bf), pltpu.VMEM((ROWS, ff), bf),
            pltpu.VMEM((dim, dim), bf), pltpu.VMEM((128, dim), bf), pltpu.VMEM((128, dim), bf), pltpu.VMEM((dim, dim), bf),
            pltpu.VMEM((dim, ff), bf), pltpu.VMEM((dim, ff), bf), pltpu.VMEM((ff, dim), bf),
            pltpu.SemaphoreType.DMA((7,))],
        compiler_params=pltpu.CompilerParams(vmem_limit_bytes=66000000),
        cost_estimate=pl.CostEstimate(flops=60_000_000_000, bytes_accessed=40_000_000, transcendentals=0),
        name="layer",
    )(max_start, dest_rows, start[:, None], cos_t, sin_t, g_attn[None, :], g_mlp[None, :], wq_t, wk_t, wv_t, wo_t, w_gate, w_up, w_down)


def solution(mesh):
    row_spec = P(('dp', 'sp'), None)
    vec_spec = P(('dp', 'sp'))
    rep_spec = P()

    def per_device(hidden, tok_perm, send_off, send_len, recv_off, recv_len, recv_doc, recv_pos, g_attn, w_q, w_k, w_v, w_o, g_mlp, w_gate, w_up, w_down):
        n_tok, model_dim = hidden.shape
        n_cap = recv_doc.shape[0]
        group_devs = send_off.shape[0]
        zero_val = jnp.zeros((), hidden.dtype)
        pair_row = jnp.arange(n_cap)[None, :]
        dev_base = jnp.arange(group_devs)[None, :] * n_cap
        send_idx = jnp.minimum(send_off[:, None] + pair_row, n_tok - 1).reshape(-1)
        send_buf = jnp.take(hidden, jnp.take(tok_perm, send_idx), axis=0).reshape(group_devs, n_cap, model_dim)
        recv_buf = lax.all_to_all(send_buf, 'sp', 0, 0, tiled=True).reshape(group_devs * n_cap, model_dim)
        slot_idx = jnp.arange(n_cap)[:, None]
        in_run = (slot_idx >= recv_off[None, :]) & (slot_idx < (recv_off + recv_len)[None, :])
        flat_pos = jnp.sum(jnp.where(in_run, dev_base + slot_idx - recv_off[None, :], 0), axis=1)
        dest_rows = jnp.take(recv_buf, flat_pos, axis=0)
        layer_rows = layer(dest_rows, recv_pos, g_attn, w_q, w_k, w_v, w_o, g_mlp, w_gate, w_up, w_down)
        back_idx = jnp.minimum(recv_off[:, None] + pair_row, n_cap - 1).reshape(-1)
        back_buf = jnp.take(layer_rows, back_idx, axis=0).reshape(group_devs, n_cap, model_dim)
        back_recv = lax.all_to_all(back_buf, 'sp', 0, 0, tiled=True).reshape(group_devs * n_cap, model_dim)
        inv_perm = jnp.argsort(tok_perm)[:, None]
        in_back = (inv_perm >= send_off[None, :]) & (inv_perm < (send_off + send_len)[None, :])
        back_pos = jnp.sum(jnp.where(in_back, dev_base + inv_perm - send_off[None, :], 0), axis=1)
        was_sent = jnp.any(in_back, axis=1)
        return jnp.where(was_sent[:, None], jnp.take(back_recv, back_pos, axis=0), zero_val)

    return jax.shard_map(per_device, mesh=mesh, in_specs=(row_spec,) + (vec_spec,) * 7 + (rep_spec,) * 9, out_specs=row_spec, check_vma=False)
```

```python
import functools

import jax
import jax.numpy as jnp
from jax import lax
from jax.experimental import pallas as pl
from jax.experimental.pallas import tpu as pltpu
from jax.sharding import PartitionSpec as P

ROPE_BASE = 500000.0
NORM_EPS = 1e-5
ROWS = 512
QB = 256
FT = 256


def norm_rows(rows_f, gain):
    inv = lax.rsqrt(jnp.mean(rows_f * rows_f, axis=-1, keepdims=True) + NORM_EPS)
    return (rows_f * inv * gain).astype(jnp.bfloat16)


def rope_pair(x, cos_t, sin_t, first_half):
    swapped = jnp.where(first_half, pltpu.roll(x, 96, 1), pltpu.roll(x, 32, 1))
    return x * cos_t + swapped * sin_t


def dot_t(a, b):
    return lax.dot_general(a, b, (((1,), (1,)), ((), ())), preferred_element_type=jnp.float32)


def dot_n(a, b):
    return jnp.dot(a, b, preferred_element_type=jnp.float32)


def layer_kernel(maxs_ref, r_ref, start_ref, cos_ref, sin_ref, ga_ref, gm_ref, wq_h, wk_h, wv_h, wo_h, wg_h, wu_h, wd_h, out_ref,
                 q_s, k_s, v_s, o_s, h_s, m_s, wq_s, wk_s, wv_s, wo_s, wg_s, wu_s, wd_s, sems):
    n_rows, dim = r_ref.shape
    n_pairs = dim // 128
    ff = wg_s.shape[1]
    loads = [pltpu.make_async_copy(a, b, sems.at[i]) for i, (a, b) in enumerate(
        [(wq_h, wq_s), (wk_h, wk_s), (wv_h, wv_s), (wo_h, wo_s), (wg_h, wg_s), (wu_h, wu_s), (wd_h, wd_s)])]
    for c in loads:
        c.start()
    for c in loads[:3]:
        c.wait()
    gain_a = ga_ref[...].astype(jnp.float32)
    gain_m = gm_ref[...].astype(jnp.float32)

    @pl.loop(0, n_rows // QB)
    def _qkv(b):
        rows = pl.ds(pl.multiple_of(b * QB, QB), QB)
        lane = lax.broadcasted_iota(jnp.int32, (QB, 128), 1)
        first_half = lane % 64 < 32
        low = lane < 64
        h = norm_rows(r_ref[rows, :].astype(jnp.float32), gain_a)
        cos_t = cos_ref[rows, :]
        sin_t = sin_ref[rows, :]
        q = dot_t(h, wq_s[...])
        for p in range(n_pairs):
            qp = rope_pair(q[:, 128 * p:128 * (p + 1)], cos_t, sin_t, first_half)
            q_s[p, rows, :] = (qp.astype(jnp.bfloat16) * 0.125).astype(jnp.bfloat16)
        k = rope_pair(dot_t(h, wk_s[...]), cos_t, sin_t, first_half)
        v = dot_t(h, wv_s[...])
        for s, x in ((k_s, k), (v_s, v)):
            other = pltpu.roll(x, 64, 1)
            s[0, rows, :] = jnp.where(low, x, other).astype(jnp.bfloat16)
            s[1, rows, :] = jnp.where(low, other, x).astype(jnp.bfloat16)

    for c in range(n_rows // QB):
        length = (c + 1) * QB
        row = c * QB + lax.broadcasted_iota(jnp.int32, (QB, QB), 0)
        col = c * QB + lax.broadcasted_iota(jnp.int32, (QB, QB), 1)
        start = start_ref[c * QB:(c + 1) * QB, :]
        low_q = lax.broadcasted_iota(jnp.int32, (QB, 128), 1) < 64

        def heads(p, masked):
            outs = []
            qp = q_s[p, c * QB:(c + 1) * QB, :]
            for half in range(2):
                g = (2 * p + half) // 7
                qh = jnp.where(low_q if half == 0 else ~low_q, qp, jnp.zeros_like(qp))
                s = dot_t(qh, k_s[g, :length, :])
                diag = jnp.where((col >= start) & (col <= row), s[:, c * QB:], -1e30)
                if c == 0:
                    s = diag
                else:
                    body = s[:, :c * QB]
                    if masked:
                        body_col = lax.broadcasted_iota(jnp.int32, (QB, c * QB), 1)
                        body = jnp.where(body_col >= start, body, -1e30)
                    s = jnp.concatenate([body, diag], axis=1)
                top = jnp.max(s, axis=1, keepdims=True)
                e = jnp.exp(s - top)
                total = jnp.sum(e, axis=1, keepdims=True)
                outs.append(dot_n(e.astype(jnp.bfloat16), v_s[g, :length, :]) / total)
            o_s[c * QB:(c + 1) * QB, pl.ds(pl.multiple_of(p * 128, 128), 128)] = jnp.where(low_q, outs[0], outs[1]).astype(jnp.bfloat16)

        if c == 0:
            @pl.loop(0, n_pairs)
            def _pair(p):
                heads(p, False)
        else:
            has_start = maxs_ref[c] > 0

            @pl.when(has_start)
            def _masked():
                @pl.loop(0, n_pairs)
                def _pair(p):
                    heads(p, True)

            @pl.when(jnp.logical_not(has_start))
            def _plain():
                @pl.loop(0, n_pairs)
                def _pair(p):
                    heads(p, False)

    for c in loads[3:]:
        c.wait()

    @pl.loop(0, n_rows // ROWS)
    def _mlp(b):
        rows = pl.ds(pl.multiple_of(b * ROWS, ROWS), ROWS)
        attn = dot_n(o_s[rows, :], wo_s[...]).astype(jnp.bfloat16)
        z = (r_ref[rows, :].astype(jnp.float32) + attn.astype(jnp.float32)).astype(jnp.bfloat16)
        out_ref[rows, :] = z
        h_s[...] = norm_rows(z.astype(jnp.float32), gain_m)
        for t in range(ff // FT):
            cols = slice(t * FT, (t + 1) * FT)
            gate = dot_n(h_s[...], wg_s[:, cols])
            up = dot_n(h_s[...], wu_s[:, cols])
            m_s[:, cols] = (gate / (1.0 + jnp.exp(-gate)) * up).astype(jnp.bfloat16)
        down = dot_n(m_s[...], wd_s[...]).astype(jnp.bfloat16)
        out_ref[rows, :] = (out_ref[rows, :].astype(jnp.float32) + down.astype(jnp.float32)).astype(jnp.bfloat16)


def layer(dest_rows, positions, g_attn, w_q, w_k, w_v, w_o, g_mlp, w_gate, w_up, w_down):
    n_rows, dim = dest_rows.shape
    head_dim = w_q.shape[2]
    half_dim = head_dim // 2
    ff = w_gate.shape[1]
    inv_freq = jnp.power(jnp.float32(ROPE_BASE), -2.0 * jnp.arange(half_dim, dtype=jnp.float32) / head_dim)
    angles = positions.astype(jnp.float32)[:, None] * inv_freq[None, :]
    cos_t = jnp.cos(angles)
    sin_t = jnp.sin(angles)
    cos_t = jnp.concatenate([cos_t, cos_t, cos_t, cos_t], axis=1)
    sin_t = jnp.concatenate([-sin_t, sin_t, -sin_t, sin_t], axis=1)
    start = jnp.arange(n_rows, dtype=jnp.int32) - positions
    max_start = jnp.max(start.reshape(n_rows // QB, QB), axis=1)
    wq_t = jnp.transpose(w_q, (1, 2, 0)).reshape(dim, dim)
    wk_t = jnp.transpose(w_k, (1, 2, 0)).reshape(128, dim)
    wv_t = jnp.transpose(w_v, (1, 2, 0)).reshape(128, dim)
    wo_t = w_o.reshape(dim, dim)
    vm = pl.BlockSpec(memory_space=pltpu.VMEM)
    hb = pl.BlockSpec(memory_space=pl.ANY)
    bf = jnp.bfloat16
    return pl.pallas_call(
        layer_kernel,
        out_shape=jax.ShapeDtypeStruct((n_rows, dim), bf),
        in_specs=[pl.BlockSpec(memory_space=pltpu.SMEM)] + [vm] * 6 + [hb] * 7,
        out_specs=vm,
        scratch_shapes=[
            pltpu.VMEM((dim // 128, n_rows, 128), bf), pltpu.VMEM((2, n_rows, 128), bf), pltpu.VMEM((2, n_rows, 128), bf),
            pltpu.VMEM((n_rows, dim), bf), pltpu.VMEM((ROWS, dim), bf), pltpu.VMEM((ROWS, ff), bf),
            pltpu.VMEM((dim, dim), bf), pltpu.VMEM((128, dim), bf), pltpu.VMEM((128, dim), bf), pltpu.VMEM((dim, dim), bf),
            pltpu.VMEM((dim, ff), bf), pltpu.VMEM((dim, ff), bf), pltpu.VMEM((ff, dim), bf),
            pltpu.SemaphoreType.DMA((7,))],
        compiler_params=pltpu.CompilerParams(vmem_limit_bytes=66000000),
        cost_estimate=pl.CostEstimate(flops=60_000_000_000, bytes_accessed=40_000_000, transcendentals=0),
        name="layer",
    )(max_start, dest_rows, start[:, None], cos_t, sin_t, g_attn[None, :], g_mlp[None, :], wq_t, wk_t, wv_t, wo_t, w_gate, w_up, w_down)


CHUNK = 128
MESH_ID = pl.DeviceIdType.MESH
ANY = pl.BlockSpec(memory_space=pl.ANY)
VM = pl.BlockSpec(memory_space=pltpu.VMEM)
SM = pl.BlockSpec(memory_space=pltpu.SMEM)


def meet(devices):
    barrier = pltpu.get_barrier_semaphore()
    for dev in devices:
        pl.semaphore_signal(barrier, inc=1, device_id={"sp": dev}, device_id_type=MESH_ID)
    pl.semaphore_wait(barrier, len(devices))


def push(src, dst, send_sem, recv_sem, dev):
    return pltpu.make_async_remote_copy(src_ref=src, dst_ref=dst, send_sem=send_sem, recv_sem=recv_sem,
                                        device_id={"sp": dev}, device_id_type=MESH_ID)


def share_kernel(n_split, *refs):
    n = (len(refs) - 2) // 2
    ins, outs, send_sems, recv_sems = refs[:n], refs[n:2 * n], refs[-2], refs[-1]
    me = lax.axis_index("sp")
    sib = me + 1 - 2 * lax.rem(me, 2)
    meet([sib])
    copies = []
    for a, b in zip(ins, outs):
        parts = n_split if a.shape[0] % (16 * n_split) == 0 else 1
        step = a.shape[0] // parts
        for p in range(parts):
            rows = pl.ds(p * step, step)
            copies.append((a.at[rows], b.at[rows]))
    started = []
    for i, (a, b) in enumerate(copies):
        cp = push(a, b, send_sems.at[i], recv_sems.at[i], sib)
        cp.start()
        started.append(cp)
    for cp in started:
        cp.wait()


def share(arrays, collective_id):
    return pl.pallas_call(
        functools.partial(share_kernel, 4),
        out_shape=[jax.ShapeDtypeStruct(a.shape, a.dtype) for a in arrays],
        in_specs=[ANY] * len(arrays), out_specs=[ANY] * len(arrays),
        scratch_shapes=[pltpu.SemaphoreType.DMA((8,)), pltpu.SemaphoreType.DMA((8,))],
        compiler_params=pltpu.CompilerParams(collective_id=collective_id, has_side_effects=True),
        name="share",
    )(*arrays)


def cross_kernel(count, half, src, dst, s1, r1, s2, r2):
    me = lax.axis_index("sp")
    core = lax.rem(me, 2)
    sib = me + 1 - 2 * core
    peer = lax.rem(me + 2, 4)
    meet([sib, peer])
    outs = []
    for q in range(count):
        rows = pl.ds(q * CHUNK, CHUNK)
        cp = push(src.at[rows], dst.at[rows], s1.at[q], r1.at[q], peer)
        cp.start()
        outs.append(cp)
    fwd = []
    for q in range(count):
        outs[q].wait_recv()
        cp = push(dst.at[pl.ds(q * CHUNK, CHUNK)], dst.at[pl.ds(half + q * CHUNK, CHUNK)], s2.at[q], r2.at[q], sib)
        cp.start()
        fwd.append(cp)
    for q in range(count):
        outs[q].wait_send()
        fwd[q].wait()


def cross(stream, count, collective_id):
    half, dim = stream.shape
    return pl.pallas_call(
        functools.partial(cross_kernel, count, half),
        out_shape=jax.ShapeDtypeStruct((2 * half, dim), stream.dtype),
        in_specs=[ANY], out_specs=ANY,
        scratch_shapes=[pltpu.SemaphoreType.DMA((count,))] * 4,
        compiler_params=pltpu.CompilerParams(collective_id=collective_id, has_side_effects=True),
        name="cross",
    )(stream)


def exchange(stream, units, collective_id):
    top = stream.shape[0] // CHUNK
    return lax.switch(units - 1, [functools.partial(cross, count=k + 1, collective_id=collective_id) for k in range(top)], stream)


LOAD = 256


def load_table(parts, tab, stage, sems):
    base = 0
    for ref, rows, blocks in parts:
        n_blk = rows // LOAD if blocks is None else blocks

        def fetch(i, slot, ref=ref):
            return pltpu.make_async_copy(ref.at[pl.ds(pl.multiple_of(i * LOAD, LOAD), LOAD)], stage.at[slot], sems.at[slot])

        @pl.when(n_blk > 0)
        def _first():
            fetch(0, 0).start()

        @pl.loop(0, n_blk)
        def _blk(i, base=base):
            slot = lax.rem(i, 2)

            @pl.when(i + 1 < n_blk)
            def _next():
                fetch(i + 1, 1 - slot).start()

            fetch(i, slot).wait()
            tab[pl.ds(pl.multiple_of(base + i * LOAD, LOAD), LOAD), 0, :] = stage[slot].astype(jnp.float32)

        base += rows


UNROLL = 16


def copy_rows(n_rows, move):
    @pl.loop(0, n_rows // UNROLL)
    def _grp(i):
        for k in range(UNROLL):
            move(i * UNROLL + k)


def rows_out(n_rows, src3, dst):
    @pl.loop(0, n_rows // CHUNK)
    def _blk(i):
        rows = pl.ds(pl.multiple_of(i * CHUNK, CHUNK), CHUNK)
        dst[rows, :] = src3[rows, 0, :].astype(dst.dtype)


def pick_kernel(cnt, perm, upos, rpos, own, sib, stream, rloc, tab, out3, stage, sems):
    n_tok = own.shape[0]
    cap = rloc.shape[0]
    load_table([(own, n_tok, None), (sib, n_tok, None)], tab, stage, sems)

    def one_u(k):
        out3[k] = tab[perm[upos[k]]]

    copy_rows(cnt[0] * CHUNK, one_u)
    rows_out(cnt[0] * CHUNK, out3, stream)

    def one_r(k):
        out3[k] = tab[perm[rpos[k]]]

    copy_rows(cap, one_r)
    rows_out(cap, out3, rloc)


def place_kernel(cnt, spos, rloc, stream, out, tab, out3, stage, sems):
    cap = out.shape[0]
    blocks = (cnt[0] * CHUNK + LOAD - 1) // LOAD
    load_table([(stream.at[pl.ds(0, cap)], cap, blocks), (stream.at[pl.ds(cap, cap)], cap, blocks)], tab, stage, sems)
    first, last = cnt[1], cnt[1] + cnt[2]

    def one(k):
        out3[k] = tab[spos[k]]

    lo = first // UNROLL * UNROLL

    @pl.loop(lo // UNROLL, (last + UNROLL - 1) // UNROLL)
    def _grp(i):
        for k in range(UNROLL):
            one(i * UNROLL + k)

    @pl.loop(0, cap // CHUNK)
    def _blk(i):
        rows = pl.ds(pl.multiple_of(i * CHUNK, CHUNK), CHUNK)
        row = i * CHUNK + lax.broadcasted_iota(jnp.int32, (CHUNK, out.shape[1]), 0)
        keep = (row >= first) & (row < last)
        out[rows, :] = jnp.where(keep, out3[rows, 0, :], rloc[rows, :].astype(jnp.float32)).astype(out.dtype)


def back_pick_kernel(cnt, ypos, own, sib, stream, tab, out3, stage, sems):
    cap = own.shape[0]
    load_table([(own, cap, None), (sib, cap, None)], tab, stage, sems)

    def one(k):
        out3[k] = tab[ypos[k]]

    copy_rows(cnt[0] * CHUNK, one)
    rows_out(cnt[0] * CHUNK, out3, stream)


def back_place_kernel(cnt, perm, ridx, own, sib, stream, out, tab, out3, stage, sems):
    cap = own.shape[0]
    n_tok = out.shape[0]
    blocks = (cnt[0] * CHUNK + LOAD - 1) // LOAD
    load_table([(own, cap, None), (sib, cap, None), (stream.at[pl.ds(0, cap)], cap, blocks), (stream.at[pl.ds(cap, cap)], cap, blocks)], tab, stage, sems)
    tab[4 * cap] = jnp.zeros((1, out.shape[1]), jnp.float32)

    def one(k):
        out3[perm[k]] = tab[ridx[k]]

    copy_rows(n_tok, one)
    rows_out(n_tok, out3, out)


def local_call(body, out_shapes, n_smem, n_vmem, n_any, tab_rows, out_rows, dim, name):
    return pl.pallas_call(
        body,
        out_shape=out_shapes,
        in_specs=[SM] * n_smem + [VM] * n_vmem + [ANY] * n_any,
        out_specs=jax.tree.map(lambda _: VM, out_shapes),
        scratch_shapes=[pltpu.VMEM((tab_rows + 8, 1, dim), jnp.float32), pltpu.VMEM((out_rows + 8, 1, dim), jnp.float32),
                        pltpu.VMEM((2, LOAD, dim), jnp.bfloat16), pltpu.SemaphoreType.DMA((2,))],
        compiler_params=pltpu.CompilerParams(vmem_limit_bytes=66000000),
        name=name,
    )


def solution(mesh):
    row_spec = P(('dp', 'sp'), None)
    vec_spec = P(('dp', 'sp'))
    rep_spec = P()

    def per_device(hidden, tok_perm, send_off, send_len, recv_off, recv_len, recv_doc, recv_pos, g_attn, w_q, w_k, w_v, w_o, g_mlp, w_gate, w_up, w_down):
        n_tok, dim = hidden.shape
        cap = recv_doc.shape[0]
        i32 = jnp.int32
        me = lax.axis_index('sp')
        core = me % 2
        chip = me // 2
        plan = jnp.concatenate([tok_perm, send_off, send_len, recv_off, recv_len, jnp.zeros((1024 - 16,), i32)]).reshape(-1, 128)
        sib_hidden, sib_plan = share([hidden, plan], 0)
        sib_plan = sib_plan.reshape(-1)
        sib_perm = sib_plan[:n_tok]

        def both(own, at):
            other = lax.slice(sib_plan, (n_tok + at,), (n_tok + at + 4,))
            return jnp.where(core == 0, jnp.stack([own, other]), jnp.stack([other, own]))

        so, sl, ro, rl = both(send_off, 0), both(send_len, 4), both(recv_off, 8), both(recv_len, 12)
        far = 2 * (1 - chip)
        cores = jnp.arange(2, dtype=i32)
        fo = jnp.where(cores == core, 0, n_tok)
        half_of = jnp.where(cores == core, 0, cap)
        far_len = lax.dynamic_slice(sl, (0, far), (2, 2))
        far_off = lax.dynamic_slice(so, (0, far), (2, 2))
        seg_len = far_len.T.reshape(4)
        seg_base = jnp.cumsum(seg_len) - seg_len
        seg_src = (fo[:, None] + far_off).T.reshape(4)
        n_out = jnp.sum(seg_len)
        in_len = jnp.sum(lax.dynamic_slice(rl, (0, far), (2, 2)), axis=1)
        in_row = lax.dynamic_slice(ro, (0, far), (2, 1))[:, 0]
        in_base = jnp.stack([jnp.zeros((), i32), in_len[0]])
        n_in = jnp.sum(in_len)
        units = jnp.maximum((jnp.maximum(n_out, n_in) + 2 * CHUNK - 1) // (2 * CHUNK), 1)

        u = jnp.arange(cap, dtype=i32)
        p_of_u = (u // CHUNK * 2 + core) * CHUNK + u % CHUNK

        def pieces(x, base, length, src):
            inside = (x[:, None] >= base[None, :]) & (x[:, None] < (base + length)[None, :])
            return jnp.sum(jnp.where(inside, x[:, None] - base[None, :] + src[None, :], 0), axis=1), jnp.any(inside, axis=1)

        def stream_row(p):
            m = p // CHUNK
            return m // 2 * CHUNK + p % CHUNK + jnp.where(m % 2 == core, 0, cap)

        upos, _ = pieces(p_of_u, seg_base, seg_len, seg_src)
        near = 2 * chip
        near_base = lax.dynamic_slice(recv_off, (near,), (2,))
        near_len = lax.dynamic_slice(recv_len, (near,), (2,))
        near_src = fo + lax.dynamic_slice(so, (0, me), (2, 1))[:, 0]
        rpos, _ = pieces(u, near_base, near_len, near_src)
        my_row = lax.dynamic_slice(in_row, (core,), (1,))[0]
        my_len = lax.dynamic_slice(in_len, (core,), (1,))[0]
        my_base = lax.dynamic_slice(in_base, (core,), (1,))[0]
        spos = stream_row(jnp.clip(my_base + u - my_row, 0, 2 * cap - 1))
        ypos, _ = pieces(p_of_u, in_base, in_len, in_row + half_of)
        q = jnp.arange(n_tok, dtype=i32)
        far_base = lax.dynamic_slice(seg_base.reshape(2, 2), (0, core), (2, 1))[:, 0]
        my_far_off = lax.dynamic_slice(send_off, (far,), (2,))
        my_far_len = lax.dynamic_slice(send_len, (far,), (2,))
        my_near_off = lax.dynamic_slice(send_off, (near,), (2,))
        my_near_len = lax.dynamic_slice(send_len, (near,), (2,))
        far_pos, is_far = pieces(q, my_far_off, my_far_len, far_base)
        near_pos, is_near = pieces(q, my_near_off, my_near_len, half_of + lax.dynamic_slice(ro, (0, me), (2, 1))[:, 0])
        ridx = jnp.where(is_far, 2 * cap + stream_row(far_pos), jnp.where(is_near, near_pos, 4 * cap))
        perm = jnp.concatenate([tok_perm, sib_perm + n_tok])
        cnt = jnp.stack([units, my_row, my_len])

        rows_bf = jax.ShapeDtypeStruct((cap, dim), hidden.dtype)
        stream, rloc = local_call(pick_kernel, [rows_bf, rows_bf], 4, 0, 2, 2 * n_tok, cap, dim, "pick")(cnt, perm, upos, rpos, hidden, sib_hidden)
        arrived = exchange(stream, units, 1)
        dest_rows = local_call(place_kernel, rows_bf, 2, 1, 1, 2 * cap, cap, dim, "place")(cnt, spos, rloc, arrived)
        layer_rows = layer(dest_rows, recv_pos, g_attn, w_q, w_k, w_v, w_o, g_mlp, w_gate, w_up, w_down)
        sib_rows, = share([layer_rows], 2)
        back = local_call(back_pick_kernel, rows_bf, 2, 0, 2, 2 * cap, cap, dim, "back_pick")(cnt, ypos, layer_rows, sib_rows)
        returned = exchange(back, units, 3)
        return local_call(back_place_kernel, jax.ShapeDtypeStruct((n_tok, dim), hidden.dtype), 3, 0, 3, 4 * cap + 8, n_tok, dim, "back_place")(cnt, tok_perm, ridx, layer_rows, sib_rows, returned)

    return jax.shard_map(per_device, mesh=mesh, in_specs=(row_spec,) + (vec_spec,) * 7 + (rep_spec,) * 9, out_specs=row_spec, check_vma=False)
```

```python
import functools

import jax
import jax.numpy as jnp
from jax import lax
from jax.experimental import pallas as pl
from jax.experimental.pallas import tpu as pltpu
from jax.sharding import PartitionSpec as P

ROPE_BASE = 500000.0
NORM_EPS = 1e-5
ROWS = 512
QB = 256
FT = 256


def norm_rows(rows_f, gain):
    inv = lax.rsqrt(jnp.mean(rows_f * rows_f, axis=-1, keepdims=True) + NORM_EPS)
    return (rows_f * inv * gain).astype(jnp.bfloat16)


def rope_pair(x, cos_t, sin_t, first_half):
    swapped = jnp.where(first_half, pltpu.roll(x, 96, 1), pltpu.roll(x, 32, 1))
    return x * cos_t + swapped * sin_t


def dot_t(a, b):
    return lax.dot_general(a, b, (((1,), (1,)), ((), ())), preferred_element_type=jnp.float32)


def dot_n(a, b):
    return jnp.dot(a, b, preferred_element_type=jnp.float32)


def layer_kernel(maxs_ref, r_ref, start_ref, cos_ref, sin_ref, ga_ref, gm_ref, wq_h, wk_h, wv_h, wo_h, wg_h, wu_h, wd_h, out_ref,
                 q_s, k_s, v_s, o_s, h_s, m_s, wq_s, wk_s, wv_s, wo_s, wg_s, wu_s, wd_s, sems):
    n_rows, dim = r_ref.shape
    n_pairs = dim // 128
    ff = wg_s.shape[1]
    loads = [pltpu.make_async_copy(a, b, sems.at[i]) for i, (a, b) in enumerate(
        [(wq_h, wq_s), (wk_h, wk_s), (wv_h, wv_s), (wo_h, wo_s), (wg_h, wg_s), (wu_h, wu_s), (wd_h, wd_s)])]
    for c in loads:
        c.start()
    for c in loads[:3]:
        c.wait()
    gain_a = ga_ref[...].astype(jnp.float32)
    gain_m = gm_ref[...].astype(jnp.float32)

    @pl.loop(0, n_rows // QB)
    def _qkv(b):
        rows = pl.ds(pl.multiple_of(b * QB, QB), QB)
        lane = lax.broadcasted_iota(jnp.int32, (QB, 128), 1)
        first_half = lane % 64 < 32
        low = lane < 64
        h = norm_rows(r_ref[rows, :].astype(jnp.float32), gain_a)
        cos_t = cos_ref[rows, :]
        sin_t = sin_ref[rows, :]
        q = dot_t(h, wq_s[...])
        for p in range(n_pairs):
            qp = rope_pair(q[:, 128 * p:128 * (p + 1)], cos_t, sin_t, first_half)
            q_s[p, rows, :] = (qp.astype(jnp.bfloat16) * 0.125).astype(jnp.bfloat16)
        k = rope_pair(dot_t(h, wk_s[...]), cos_t, sin_t, first_half)
        v = dot_t(h, wv_s[...])
        for s, x in ((k_s, k), (v_s, v)):
            other = pltpu.roll(x, 64, 1)
            s[0, rows, :] = jnp.where(low, x, other).astype(jnp.bfloat16)
            s[1, rows, :] = jnp.where(low, other, x).astype(jnp.bfloat16)

    for c in range(n_rows // QB):
        length = (c + 1) * QB
        row = c * QB + lax.broadcasted_iota(jnp.int32, (QB, QB), 0)
        col = c * QB + lax.broadcasted_iota(jnp.int32, (QB, QB), 1)
        start = start_ref[c * QB:(c + 1) * QB, :]
        low_q = lax.broadcasted_iota(jnp.int32, (QB, 128), 1) < 64

        def heads(p, masked):
            outs = []
            qp = q_s[p, c * QB:(c + 1) * QB, :]
            for half in range(2):
                g = (2 * p + half) // 7
                qh = jnp.where(low_q if half == 0 else ~low_q, qp, jnp.zeros_like(qp))
                s = dot_t(qh, k_s[g, :length, :])
                diag = jnp.where((col >= start) & (col <= row), s[:, c * QB:], -1e30)
                if c == 0:
                    s = diag
                else:
                    body = s[:, :c * QB]
                    if masked:
                        body_col = lax.broadcasted_iota(jnp.int32, (QB, c * QB), 1)
                        body = jnp.where(body_col >= start, body, -1e30)
                    s = jnp.concatenate([body, diag], axis=1)
                top = jnp.max(s, axis=1, keepdims=True)
                e = jnp.exp(s - top)
                total = jnp.sum(e, axis=1, keepdims=True)
                outs.append(dot_n(e.astype(jnp.bfloat16), v_s[g, :length, :]) / total)
            o_s[c * QB:(c + 1) * QB, pl.ds(pl.multiple_of(p * 128, 128), 128)] = jnp.where(low_q, outs[0], outs[1]).astype(jnp.bfloat16)

        if c == 0:
            @pl.loop(0, n_pairs)
            def _pair(p):
                heads(p, False)
        else:
            has_start = maxs_ref[c] > 0

            @pl.when(has_start)
            def _masked():
                @pl.loop(0, n_pairs)
                def _pair(p):
                    heads(p, True)

            @pl.when(jnp.logical_not(has_start))
            def _plain():
                @pl.loop(0, n_pairs)
                def _pair(p):
                    heads(p, False)

    for c in loads[3:]:
        c.wait()

    @pl.loop(0, n_rows // ROWS)
    def _mlp(b):
        rows = pl.ds(pl.multiple_of(b * ROWS, ROWS), ROWS)
        attn = dot_n(o_s[rows, :], wo_s[...]).astype(jnp.bfloat16)
        z = (r_ref[rows, :].astype(jnp.float32) + attn.astype(jnp.float32)).astype(jnp.bfloat16)
        out_ref[rows, :] = z
        h_s[...] = norm_rows(z.astype(jnp.float32), gain_m)
        for t in range(ff // FT):
            cols = slice(t * FT, (t + 1) * FT)
            gate = dot_n(h_s[...], wg_s[:, cols])
            up = dot_n(h_s[...], wu_s[:, cols])
            m_s[:, cols] = (gate / (1.0 + jnp.exp(-gate)) * up).astype(jnp.bfloat16)
        down = dot_n(m_s[...], wd_s[...]).astype(jnp.bfloat16)
        out_ref[rows, :] = (out_ref[rows, :].astype(jnp.float32) + down.astype(jnp.float32)).astype(jnp.bfloat16)


def layer(dest_rows, positions, g_attn, w_q, w_k, w_v, w_o, g_mlp, w_gate, w_up, w_down):
    n_rows, dim = dest_rows.shape
    head_dim = w_q.shape[2]
    half_dim = head_dim // 2
    ff = w_gate.shape[1]
    inv_freq = jnp.power(jnp.float32(ROPE_BASE), -2.0 * jnp.arange(half_dim, dtype=jnp.float32) / head_dim)
    angles = positions.astype(jnp.float32)[:, None] * inv_freq[None, :]
    cos_t = jnp.cos(angles)
    sin_t = jnp.sin(angles)
    cos_t = jnp.concatenate([cos_t, cos_t, cos_t, cos_t], axis=1)
    sin_t = jnp.concatenate([-sin_t, sin_t, -sin_t, sin_t], axis=1)
    start = jnp.arange(n_rows, dtype=jnp.int32) - positions
    max_start = jnp.max(start.reshape(n_rows // QB, QB), axis=1)
    wq_t = jnp.transpose(w_q, (1, 2, 0)).reshape(dim, dim)
    wk_t = jnp.transpose(w_k, (1, 2, 0)).reshape(128, dim)
    wv_t = jnp.transpose(w_v, (1, 2, 0)).reshape(128, dim)
    wo_t = w_o.reshape(dim, dim)
    vm = pl.BlockSpec(memory_space=pltpu.VMEM)
    hb = pl.BlockSpec(memory_space=pl.ANY)
    bf = jnp.bfloat16
    return pl.pallas_call(
        layer_kernel,
        out_shape=jax.ShapeDtypeStruct((n_rows, dim), bf),
        in_specs=[pl.BlockSpec(memory_space=pltpu.SMEM)] + [vm] * 6 + [hb] * 7,
        out_specs=vm,
        scratch_shapes=[
            pltpu.VMEM((dim // 128, n_rows, 128), bf), pltpu.VMEM((2, n_rows, 128), bf), pltpu.VMEM((2, n_rows, 128), bf),
            pltpu.VMEM((n_rows, dim), bf), pltpu.VMEM((ROWS, dim), bf), pltpu.VMEM((ROWS, ff), bf),
            pltpu.VMEM((dim, dim), bf), pltpu.VMEM((128, dim), bf), pltpu.VMEM((128, dim), bf), pltpu.VMEM((dim, dim), bf),
            pltpu.VMEM((dim, ff), bf), pltpu.VMEM((dim, ff), bf), pltpu.VMEM((ff, dim), bf),
            pltpu.SemaphoreType.DMA((7,))],
        compiler_params=pltpu.CompilerParams(vmem_limit_bytes=66000000),
        cost_estimate=pl.CostEstimate(flops=60_000_000_000, bytes_accessed=40_000_000, transcendentals=0),
        name="layer",
    )(max_start, dest_rows, start[:, None], cos_t, sin_t, g_attn[None, :], g_mlp[None, :], wq_t, wk_t, wv_t, wo_t, w_gate, w_up, w_down)


CHUNK = 128
MESH_ID = pl.DeviceIdType.MESH
ANY = pl.BlockSpec(memory_space=pl.ANY)
VM = pl.BlockSpec(memory_space=pltpu.VMEM)
SM = pl.BlockSpec(memory_space=pltpu.SMEM)


def meet(devices):
    barrier = pltpu.get_barrier_semaphore()
    for dev in devices:
        pl.semaphore_signal(barrier, inc=1, device_id={"sp": dev}, device_id_type=MESH_ID)
    pl.semaphore_wait(barrier, len(devices))


def push(src, dst, send_sem, recv_sem, dev):
    return pltpu.make_async_remote_copy(src_ref=src, dst_ref=dst, send_sem=send_sem, recv_sem=recv_sem,
                                        device_id={"sp": dev}, device_id_type=MESH_ID)


def share_kernel(n_split, *refs):
    n = (len(refs) - 2) // 2
    ins, outs, send_sems, recv_sems = refs[:n], refs[n:2 * n], refs[-2], refs[-1]
    me = lax.axis_index("sp")
    sib = me + 1 - 2 * lax.rem(me, 2)
    meet([sib])
    copies = []
    for a, b in zip(ins, outs):
        parts = n_split if a.shape[0] % (16 * n_split) == 0 else 1
        step = a.shape[0] // parts
        for p in range(parts):
            rows = pl.ds(p * step, step)
            copies.append((a.at[rows], b.at[rows]))
    started = []
    for i, (a, b) in enumerate(copies):
        cp = push(a, b, send_sems.at[i], recv_sems.at[i], sib)
        cp.start()
        started.append(cp)
    for cp in started:
        cp.wait()


def share(arrays, collective_id):
    return pl.pallas_call(
        functools.partial(share_kernel, 4),
        out_shape=[jax.ShapeDtypeStruct(a.shape, a.dtype) for a in arrays],
        in_specs=[ANY] * len(arrays), out_specs=[ANY] * len(arrays),
        scratch_shapes=[pltpu.SemaphoreType.DMA((8,)), pltpu.SemaphoreType.DMA((8,))],
        compiler_params=pltpu.CompilerParams(collective_id=collective_id, has_side_effects=True),
        name="share",
    )(*arrays)


def cross_kernel(count, half, src, dst, s1, r1, s2, r2):
    me = lax.axis_index("sp")
    core = lax.rem(me, 2)
    sib = me + 1 - 2 * core
    peer = lax.rem(me + 2, 4)
    meet([sib, peer])
    outs = []
    for q in range(count):
        rows = pl.ds(q * CHUNK, CHUNK)
        cp = push(src.at[rows], dst.at[rows], s1.at[q], r1.at[q], peer)
        cp.start()
        outs.append(cp)
    fwd = []
    for q in range(count):
        outs[q].wait_recv()
        cp = push(dst.at[pl.ds(q * CHUNK, CHUNK)], dst.at[pl.ds(half + q * CHUNK, CHUNK)], s2.at[q], r2.at[q], sib)
        cp.start()
        fwd.append(cp)
    for q in range(count):
        outs[q].wait_send()
        fwd[q].wait()


def cross(stream, count, collective_id):
    half, dim = stream.shape
    return pl.pallas_call(
        functools.partial(cross_kernel, count, half),
        out_shape=jax.ShapeDtypeStruct((2 * half, dim), stream.dtype),
        in_specs=[ANY], out_specs=ANY,
        scratch_shapes=[pltpu.SemaphoreType.DMA((count,))] * 4,
        compiler_params=pltpu.CompilerParams(collective_id=collective_id, has_side_effects=True),
        name="cross",
    )(stream)


def exchange(stream, units, collective_id):
    top = stream.shape[0] // CHUNK
    return lax.switch(units - 1, [functools.partial(cross, count=k + 1, collective_id=collective_id) for k in range(top)], stream)


LOAD = 256


def load_table(parts, tab, stage, sems):
    base = 0
    for ref, rows, blocks in parts:
        n_blk = rows // LOAD if blocks is None else blocks

        def fetch(i, slot, ref=ref):
            return pltpu.make_async_copy(ref.at[pl.ds(pl.multiple_of(i * LOAD, LOAD), LOAD)], stage.at[slot], sems.at[slot])

        @pl.when(n_blk > 0)
        def _first():
            fetch(0, 0).start()

        @pl.loop(0, n_blk)
        def _blk(i, base=base):
            slot = lax.rem(i, 2)

            @pl.when(i + 1 < n_blk)
            def _next():
                fetch(i + 1, 1 - slot).start()

            fetch(i, slot).wait()
            first = pl.multiple_of((base + i * LOAD) * 8, 8)
            for j in range(stage.shape[2] // 128):
                tab[pl.ds(first + j, LOAD, stride=8), :] = stage[slot, :, 128 * j:128 * (j + 1)].astype(jnp.float32)

        base += rows


UNROLL = 16


def slab(k):
    return pl.ds(pl.multiple_of(k * 8, 8), 8)


def copy_rows(n_rows, move):
    @pl.loop(0, n_rows // UNROLL)
    def _grp(i):
        for k in range(UNROLL):
            move(i * UNROLL + k)


def rows_out(n_rows, src3, dst):
    @pl.loop(0, n_rows // CHUNK)
    def _blk(i):
        rows = pl.ds(pl.multiple_of(i * CHUNK, CHUNK), CHUNK)
        for j in range(dst.shape[1] // 128):
            dst[rows, 128 * j:128 * (j + 1)] = src3[pl.ds(pl.multiple_of(i * CHUNK * 8, 8) + j, CHUNK, stride=8), :].astype(dst.dtype)


def pick_kernel(cnt, perm, upos, rpos, own, sib, stream, rloc, tab, out3, stage, sems):
    n_tok = own.shape[0]
    cap = rloc.shape[0]
    load_table([(own, n_tok, None), (sib, n_tok, None)], tab, stage, sems)

    def one_u(k):
        out3[slab(k), :] = tab[slab(perm[upos[k]]), :]

    copy_rows(cnt[0] * CHUNK, one_u)
    rows_out(cnt[0] * CHUNK, out3, stream)

    def one_r(k):
        out3[slab(k), :] = tab[slab(perm[rpos[k]]), :]

    copy_rows(cap, one_r)
    rows_out(cap, out3, rloc)


def place_kernel(cnt, spos, rloc, stream, out, tab, out3, stage, sems):
    cap = out.shape[0]
    blocks = (cnt[0] * CHUNK + LOAD - 1) // LOAD
    load_table([(stream.at[pl.ds(0, cap)], cap, blocks), (stream.at[pl.ds(cap, cap)], cap, blocks)], tab, stage, sems)
    first, last = cnt[1], cnt[1] + cnt[2]

    def one(k):
        out3[slab(k), :] = tab[slab(spos[k]), :]

    lo = first // UNROLL * UNROLL

    @pl.loop(lo // UNROLL, (last + UNROLL - 1) // UNROLL)
    def _grp(i):
        for k in range(UNROLL):
            one(i * UNROLL + k)

    @pl.loop(0, cap // CHUNK)
    def _blk(i):
        rows = pl.ds(pl.multiple_of(i * CHUNK, CHUNK), CHUNK)
        row = i * CHUNK + lax.broadcasted_iota(jnp.int32, (CHUNK, 128), 0)
        keep = (row >= first) & (row < last)
        for j in range(out.shape[1] // 128):
            cols = slice(128 * j, 128 * (j + 1))
            far = out3[pl.ds(pl.multiple_of(i * CHUNK * 8, 8) + j, CHUNK, stride=8), :]
            out[rows, cols] = jnp.where(keep, far, rloc[rows, cols].astype(jnp.float32)).astype(out.dtype)


def back_pick_kernel(cnt, ypos, own, sib, stream, tab, out3, stage, sems):
    cap = own.shape[0]
    load_table([(own, cap, None), (sib, cap, None)], tab, stage, sems)

    def one(k):
        out3[slab(k), :] = tab[slab(ypos[k]), :]

    copy_rows(cnt[0] * CHUNK, one)
    rows_out(cnt[0] * CHUNK, out3, stream)


def back_place_kernel(cnt, perm, ridx, own, sib, stream, out, tab, out3, stage, sems):
    cap = own.shape[0]
    n_tok = out.shape[0]
    blocks = (cnt[0] * CHUNK + LOAD - 1) // LOAD
    load_table([(own, cap, None), (sib, cap, None), (stream.at[pl.ds(0, cap)], cap, blocks), (stream.at[pl.ds(cap, cap)], cap, blocks)], tab, stage, sems)
    tab[slab(4 * cap), :] = jnp.zeros((8, 128), jnp.float32)

    def one(k):
        out3[slab(perm[k]), :] = tab[slab(ridx[k]), :]

    copy_rows(n_tok, one)
    rows_out(n_tok, out3, out)


def local_call(body, out_shapes, n_smem, n_vmem, n_any, tab_rows, out_rows, dim, name):
    return pl.pallas_call(
        body,
        out_shape=out_shapes,
        in_specs=[SM] * n_smem + [VM] * n_vmem + [ANY] * n_any,
        out_specs=jax.tree.map(lambda _: VM, out_shapes),
        scratch_shapes=[pltpu.VMEM((tab_rows * 8, 128), jnp.float32), pltpu.VMEM((out_rows * 8, 128), jnp.float32),
                        pltpu.VMEM((2, LOAD, dim), jnp.bfloat16), pltpu.SemaphoreType.DMA((2,))],
        compiler_params=pltpu.CompilerParams(vmem_limit_bytes=66000000),
        name=name,
    )


def solution(mesh):
    row_spec = P(('dp', 'sp'), None)
    vec_spec = P(('dp', 'sp'))
    rep_spec = P()

    def per_device(hidden, tok_perm, send_off, send_len, recv_off, recv_len, recv_doc, recv_pos, g_attn, w_q, w_k, w_v, w_o, g_mlp, w_gate, w_up, w_down):
        n_tok, dim = hidden.shape
        cap = recv_doc.shape[0]
        i32 = jnp.int32
        me = lax.axis_index('sp')
        core = me % 2
        chip = me // 2
        plan = jnp.concatenate([tok_perm, send_off, send_len, recv_off, recv_len, jnp.zeros((1024 - 16,), i32)]).reshape(-1, 128)
        sib_hidden, sib_plan = share([hidden, plan], 0)
        sib_plan = sib_plan.reshape(-1)
        sib_perm = sib_plan[:n_tok]

        def both(own, at):
            other = lax.slice(sib_plan, (n_tok + at,), (n_tok + at + 4,))
            return jnp.where(core == 0, jnp.stack([own, other]), jnp.stack([other, own]))

        so, sl, ro, rl = both(send_off, 0), both(send_len, 4), both(recv_off, 8), both(recv_len, 12)
        far = 2 * (1 - chip)
        cores = jnp.arange(2, dtype=i32)
        fo = jnp.where(cores == core, 0, n_tok)
        half_of = jnp.where(cores == core, 0, cap)
        far_len = lax.dynamic_slice(sl, (0, far), (2, 2))
        far_off = lax.dynamic_slice(so, (0, far), (2, 2))
        seg_len = far_len.T.reshape(4)
        seg_base = jnp.cumsum(seg_len) - seg_len
        seg_src = (fo[:, None] + far_off).T.reshape(4)
        n_out = jnp.sum(seg_len)
        in_len = jnp.sum(lax.dynamic_slice(rl, (0, far), (2, 2)), axis=1)
        in_row = lax.dynamic_slice(ro, (0, far), (2, 1))[:, 0]
        in_base = jnp.stack([jnp.zeros((), i32), in_len[0]])
        n_in = jnp.sum(in_len)
        units = jnp.maximum((jnp.maximum(n_out, n_in) + 2 * CHUNK - 1) // (2 * CHUNK), 1)

        u = jnp.arange(cap, dtype=i32)
        p_of_u = (u // CHUNK * 2 + core) * CHUNK + u % CHUNK

        def pieces(x, base, length, src):
            inside = (x[:, None] >= base[None, :]) & (x[:, None] < (base + length)[None, :])
            return jnp.sum(jnp.where(inside, x[:, None] - base[None, :] + src[None, :], 0), axis=1), jnp.any(inside, axis=1)

        def stream_row(p):
            m = p // CHUNK
            return m // 2 * CHUNK + p % CHUNK + jnp.where(m % 2 == core, 0, cap)

        upos, _ = pieces(p_of_u, seg_base, seg_len, seg_src)
        near = 2 * chip
        near_base = lax.dynamic_slice(recv_off, (near,), (2,))
        near_len = lax.dynamic_slice(recv_len, (near,), (2,))
        near_src = fo + lax.dynamic_slice(so, (0, me), (2, 1))[:, 0]
        rpos, _ = pieces(u, near_base, near_len, near_src)
        my_row = lax.dynamic_slice(in_row, (core,), (1,))[0]
        my_len = lax.dynamic_slice(in_len, (core,), (1,))[0]
        my_base = lax.dynamic_slice(in_base, (core,), (1,))[0]
        spos = stream_row(jnp.clip(my_base + u - my_row, 0, 2 * cap - 1))
        ypos, _ = pieces(p_of_u, in_base, in_len, in_row + half_of)
        q = jnp.arange(n_tok, dtype=i32)
        far_base = lax.dynamic_slice(seg_base.reshape(2, 2), (0, core), (2, 1))[:, 0]
        my_far_off = lax.dynamic_slice(send_off, (far,), (2,))
        my_far_len = lax.dynamic_slice(send_len, (far,), (2,))
        my_near_off = lax.dynamic_slice(send_off, (near,), (2,))
        my_near_len = lax.dynamic_slice(send_len, (near,), (2,))
        far_pos, is_far = pieces(q, my_far_off, my_far_len, far_base)
        near_pos, is_near = pieces(q, my_near_off, my_near_len, half_of + lax.dynamic_slice(ro, (0, me), (2, 1))[:, 0])
        ridx = jnp.where(is_far, 2 * cap + stream_row(far_pos), jnp.where(is_near, near_pos, 4 * cap))
        perm = jnp.concatenate([tok_perm, sib_perm + n_tok])
        cnt = jnp.stack([units, my_row, my_len])

        rows_bf = jax.ShapeDtypeStruct((cap, dim), hidden.dtype)
        stream, rloc = local_call(pick_kernel, [rows_bf, rows_bf], 4, 0, 2, 2 * n_tok, cap, dim, "pick")(cnt, perm, upos, rpos, hidden, sib_hidden)
        arrived = exchange(stream, units, 1)
        dest_rows = local_call(place_kernel, rows_bf, 2, 1, 1, 2 * cap, cap, dim, "place")(cnt, spos, rloc, arrived)
        layer_rows = layer(dest_rows, recv_pos, g_attn, w_q, w_k, w_v, w_o, g_mlp, w_gate, w_up, w_down)
        sib_rows, = share([layer_rows], 2)
        back = local_call(back_pick_kernel, rows_bf, 2, 0, 2, 2 * cap, cap, dim, "back_pick")(cnt, ypos, layer_rows, sib_rows)
        returned = exchange(back, units, 3)
        return local_call(back_place_kernel, jax.ShapeDtypeStruct((n_tok, dim), hidden.dtype), 3, 0, 3, 4 * cap + 8, n_tok, dim, "back_place")(cnt, tok_perm, ridx, layer_rows, sib_rows, returned)

    return jax.shard_map(per_device, mesh=mesh, in_specs=(row_spec,) + (vec_spec,) * 7 + (rep_spec,) * 9, out_specs=row_spec, check_vma=False)
```

```python
import functools

import jax
import jax.numpy as jnp
from jax import lax
from jax.experimental import pallas as pl
from jax.experimental.pallas import tpu as pltpu
from jax.sharding import PartitionSpec as P

ROPE_BASE = 500000.0
NORM_EPS = 1e-5
ROWS = 512
QB = 256
FT = 256


def norm_rows(rows_f, gain):
    inv = lax.rsqrt(jnp.mean(rows_f * rows_f, axis=-1, keepdims=True) + NORM_EPS)
    return (rows_f * inv * gain).astype(jnp.bfloat16)


def rope_pair(x, cos_t, sin_t, first_half):
    swapped = jnp.where(first_half, pltpu.roll(x, 96, 1), pltpu.roll(x, 32, 1))
    return x * cos_t + swapped * sin_t


def dot_t(a, b):
    return lax.dot_general(a, b, (((1,), (1,)), ((), ())), preferred_element_type=jnp.float32)


def dot_n(a, b):
    return jnp.dot(a, b, preferred_element_type=jnp.float32)


def attn_kernel(maxs_ref, r_ref, start_ref, cos_ref, sin_ref, ga_ref, wq_h, wk_h, wv_h, wo_h, out_ref,
                q_s, k_s, v_s, o_s, wq_s, wk_s, wv_s, wo_s, sems):
    n_rows, dim = r_ref.shape
    n_pairs = dim // 128
    loads = [pltpu.make_async_copy(a, b, sems.at[i]) for i, (a, b) in enumerate(
        [(wq_h, wq_s), (wk_h, wk_s), (wv_h, wv_s), (wo_h, wo_s)])]
    for c in loads:
        c.start()
    for c in loads[:3]:
        c.wait()
    gain_a = ga_ref[...].astype(jnp.float32)

    @pl.loop(0, n_rows // QB)
    def _qkv(b):
        rows = pl.ds(pl.multiple_of(b * QB, QB), QB)
        lane = lax.broadcasted_iota(jnp.int32, (QB, 128), 1)
        first_half = lane % 64 < 32
        low = lane < 64
        h = norm_rows(r_ref[rows, :].astype(jnp.float32), gain_a)
        cos_t = cos_ref[rows, :]
        sin_t = sin_ref[rows, :]
        q = dot_t(h, wq_s[...])
        for p in range(n_pairs):
            qp = rope_pair(q[:, 128 * p:128 * (p + 1)], cos_t, sin_t, first_half)
            q_s[p, rows, :] = (qp.astype(jnp.bfloat16) * 0.125).astype(jnp.bfloat16)
        k = rope_pair(dot_t(h, wk_s[...]), cos_t, sin_t, first_half)
        v = dot_t(h, wv_s[...])
        for s, x in ((k_s, k), (v_s, v)):
            other = pltpu.roll(x, 64, 1)
            s[0, rows, :] = jnp.where(low, x, other).astype(jnp.bfloat16)
            s[1, rows, :] = jnp.where(low, other, x).astype(jnp.bfloat16)

    for c in range(n_rows // QB):
        length = (c + 1) * QB
        row = c * QB + lax.broadcasted_iota(jnp.int32, (QB, QB), 0)
        col = c * QB + lax.broadcasted_iota(jnp.int32, (QB, QB), 1)
        start = start_ref[c * QB:(c + 1) * QB, :]
        low_q = lax.broadcasted_iota(jnp.int32, (QB, 128), 1) < 64

        def heads(p, masked):
            outs = []
            qp = q_s[p, c * QB:(c + 1) * QB, :]
            for half in range(2):
                g = (2 * p + half) // 7
                qh = jnp.where(low_q if half == 0 else ~low_q, qp, jnp.zeros_like(qp))
                s = dot_t(qh, k_s[g, :length, :])
                diag = jnp.where((col >= start) & (col <= row), s[:, c * QB:], -1e30)
                if c == 0:
                    s = diag
                else:
                    body = s[:, :c * QB]
                    if masked:
                        body_col = lax.broadcasted_iota(jnp.int32, (QB, c * QB), 1)
                        body = jnp.where(body_col >= start, body, -1e30)
                    s = jnp.concatenate([body, diag], axis=1)
                top = jnp.max(s, axis=1, keepdims=True)
                e = jnp.exp(s - top)
                total = jnp.sum(e, axis=1, keepdims=True)
                outs.append(dot_n(e.astype(jnp.bfloat16), v_s[g, :length, :]) / total)
            o_s[c * QB:(c + 1) * QB, pl.ds(pl.multiple_of(p * 128, 128), 128)] = jnp.where(low_q, outs[0], outs[1]).astype(jnp.bfloat16)

        if c == 0:
            @pl.loop(0, n_pairs)
            def _pair(p):
                heads(p, False)
        else:
            has_start = maxs_ref[c] > 0

            @pl.when(has_start)
            def _masked():
                @pl.loop(0, n_pairs)
                def _pair(p):
                    heads(p, True)

            @pl.when(jnp.logical_not(has_start))
            def _plain():
                @pl.loop(0, n_pairs)
                def _pair(p):
                    heads(p, False)

    for c in loads[3:]:
        c.wait()

    @pl.loop(0, n_rows // ROWS)
    def _out(b):
        rows = pl.ds(pl.multiple_of(b * ROWS, ROWS), ROWS)
        attn = dot_n(o_s[rows, :], wo_s[...]).astype(jnp.bfloat16)
        out_ref[rows, :] = (r_ref[rows, :].astype(jnp.float32) + attn.astype(jnp.float32)).astype(jnp.bfloat16)


def attention(dest_rows, positions, g_attn, w_q, w_k, w_v, w_o):
    n_rows, dim = dest_rows.shape
    head_dim = w_q.shape[2]
    half_dim = head_dim // 2
    inv_freq = jnp.power(jnp.float32(ROPE_BASE), -2.0 * jnp.arange(half_dim, dtype=jnp.float32) / head_dim)
    angles = positions.astype(jnp.float32)[:, None] * inv_freq[None, :]
    cos_t = jnp.cos(angles)
    sin_t = jnp.sin(angles)
    cos_t = jnp.concatenate([cos_t, cos_t, cos_t, cos_t], axis=1)
    sin_t = jnp.concatenate([-sin_t, sin_t, -sin_t, sin_t], axis=1)
    start = jnp.arange(n_rows, dtype=jnp.int32) - positions
    max_start = jnp.max(start.reshape(n_rows // QB, QB), axis=1)
    wq_t = jnp.transpose(w_q, (1, 2, 0)).reshape(dim, dim)
    wk_t = jnp.transpose(w_k, (1, 2, 0)).reshape(128, dim)
    wv_t = jnp.transpose(w_v, (1, 2, 0)).reshape(128, dim)
    wo_t = w_o.reshape(dim, dim)
    vm = pl.BlockSpec(memory_space=pltpu.VMEM)
    hb = pl.BlockSpec(memory_space=pl.ANY)
    bf = jnp.bfloat16
    return pl.pallas_call(
        attn_kernel,
        out_shape=jax.ShapeDtypeStruct((n_rows, dim), bf),
        in_specs=[pl.BlockSpec(memory_space=pltpu.SMEM)] + [vm] * 5 + [hb] * 4,
        out_specs=vm,
        scratch_shapes=[
            pltpu.VMEM((dim // 128, n_rows, 128), bf), pltpu.VMEM((2, n_rows, 128), bf), pltpu.VMEM((2, n_rows, 128), bf),
            pltpu.VMEM((n_rows, dim), bf),
            pltpu.VMEM((dim, dim), bf), pltpu.VMEM((128, dim), bf), pltpu.VMEM((128, dim), bf), pltpu.VMEM((dim, dim), bf),
            pltpu.SemaphoreType.DMA((4,))],
        compiler_params=pltpu.CompilerParams(vmem_limit_bytes=66000000),
        name="attention",
    )(max_start, dest_rows, start[:, None], cos_t, sin_t, g_attn[None, :], wq_t, wk_t, wv_t, wo_t)


CHUNK = 128
MESH_ID = pl.DeviceIdType.MESH
ANY = pl.BlockSpec(memory_space=pl.ANY)
VM = pl.BlockSpec(memory_space=pltpu.VMEM)
SM = pl.BlockSpec(memory_space=pltpu.SMEM)


def meet(devices):
    barrier = pltpu.get_barrier_semaphore()
    for dev in devices:
        pl.semaphore_signal(barrier, inc=1, device_id={"sp": dev}, device_id_type=MESH_ID)
    pl.semaphore_wait(barrier, len(devices))


def push(src, dst, send_sem, recv_sem, dev):
    return pltpu.make_async_remote_copy(src_ref=src, dst_ref=dst, send_sem=send_sem, recv_sem=recv_sem,
                                        device_id={"sp": dev}, device_id_type=MESH_ID)


def share_kernel(n_split, *refs):
    n = (len(refs) - 2) // 2
    ins, outs, send_sems, recv_sems = refs[:n], refs[n:2 * n], refs[-2], refs[-1]
    me = lax.axis_index("sp")
    sib = me + 1 - 2 * lax.rem(me, 2)
    meet([sib])
    copies = []
    for a, b in zip(ins, outs):
        parts = n_split if a.shape[0] % (16 * n_split) == 0 else 1
        step = a.shape[0] // parts
        for p in range(parts):
            rows = pl.ds(p * step, step)
            copies.append((a.at[rows], b.at[rows]))
    started = []
    for i, (a, b) in enumerate(copies):
        cp = push(a, b, send_sems.at[i], recv_sems.at[i], sib)
        cp.start()
        started.append(cp)
    for cp in started:
        cp.wait()


def share(arrays, collective_id):
    return pl.pallas_call(
        functools.partial(share_kernel, 4),
        out_shape=[jax.ShapeDtypeStruct(a.shape, a.dtype) for a in arrays],
        in_specs=[ANY] * len(arrays), out_specs=[ANY] * len(arrays),
        scratch_shapes=[pltpu.SemaphoreType.DMA((8,)), pltpu.SemaphoreType.DMA((8,))],
        compiler_params=pltpu.CompilerParams(collective_id=collective_id, has_side_effects=True),
        name="share",
    )(*arrays)


def cross_kernel(count, half, src, dst, s1, r1, s2, r2):
    me = lax.axis_index("sp")
    core = lax.rem(me, 2)
    sib = me + 1 - 2 * core
    peer = lax.rem(me + 2, 4)
    meet([sib, peer])
    outs = []
    for q in range(count):
        rows = pl.ds(q * CHUNK, CHUNK)
        cp = push(src.at[rows], dst.at[rows], s1.at[q], r1.at[q], peer)
        cp.start()
        outs.append(cp)
    fwd = []
    for q in range(count):
        outs[q].wait_recv()
        cp = push(dst.at[pl.ds(q * CHUNK, CHUNK)], dst.at[pl.ds(half + q * CHUNK, CHUNK)], s2.at[q], r2.at[q], sib)
        cp.start()
        fwd.append(cp)
    for q in range(count):
        outs[q].wait_send()
        fwd[q].wait()


def cross(stream, count, collective_id):
    half, dim = stream.shape
    return pl.pallas_call(
        functools.partial(cross_kernel, count, half),
        out_shape=jax.ShapeDtypeStruct((2 * half, dim), stream.dtype),
        in_specs=[ANY], out_specs=ANY,
        scratch_shapes=[pltpu.SemaphoreType.DMA((count,))] * 4,
        compiler_params=pltpu.CompilerParams(collective_id=collective_id, has_side_effects=True),
        name="cross",
    )(stream)


def exchange(stream, units, collective_id):
    top = stream.shape[0] // CHUNK
    return lax.switch(units - 1, [functools.partial(cross, count=k + 1, collective_id=collective_id) for k in range(top)], stream)


LOAD = 512


def load_table(parts, tab, stage, sems):
    jobs = []
    for ref, blocks in parts:
        for i in range(ref.shape[0] // LOAD):
            n = len(jobs)
            copy = pltpu.make_async_copy(ref.at[pl.ds(i * LOAD, LOAD)], stage.at[pl.ds(n * LOAD, LOAD)], sems.at[n])
            jobs.append((copy, None if blocks is None else i < blocks))
    for copy, cond in jobs:
        if cond is None:
            copy.start()
        else:
            pl.when(cond)(copy.start)
    for n, (copy, cond) in enumerate(jobs):
        def fill(n=n, copy=copy):
            copy.wait()
            fill_table(stage, n * LOAD, tab, n * LOAD)
        if cond is None:
            fill()
        else:
            pl.when(cond)(fill)


def fill_table(stage, at, tab, base):
    @pl.loop(0, LOAD // 64)
    def _blk(i):
        rows = pl.ds(pl.multiple_of(at + i * 64, 64), 64)
        first = pl.multiple_of((base + i * 64) * 8, 8)
        for j in range(stage.shape[1] // 128):
            tab[pl.ds(first + j, 64, stride=8), :] = stage[rows, 128 * j:128 * (j + 1)].astype(jnp.float32)


UNROLL = 16


def slab(k):
    return pl.ds(pl.multiple_of(k * 8, 8), 8)


def copy_rows(n_rows, move):
    @pl.loop(0, n_rows // UNROLL)
    def _grp(i):
        for k in range(UNROLL):
            move(i * UNROLL + k)


def rows_out(n_rows, src3, dst):
    @pl.loop(0, n_rows // CHUNK)
    def _blk(i):
        rows = pl.ds(pl.multiple_of(i * CHUNK, CHUNK), CHUNK)
        for j in range(dst.shape[1] // 128):
            dst[rows, 128 * j:128 * (j + 1)] = src3[pl.ds(pl.multiple_of(i * CHUNK * 8, 8) + j, CHUNK, stride=8), :].astype(dst.dtype)


def pick_kernel(cnt, perm, upos, rpos, own, sib, stream, rloc, tab, out3, stage, sems):
    n_tok = own.shape[0]
    cap = rloc.shape[0]
    load_table([(own, None), (sib, None)], tab, stage, sems)

    def one_u(k):
        out3[slab(k), :] = tab[slab(perm[upos[k]]), :]

    copy_rows(cnt[0] * CHUNK, one_u)
    rows_out(cnt[0] * CHUNK, out3, stream)

    def one_r(k):
        out3[slab(k), :] = tab[slab(perm[rpos[k]]), :]

    copy_rows(cap, one_r)
    rows_out(cap, out3, rloc)


def place_kernel(cnt, spos, rloc, stream, out, tab, out3, stage, sems):
    cap = out.shape[0]
    blocks = (cnt[0] * CHUNK + LOAD - 1) // LOAD
    load_table([(stream.at[pl.ds(0, cap)], blocks), (stream.at[pl.ds(cap, cap)], blocks)], tab, stage, sems)
    first, last = cnt[1], cnt[1] + cnt[2]

    def one(k):
        out3[slab(k), :] = tab[slab(spos[k]), :]

    lo = first // UNROLL * UNROLL

    @pl.loop(lo // UNROLL, (last + UNROLL - 1) // UNROLL)
    def _grp(i):
        for k in range(UNROLL):
            one(i * UNROLL + k)

    @pl.loop(0, cap // CHUNK)
    def _blk(i):
        rows = pl.ds(pl.multiple_of(i * CHUNK, CHUNK), CHUNK)
        row = i * CHUNK + lax.broadcasted_iota(jnp.int32, (CHUNK, 128), 0)
        keep = (row >= first) & (row < last)
        for j in range(out.shape[1] // 128):
            cols = slice(128 * j, 128 * (j + 1))
            far = out3[pl.ds(pl.multiple_of(i * CHUNK * 8, 8) + j, CHUNK, stride=8), :]
            out[rows, cols] = jnp.where(keep, far, rloc[rows, cols].astype(jnp.float32)).astype(out.dtype)


def back_place_kernel(cnt, perm, ridx, own, sib, stream, out, tab, out3, stage, sems):
    cap = own.shape[0]
    n_tok = out.shape[0]
    load_table([(own, None), (sib, None), (stream, None)], tab, stage, sems)
    tab[slab(4 * cap), :] = jnp.zeros((8, 128), jnp.float32)

    def one(k):
        out3[slab(perm[k]), :] = tab[slab(ridx[k]), :]

    copy_rows(n_tok, one)
    rows_out(n_tok, out3, out)


GROUP = 256
SENDS = (2, 4, 6)


def mlp_kernel(n_send, z_ref, gm_ref, wg_h, wu_h, wd_h, own, sib_out, far, obuf, m_s, wg_s, wu_s, wd_s, w_sems, own_sem, ps, pr, ss, sr, fs, fr):
    cap, dim = z_ref.shape
    ff = wg_s.shape[1]
    n_grp = cap // GROUP
    me = lax.axis_index("sp")
    core = lax.rem(me, 2)
    chip = me // 2
    sib = me + 1 - 2 * core
    peer = lax.rem(me + 2, 4)
    loads = [pltpu.make_async_copy(x, y, w_sems.at[i]) for i, (x, y) in enumerate([(wg_h, wg_s), (wu_h, wu_s), (wd_h, wd_s)])]
    for c in loads:
        c.start()
    meet([sib, peer])
    gain = gm_ref[...].astype(jnp.float32)
    for c in loads:
        c.wait()

    def group_of(i, at_chip):
        return at_chip * i + (1 - at_chip) * (n_grp - 1 - i)

    def rows_at(g):
        return pl.ds(pl.multiple_of(g * GROUP, GROUP), GROUP)

    def to_peer(i):
        rows = rows_at(group_of(i, chip))
        return push(own.at[rows], far.at[rows], ps.at[i], pr.at[i], peer)

    def to_sib(i):
        rows = rows_at(group_of(i, chip))
        return push(own.at[rows], sib_out.at[rows], ss.at[i], sr.at[i], sib)

    def forward(i):
        g = group_of(i, 1 - chip)
        return push(far.at[rows_at(g)], far.at[pl.ds(pl.multiple_of(cap + g * GROUP, GROUP), GROUP)], fs.at[i], fr.at[i], sib)

    def keep(i):
        return pltpu.make_async_copy(obuf.at[lax.rem(i, 2)], own.at[rows_at(group_of(i, chip))], own_sem.at[i])

    def send(i):
        keep(i).wait()
        to_sib(i).start()

        @pl.when(i < n_send)
        def _peer():
            to_peer(i).start()

    @pl.loop(0, n_grp)
    def _group(i):
        z = z_ref[rows_at(group_of(i, chip)), :].astype(jnp.float32)
        h = norm_rows(z, gain)

        @pl.when(i >= 1)
        def _send():
            send(i - 1)

        @pl.when(jnp.logical_and(i >= 3, i - 3 < n_send))
        def _fwd():
            to_peer(i - 3).wait_recv()
            forward(i - 3).start()

        for t in range(ff // FT):
            cols = slice(t * FT, (t + 1) * FT)
            gate = dot_n(h, wg_s[:, cols])
            up = dot_n(h, wu_s[:, cols])
            m_s[:, cols] = (gate / (1.0 + jnp.exp(-gate)) * up).astype(jnp.bfloat16)
        down = dot_n(m_s[...], wd_s[...]).astype(jnp.bfloat16)
        obuf[lax.rem(i, 2)] = (z + down.astype(jnp.float32)).astype(jnp.bfloat16)
        keep(i).start()

    send(n_grp - 1)
    for i in range(max(n_grp - 3, 0), n_send):
        to_peer(i).wait_recv()
        forward(i).start()
    for i in range(n_grp):
        to_sib(i).wait()
    for i in range(n_send):
        to_peer(i).wait_send()
        forward(i).wait()


def mlp(z, g_mlp, w_gate, w_up, w_down, n_send):
    cap, dim = z.shape
    ff = w_gate.shape[1]
    bf = jnp.bfloat16
    n_grp = cap // GROUP
    dma = pltpu.SemaphoreType.DMA
    rows = jax.ShapeDtypeStruct((cap, dim), bf)
    return pl.pallas_call(
        functools.partial(mlp_kernel, n_send),
        out_shape=[rows, rows, jax.ShapeDtypeStruct((2 * cap, dim), bf)],
        in_specs=[VM, VM, ANY, ANY, ANY], out_specs=[ANY] * 3,
        scratch_shapes=[
            pltpu.VMEM((2, GROUP, dim), bf), pltpu.VMEM((GROUP, ff), bf),
            pltpu.VMEM((dim, ff), bf), pltpu.VMEM((dim, ff), bf), pltpu.VMEM((ff, dim), bf),
            dma((3,))] + [dma((n_grp,))] * 7,
        compiler_params=pltpu.CompilerParams(collective_id=2, has_side_effects=True, vmem_limit_bytes=66000000),
        name="mlp",
    )(z, g_mlp[None, :], w_gate, w_up, w_down)


def local_call(body, out_shapes, n_smem, n_vmem, n_any, tab_rows, out_rows, dim, name):
    return pl.pallas_call(
        body,
        out_shape=out_shapes,
        in_specs=[SM] * n_smem + [VM] * n_vmem + [ANY] * n_any,
        out_specs=jax.tree.map(lambda _: VM, out_shapes),
        scratch_shapes=[pltpu.VMEM((tab_rows * 8, 128), jnp.float32), pltpu.VMEM((out_rows * 8, 128), jnp.float32),
                        pltpu.VMEM((tab_rows // LOAD * LOAD, dim), jnp.bfloat16), pltpu.SemaphoreType.DMA((tab_rows // LOAD,))],
        compiler_params=pltpu.CompilerParams(vmem_limit_bytes=66000000),
        name=name,
    )


def solution(mesh):
    row_spec = P(('dp', 'sp'), None)
    vec_spec = P(('dp', 'sp'))
    rep_spec = P()

    def per_device(hidden, tok_perm, send_off, send_len, recv_off, recv_len, recv_doc, recv_pos, g_attn, w_q, w_k, w_v, w_o, g_mlp, w_gate, w_up, w_down):
        n_tok, dim = hidden.shape
        cap = recv_doc.shape[0]
        i32 = jnp.int32
        me = lax.axis_index('sp')
        core = me % 2
        chip = me // 2
        plan = jnp.concatenate([tok_perm, send_off, send_len, recv_off, recv_len, jnp.zeros((1024 - 16,), i32)]).reshape(-1, 128)
        sib_hidden, sib_plan = share([hidden, plan], 0)
        sib_plan = sib_plan.reshape(-1)
        sib_perm = sib_plan[:n_tok]

        def both(own, at):
            other = lax.slice(sib_plan, (n_tok + at,), (n_tok + at + 4,))
            return jnp.where(core == 0, jnp.stack([own, other]), jnp.stack([other, own]))

        so, sl, ro, rl = both(send_off, 0), both(send_len, 4), both(recv_off, 8), both(recv_len, 12)
        far = 2 * (1 - chip)
        cores = jnp.arange(2, dtype=i32)
        fo = jnp.where(cores == core, 0, n_tok)
        half_of = jnp.where(cores == core, 0, cap)
        far_len = lax.dynamic_slice(sl, (0, far), (2, 2))
        far_off = lax.dynamic_slice(so, (0, far), (2, 2))
        seg_len = far_len.T.reshape(4)
        seg_base = jnp.cumsum(seg_len) - seg_len
        seg_src = (fo[:, None] + far_off).T.reshape(4)
        n_out = jnp.sum(seg_len)
        in_len = jnp.sum(lax.dynamic_slice(rl, (0, far), (2, 2)), axis=1)
        in_row = lax.dynamic_slice(ro, (0, far), (2, 1))[:, 0]
        in_base = jnp.stack([jnp.zeros((), i32), in_len[0]])
        n_in = jnp.sum(in_len)
        units = jnp.maximum((jnp.maximum(n_out, n_in) + 2 * CHUNK - 1) // (2 * CHUNK), 1)

        u = jnp.arange(cap, dtype=i32)
        p_of_u = (u // CHUNK * 2 + core) * CHUNK + u % CHUNK

        def pieces(x, base, length, src):
            inside = (x[:, None] >= base[None, :]) & (x[:, None] < (base + length)[None, :])
            return jnp.sum(jnp.where(inside, x[:, None] - base[None, :] + src[None, :], 0), axis=1), jnp.any(inside, axis=1)

        def stream_row(p):
            m = p // CHUNK
            return m // 2 * CHUNK + p % CHUNK + jnp.where(m % 2 == core, 0, cap)

        upos, _ = pieces(p_of_u, seg_base, seg_len, seg_src)
        near = 2 * chip
        near_base = lax.dynamic_slice(recv_off, (near,), (2,))
        near_len = lax.dynamic_slice(recv_len, (near,), (2,))
        near_src = fo + lax.dynamic_slice(so, (0, me), (2, 1))[:, 0]
        rpos, _ = pieces(u, near_base, near_len, near_src)
        my_row = lax.dynamic_slice(in_row, (core,), (1,))[0]
        my_len = lax.dynamic_slice(in_len, (core,), (1,))[0]
        my_base = lax.dynamic_slice(in_base, (core,), (1,))[0]
        spos = stream_row(jnp.clip(my_base + u - my_row, 0, 2 * cap - 1))
        q = jnp.arange(n_tok, dtype=i32)
        out_len = jnp.sum(far_len, axis=0)
        far_base = jnp.where(core == 0, 0, far_len[0]) + jnp.where(chip == 0, 0, cap - out_len) + half_of
        my_far_off = lax.dynamic_slice(send_off, (far,), (2,))
        my_far_len = lax.dynamic_slice(send_len, (far,), (2,))
        my_near_off = lax.dynamic_slice(send_off, (near,), (2,))
        my_near_len = lax.dynamic_slice(send_len, (near,), (2,))
        far_pos, is_far = pieces(q, my_far_off, my_far_len, far_base)
        near_pos, is_near = pieces(q, my_near_off, my_near_len, half_of + lax.dynamic_slice(ro, (0, me), (2, 1))[:, 0])
        ridx = jnp.where(is_far, 2 * cap + far_pos, jnp.where(is_near, near_pos, 4 * cap))
        perm = jnp.concatenate([tok_perm, sib_perm + n_tok])
        cnt = jnp.stack([units, my_row, my_len])

        rows_bf = jax.ShapeDtypeStruct((cap, dim), hidden.dtype)
        stream, rloc = local_call(pick_kernel, [rows_bf, rows_bf], 4, 0, 2, 2 * n_tok, cap, dim, "pick")(cnt, perm, upos, rpos, hidden, sib_hidden)
        arrived = exchange(stream, units, 1)
        dest_rows = local_call(place_kernel, rows_bf, 2, 1, 1, 2 * cap, cap, dim, "place")(cnt, spos, rloc, arrived)
        z = attention(dest_rows, recv_pos, g_attn, w_q, w_k, w_v, w_o)
        branches = [functools.partial(mlp, n_send=n) for n in SENDS]
        longest = jnp.maximum(jnp.max(out_len), jnp.max(in_len))
        pick_branch = sum((longest > n * GROUP).astype(i32) for n in SENDS[:-1])
        done, sib_done, returned = lax.switch(pick_branch, branches, z, g_mlp, w_gate, w_up, w_down)
        return local_call(back_place_kernel, jax.ShapeDtypeStruct((n_tok, dim), hidden.dtype), 3, 0, 3, 4 * cap + 8, n_tok, dim, "back_place")(cnt, tok_perm, ridx, done, sib_done, returned)

    return jax.shard_map(per_device, mesh=mesh, in_specs=(row_spec,) + (vec_spec,) * 7 + (rep_spec,) * 9, out_specs=row_spec, check_vma=False)
```

```python
import functools

import jax
import jax.numpy as jnp
from jax import lax
from jax.experimental import pallas as pl
from jax.experimental.pallas import tpu as pltpu
from jax.sharding import PartitionSpec as P

ROPE_BASE = 500000.0
NORM_EPS = 1e-5
ROWS = 512
QB = 256
FT = 256


def norm_rows(rows_f, gain):
    inv = lax.rsqrt(jnp.mean(rows_f * rows_f, axis=-1, keepdims=True) + NORM_EPS)
    return (rows_f * inv * gain).astype(jnp.bfloat16)


def rope_pair(x, cos_t, sin_t, first_half):
    swapped = jnp.where(first_half, pltpu.roll(x, 96, 1), pltpu.roll(x, 32, 1))
    return x * cos_t + swapped * sin_t


def dot_t(a, b):
    return lax.dot_general(a, b, (((1,), (1,)), ((), ())), preferred_element_type=jnp.float32)


def dot_n(a, b):
    return jnp.dot(a, b, preferred_element_type=jnp.float32)


def attn_kernel(span_ref, outgo, rloc_ref, start_ref, cos_ref, sin_ref, ga_ref, wq_h, wk_h, wv_h, wo_h, out_ref,
                rbuf, q_s, k_s, v_s, o_s, wq_s, wk_s, wv_s, wo_s, sems, ps, pr):
    n_rows, dim = rloc_ref.shape
    n_pairs = dim // 128
    n_blk = n_rows // QB
    peer = lax.rem(lax.axis_index("sp") + 2, 4)
    loads = [pltpu.make_async_copy(a, b, sems.at[i]) for i, (a, b) in enumerate(
        [(wq_h, wq_s), (wk_h, wk_s), (wv_h, wv_s), (wo_h, wo_s)])]
    for c in loads:
        c.start()
    meet([peer])
    moves = []
    for c in range(n_blk):
        rows = pl.ds(c * QB, QB)
        moves.append(push(outgo.at[rows], rbuf.at[rows], ps.at[c], pr.at[c], peer))
        moves[-1].start()
    gain = ga_ref[...].astype(jnp.float32)
    first, last = span_ref[0], span_ref[1]
    for c in loads:
        c.wait()

    for c in range(n_blk):
        length = (c + 1) * QB
        rows = slice(c * QB, (c + 1) * QB)
        lane = lax.broadcasted_iota(jnp.int32, (QB, 128), 1)
        first_half = lane % 64 < 32
        low = lane < 64
        moves[c].wait_recv()
        where_row = c * QB + lax.broadcasted_iota(jnp.int32, (QB, dim), 0)
        arrived = (where_row >= first) & (where_row < last)
        r = jnp.where(arrived, rbuf[rows, :].astype(jnp.float32), rloc_ref[rows, :].astype(jnp.float32))
        h = norm_rows(r, gain)
        cos_t = cos_ref[rows, :]
        sin_t = sin_ref[rows, :]
        q = dot_t(h, wq_s[...])
        for p in range(n_pairs):
            qp = rope_pair(q[:, 128 * p:128 * (p + 1)], cos_t, sin_t, first_half)
            q_s[p] = (qp.astype(jnp.bfloat16) * 0.125).astype(jnp.bfloat16)
        k = rope_pair(dot_t(h, wk_s[...]), cos_t, sin_t, first_half)
        v = dot_t(h, wv_s[...])
        for s, x in ((k_s, k), (v_s, v)):
            other = pltpu.roll(x, 64, 1)
            s[0, rows, :] = jnp.where(low, x, other).astype(jnp.bfloat16)
            s[1, rows, :] = jnp.where(low, other, x).astype(jnp.bfloat16)

        start = start_ref[rows, :]
        row = c * QB + lax.broadcasted_iota(jnp.int32, (QB, length), 0)
        col = lax.broadcasted_iota(jnp.int32, (QB, length), 1)

        @pl.loop(0, n_pairs)
        def _pair(p):
            outs = []
            qp = q_s[p]
            for half in range(2):
                g = (2 * p + half) // 7
                qh = jnp.where(low if half == 0 else ~low, qp, jnp.zeros_like(qp))
                s = dot_t(qh, k_s[g, :length, :])
                s = jnp.where((col >= start) & (col <= row), s, -1e30)
                top = jnp.max(s, axis=1, keepdims=True)
                e = jnp.exp(s - top)
                total = jnp.sum(e, axis=1, keepdims=True)
                outs.append(dot_n(e.astype(jnp.bfloat16), v_s[g, :length, :]) / total)
            o_s[:, pl.ds(pl.multiple_of(p * 128, 128), 128)] = jnp.where(low, outs[0], outs[1]).astype(jnp.bfloat16)

        attn = dot_n(o_s[...], wo_s[...]).astype(jnp.bfloat16)
        r = jnp.where(arrived, rbuf[rows, :].astype(jnp.float32), rloc_ref[rows, :].astype(jnp.float32))
        out_ref[rows, :] = (r + attn.astype(jnp.float32)).astype(jnp.bfloat16)

    for c in range(n_blk):
        moves[c].wait_send()


def attention(span, outgo, rloc, positions, g_attn, w_q, w_k, w_v, w_o):
    n_rows, dim = rloc.shape
    head_dim = w_q.shape[2]
    half_dim = head_dim // 2
    inv_freq = jnp.power(jnp.float32(ROPE_BASE), -2.0 * jnp.arange(half_dim, dtype=jnp.float32) / head_dim)
    angles = positions.astype(jnp.float32)[:, None] * inv_freq[None, :]
    cos_t = jnp.cos(angles)
    sin_t = jnp.sin(angles)
    cos_t = jnp.concatenate([cos_t, cos_t, cos_t, cos_t], axis=1)
    sin_t = jnp.concatenate([-sin_t, sin_t, -sin_t, sin_t], axis=1)
    start = jnp.arange(n_rows, dtype=jnp.int32) - positions
    wq_t = jnp.transpose(w_q, (1, 2, 0)).reshape(dim, dim)
    wk_t = jnp.transpose(w_k, (1, 2, 0)).reshape(128, dim)
    wv_t = jnp.transpose(w_v, (1, 2, 0)).reshape(128, dim)
    wo_t = w_o.reshape(dim, dim)
    bf = jnp.bfloat16
    n_blk = n_rows // QB
    return pl.pallas_call(
        attn_kernel,
        out_shape=jax.ShapeDtypeStruct((n_rows, dim), bf),
        in_specs=[SM, ANY] + [VM] * 5 + [ANY] * 4,
        out_specs=VM,
        scratch_shapes=[
            pltpu.VMEM((n_rows, dim), bf), pltpu.VMEM((dim // 128, QB, 128), bf), pltpu.VMEM((2, n_rows, 128), bf), pltpu.VMEM((2, n_rows, 128), bf),
            pltpu.VMEM((QB, dim), bf),
            pltpu.VMEM((dim, dim), bf), pltpu.VMEM((128, dim), bf), pltpu.VMEM((128, dim), bf), pltpu.VMEM((dim, dim), bf),
            pltpu.SemaphoreType.DMA((4,)), pltpu.SemaphoreType.DMA((n_blk,)), pltpu.SemaphoreType.DMA((n_blk,))],
        compiler_params=pltpu.CompilerParams(collective_id=1, has_side_effects=True, vmem_limit_bytes=66000000),
        name="attention",
    )(span, outgo, rloc, start[:, None], cos_t, sin_t, g_attn[None, :], wq_t, wk_t, wv_t, wo_t)


CHUNK = 128
MESH_ID = pl.DeviceIdType.MESH
ANY = pl.BlockSpec(memory_space=pl.ANY)
VM = pl.BlockSpec(memory_space=pltpu.VMEM)
SM = pl.BlockSpec(memory_space=pltpu.SMEM)


def meet(devices):
    barrier = pltpu.get_barrier_semaphore()
    for dev in devices:
        pl.semaphore_signal(barrier, inc=1, device_id={"sp": dev}, device_id_type=MESH_ID)
    pl.semaphore_wait(barrier, len(devices))


def push(src, dst, send_sem, recv_sem, dev):
    return pltpu.make_async_remote_copy(src_ref=src, dst_ref=dst, send_sem=send_sem, recv_sem=recv_sem,
                                        device_id={"sp": dev}, device_id_type=MESH_ID)


def share_kernel(n_split, *refs):
    n = (len(refs) - 2) // 2
    ins, outs, send_sems, recv_sems = refs[:n], refs[n:2 * n], refs[-2], refs[-1]
    me = lax.axis_index("sp")
    sib = me + 1 - 2 * lax.rem(me, 2)
    meet([sib])
    copies = []
    for a, b in zip(ins, outs):
        parts = n_split if a.shape[0] % (16 * n_split) == 0 else 1
        step = a.shape[0] // parts
        for p in range(parts):
            rows = pl.ds(p * step, step)
            copies.append((a.at[rows], b.at[rows]))
    started = []
    for i, (a, b) in enumerate(copies):
        cp = push(a, b, send_sems.at[i], recv_sems.at[i], sib)
        cp.start()
        started.append(cp)
    for cp in started:
        cp.wait()


def share(arrays, collective_id):
    return pl.pallas_call(
        functools.partial(share_kernel, 4),
        out_shape=[jax.ShapeDtypeStruct(a.shape, a.dtype) for a in arrays],
        in_specs=[ANY] * len(arrays), out_specs=[ANY] * len(arrays),
        scratch_shapes=[pltpu.SemaphoreType.DMA((8,)), pltpu.SemaphoreType.DMA((8,))],
        compiler_params=pltpu.CompilerParams(collective_id=collective_id, has_side_effects=True),
        name="share",
    )(*arrays)


LOAD = 512


def load_table(parts, tab, stage, sems):
    jobs = []
    for ref, blocks in parts:
        for i in range(ref.shape[0] // LOAD):
            n = len(jobs)
            copy = pltpu.make_async_copy(ref.at[pl.ds(i * LOAD, LOAD)], stage.at[pl.ds(n * LOAD, LOAD)], sems.at[n])
            jobs.append((copy, None if blocks is None else i < blocks))
    for copy, cond in jobs:
        if cond is None:
            copy.start()
        else:
            pl.when(cond)(copy.start)
    for n, (copy, cond) in enumerate(jobs):
        def fill(n=n, copy=copy):
            copy.wait()
            fill_table(stage, n * LOAD, tab, n * LOAD)
        if cond is None:
            fill()
        else:
            pl.when(cond)(fill)


def fill_table(stage, at, tab, base):
    @pl.loop(0, LOAD // 64)
    def _blk(i):
        rows = pl.ds(pl.multiple_of(at + i * 64, 64), 64)
        first = pl.multiple_of((base + i * 64) * 8, 8)
        for j in range(stage.shape[1] // 128):
            tab[pl.ds(first + j, 64, stride=8), :] = stage[rows, 128 * j:128 * (j + 1)].astype(jnp.float32)


UNROLL = 16


def slab(k):
    return pl.ds(pl.multiple_of(k * 8, 8), 8)


def copy_rows(n_rows, move):
    @pl.loop(0, n_rows // UNROLL)
    def _grp(i):
        for k in range(UNROLL):
            move(i * UNROLL + k)


def rows_out(n_rows, src3, dst):
    @pl.loop(0, n_rows // CHUNK)
    def _blk(i):
        rows = pl.ds(pl.multiple_of(i * CHUNK, CHUNK), CHUNK)
        for j in range(dst.shape[1] // 128):
            dst[rows, 128 * j:128 * (j + 1)] = src3[pl.ds(pl.multiple_of(i * CHUNK * 8, 8) + j, CHUNK, stride=8), :].astype(dst.dtype)


def pick_kernel(cnt, perm, opos, rpos, own, sib, outgo, rloc, tab, out3, stage, sems):
    cap = rloc.shape[0]
    load_table([(own, None), (sib, None)], tab, stage, sems)
    for lo, hi, pos, dst in ((cnt[0], cnt[1], opos, outgo), (cnt[2], cnt[3], rpos, rloc)):
        @pl.loop(lo // UNROLL, (hi + UNROLL - 1) // UNROLL)
        def _grp(i, pos=pos):
            for k in range(UNROLL):
                at = i * UNROLL + k
                out3[slab(at), :] = tab[slab(perm[pos[at]]), :]
        rows_out(cap, out3, dst)


def back_place_kernel(perm, ridx, own, sib, stream, out, tab, out3, stage, sems):
    cap = own.shape[0]
    n_tok = out.shape[0]
    load_table([(own, None), (sib, None), (stream, None)], tab, stage, sems)
    tab[slab(4 * cap), :] = jnp.zeros((8, 128), jnp.float32)

    def one(k):
        out3[slab(perm[k]), :] = tab[slab(ridx[k]), :]

    copy_rows(n_tok, one)
    rows_out(n_tok, out3, out)


GROUP = 256
PIECE = 5 * FT


def mlp_kernel(z_ref, gm_ref, wg_h, wu_h, wd_h, own, sib_out, far, obuf, m_s, wg_s, wu_s, wd_s, w_sems, own_sem, ps, pr, ss, sr, fs, fr):
    cap, dim = z_ref.shape
    ff = wg_s.shape[1]
    n_grp = cap // GROUP
    me = lax.axis_index("sp")
    core = lax.rem(me, 2)
    chip = me // 2
    sib = me + 1 - 2 * core
    peer = lax.rem(me + 2, 4)
    piece = [slice(at, min(at + PIECE, ff)) for at in range(0, ff, PIECE)]
    loads = []
    for n, cols in enumerate(piece):
        for x, y in ((wg_h, wg_s), (wu_h, wu_s)):
            loads.append(pltpu.make_async_copy(x.at[:, cols], y.at[:, cols], w_sems.at[len(loads)]))
    loads.append(pltpu.make_async_copy(wd_h, wd_s, w_sems.at[len(loads)]))
    for c in loads:
        c.start()
    meet([sib, peer])
    gain = gm_ref[...].astype(jnp.float32)

    def group_of(i, at_chip):
        return at_chip * i + (1 - at_chip) * (n_grp - 1 - i)

    def rows_at(g):
        return pl.ds(pl.multiple_of(g * GROUP, GROUP), GROUP)

    def to_peer(i):
        rows = rows_at(group_of(i, chip))
        return push(own.at[rows], far.at[rows], ps.at[i], pr.at[i], peer)

    def to_sib(i):
        rows = rows_at(group_of(i, chip))
        return push(own.at[rows], sib_out.at[rows], ss.at[i], sr.at[i], sib)

    def forward(i):
        g = group_of(i, 1 - chip)
        return push(far.at[rows_at(g)], far.at[pl.ds(pl.multiple_of(cap + g * GROUP, GROUP), GROUP)], fs.at[i], fr.at[i], sib)

    def keep(i):
        return pltpu.make_async_copy(obuf.at[lax.rem(i, 2)], own.at[rows_at(group_of(i, chip))], own_sem.at[i])

    def send(i):
        keep(i).wait()
        to_peer(i).start()
        to_sib(i).start()

    def group(i, arriving):
        z = z_ref[rows_at(group_of(i, chip)), :].astype(jnp.float32)
        h = norm_rows(z, gain)
        if not arriving:
            send(i - 1)

            @pl.when(i >= 3)
            def _fwd():
                to_peer(i - 3).wait_recv()
                forward(i - 3).start()

        for t in range(ff // FT):
            cols = slice(t * FT, (t + 1) * FT)
            if arriving and t * FT % PIECE == 0:
                loads[2 * (t * FT // PIECE)].wait()
                loads[2 * (t * FT // PIECE) + 1].wait()
            gate = 0.5 * dot_n(h, wg_s[:, cols])
            up = dot_n(h, wu_s[:, cols])
            m_s[:, cols] = ((gate + gate * jnp.tanh(gate)) * up).astype(jnp.bfloat16)
        if arriving:
            loads[-1].wait()
        down = dot_n(m_s[...], wd_s[...]).astype(jnp.bfloat16)
        obuf[i % 2 if arriving else lax.rem(i, 2)] = (z + down.astype(jnp.float32)).astype(jnp.bfloat16)
        keep(i).start()

    group(0, True)

    @pl.loop(1, n_grp)
    def _group(i):
        group(i, False)

    send(n_grp - 1)
    for i in range(n_grp - 3, n_grp):
        to_peer(i).wait_recv()
        forward(i).start()
    for i in range(n_grp):
        to_sib(i).wait()
        to_peer(i).wait_send()
        forward(i).wait()


def mlp(z, g_mlp, w_gate, w_up, w_down):
    cap, dim = z.shape
    ff = w_gate.shape[1]
    bf = jnp.bfloat16
    n_grp = cap // GROUP
    dma = pltpu.SemaphoreType.DMA
    rows = jax.ShapeDtypeStruct((cap, dim), bf)
    return pl.pallas_call(
        mlp_kernel,
        out_shape=[rows, rows, jax.ShapeDtypeStruct((2 * cap, dim), bf)],
        in_specs=[VM, VM, ANY, ANY, ANY], out_specs=[ANY] * 3,
        scratch_shapes=[
            pltpu.VMEM((2, GROUP, dim), bf), pltpu.VMEM((GROUP, ff), bf),
            pltpu.VMEM((dim, ff), bf), pltpu.VMEM((dim, ff), bf), pltpu.VMEM((ff, dim), bf),
            dma((2 * -(-ff // PIECE) + 1,))] + [dma((n_grp,))] * 7,
        compiler_params=pltpu.CompilerParams(collective_id=2, has_side_effects=True, vmem_limit_bytes=66000000),
        name="mlp",
    )(z, g_mlp[None, :], w_gate, w_up, w_down)


def local_call(body, out_shapes, n_smem, n_vmem, n_any, tab_rows, out_rows, dim, name):
    return pl.pallas_call(
        body,
        out_shape=out_shapes,
        in_specs=[SM] * n_smem + [VM] * n_vmem + [ANY] * n_any,
        out_specs=jax.tree.map(lambda _: VM, out_shapes),
        scratch_shapes=[pltpu.VMEM((tab_rows * 8, 128), jnp.float32), pltpu.VMEM((out_rows * 8, 128), jnp.float32),
                        pltpu.VMEM((tab_rows // LOAD * LOAD, dim), jnp.bfloat16), pltpu.SemaphoreType.DMA((tab_rows // LOAD,))],
        compiler_params=pltpu.CompilerParams(vmem_limit_bytes=66000000),
        name=name,
    )


def solution(mesh):
    row_spec = P(('dp', 'sp'), None)
    vec_spec = P(('dp', 'sp'))
    rep_spec = P()

    def per_device(hidden, tok_perm, send_off, send_len, recv_off, recv_len, recv_doc, recv_pos, g_attn, w_q, w_k, w_v, w_o, g_mlp, w_gate, w_up, w_down):
        n_tok, dim = hidden.shape
        cap = recv_doc.shape[0]
        i32 = jnp.int32
        me = lax.axis_index('sp')
        core = me % 2
        chip = me // 2
        plan = jnp.concatenate([tok_perm, send_off, send_len, recv_off, recv_len, jnp.zeros((1024 - 16,), i32)]).reshape(-1, 128)
        sib_hidden, sib_plan = share([hidden, plan], 0)
        sib_plan = sib_plan.reshape(-1)
        sib_perm = sib_plan[:n_tok]

        def both(own, at):
            other = lax.slice(sib_plan, (n_tok + at,), (n_tok + at + 4,))
            return jnp.where(core == 0, jnp.stack([own, other]), jnp.stack([other, own]))

        so, sl, ro, rl = both(send_off, 0), both(send_len, 4), both(recv_off, 8), both(recv_len, 12)
        far = 2 * (1 - chip)
        cores = jnp.arange(2, dtype=i32)
        fo = jnp.where(cores == core, 0, n_tok)
        half_of = jnp.where(cores == core, 0, cap)
        far_len = lax.dynamic_slice(sl, (0, far), (2, 2))
        far_off = lax.dynamic_slice(so, (0, far), (2, 2))
        out_len = jnp.sum(far_len, axis=0)
        in_len = jnp.sum(lax.dynamic_slice(recv_len, (far,), (2,)))
        far_row = jnp.where(chip == 0, 0, cap - out_len)
        u = jnp.arange(cap, dtype=i32)

        def pieces(x, base, length, src):
            inside = (x[:, None] >= base[None, :]) & (x[:, None] < (base + length)[None, :])
            return jnp.sum(jnp.where(inside, x[:, None] - base[None, :] + src[None, :], 0), axis=1), jnp.any(inside, axis=1)

        def column(x, at):
            return lax.dynamic_slice(x, (0, at), (2, 1))[:, 0]

        to_len = column(far_len, core)
        to_row = lax.dynamic_slice(far_row, (core,), (1,))[0]
        to_base = to_row + jnp.stack([jnp.zeros((), i32), to_len[0]])
        opos, _ = pieces(u, to_base, to_len, fo + column(far_off, core))
        near = 2 * chip
        near_base = lax.dynamic_slice(recv_off, (near,), (2,))
        near_len = lax.dynamic_slice(recv_len, (near,), (2,))
        rpos, _ = pieces(u, near_base, near_len, fo + column(so, me))
        in_row = jnp.where(chip == 0, cap - in_len, 0)
        near_row = jnp.where(chip == 0, 0, in_len)
        q = jnp.arange(n_tok, dtype=i32)
        far_base = jnp.where(core == 0, 0, far_len[0]) + far_row + half_of
        my_far_off = lax.dynamic_slice(send_off, (far,), (2,))
        my_far_len = lax.dynamic_slice(send_len, (far,), (2,))
        my_near_off = lax.dynamic_slice(send_off, (near,), (2,))
        my_near_len = lax.dynamic_slice(send_len, (near,), (2,))
        far_pos, is_far = pieces(q, my_far_off, my_far_len, far_base)
        near_pos, is_near = pieces(q, my_near_off, my_near_len, half_of + lax.dynamic_slice(ro, (0, me), (2, 1))[:, 0])
        ridx = jnp.where(is_far, 2 * cap + far_pos, jnp.where(is_near, near_pos, 4 * cap))
        perm = jnp.concatenate([tok_perm, sib_perm + n_tok])
        cnt = jnp.stack([to_row, to_row + jnp.sum(to_len), near_row, near_row + cap - in_len])
        span = jnp.stack([in_row, in_row + in_len])

        rows_bf = jax.ShapeDtypeStruct((cap, dim), hidden.dtype)
        outgo, rloc = local_call(pick_kernel, [rows_bf, rows_bf], 4, 0, 2, 2 * n_tok, cap, dim, "pick")(cnt, perm, opos, rpos, hidden, sib_hidden)
        z = attention(span, outgo, rloc, recv_pos, g_attn, w_q, w_k, w_v, w_o)
        done, sib_done, returned = mlp(z, g_mlp, w_gate, w_up, w_down)
        return local_call(back_place_kernel, jax.ShapeDtypeStruct((n_tok, dim), hidden.dtype), 2, 0, 3, 4 * cap + 8, n_tok, dim, "back_place")(tok_perm, ridx, done, sib_done, returned)

    return jax.shard_map(per_device, mesh=mesh, in_specs=(row_spec,) + (vec_spec,) * 7 + (rep_spec,) * 9, out_specs=row_spec, check_vma=False)
```

```python
import functools

import jax
import jax.numpy as jnp
import numpy as np
from jax import lax
from jax.experimental import pallas as pl
from jax.experimental.pallas import tpu as pltpu
from jax.sharding import PartitionSpec as P

ROPE_BASE = 500000.0
NORM_EPS = 1e-5
ROWS = 512
QB = 256
FT = 256


def norm_rows(rows_f, gain):
    inv = lax.rsqrt(jnp.mean(rows_f * rows_f, axis=-1, keepdims=True) + NORM_EPS)
    return (rows_f * inv * gain).astype(jnp.bfloat16)


def rope_pair(x, cos_t, sin_t, first_half):
    swapped = jnp.where(first_half, pltpu.roll(x, 96, 1), pltpu.roll(x, 32, 1))
    return x * cos_t + swapped * sin_t


def dot_t(a, b):
    return lax.dot_general(a, b, (((1,), (1,)), ((), ())), preferred_element_type=jnp.float32)


def dot_n(a, b):
    return jnp.dot(a, b, preferred_element_type=jnp.float32)


def attn_kernel(span_ref, outgo, rloc_ref, pos_ref, freq_ref, ga_ref, wq_h, wk_h, wv_h, wo_h, out_ref,
                rbuf, q_s, k_s, v_s, o_s, sa, sb, bias, cos_s, sin_s, start_s, wq_s, wk_s, wv_s, wo_s, sems, ps, pr):
    n_rows, dim = rloc_ref.shape
    n_pairs = dim // 128
    n_blk = n_rows // QB
    peer = lax.rem(lax.axis_index("sp") + 2, 4)
    loads = [pltpu.make_async_copy(a, b, sems.at[i]) for i, (a, b) in enumerate(
        [(wq_h, wq_s), (wk_h, wk_s), (wv_h, wv_s), (wo_h, wo_s)])]
    for c in loads:
        c.start()
    meet([peer])
    moves = []
    for c in range(n_blk):
        rows = pl.ds(c * QB, QB)
        moves.append(push(outgo.at[rows], rbuf.at[rows], ps.at[c], pr.at[c], peer))
        moves[-1].start()
    gain = ga_ref[...].astype(jnp.float32).reshape(1, dim)
    first, last = span_ref[0], span_ref[1]
    tile_lane = lax.broadcasted_iota(jnp.int32, (128, 128), 1)
    tile_row = lax.broadcasted_iota(jnp.int32, (128, 128), 0)
    sign = jnp.where(tile_lane % 64 < 32, -1.0, 1.0)
    for t in range(n_rows // 128):
        rows = slice(128 * t, 128 * (t + 1))
        pos = jnp.transpose(jnp.broadcast_to(pos_ref[t:t + 1, :].astype(jnp.float32), (128, 128)))
        angle = pos * freq_ref[...]
        cos_s[rows, :] = jnp.cos(angle)
        sin_s[rows, :] = jnp.sin(angle) * sign
        start_s[rows, :] = 128 * t + tile_row - pos.astype(jnp.int32)
    for c in loads:
        c.wait()

    lane = lax.broadcasted_iota(jnp.int32, (QB, 128), 1)
    first_half = lane % 64 < 32
    low = lane < 64

    for c in range(n_blk):
        length = (c + 1) * QB
        rows = slice(c * QB, (c + 1) * QB)
        start = start_s[rows, :]
        row = c * QB + lax.broadcasted_iota(jnp.int32, (QB, 128), 0)
        for t in range(length // 128):
            col = 128 * t + lane
            bias[:, 128 * t:128 * (t + 1)] = jnp.where((col >= start) & (col <= row), 3e38, -1e30)
        moves[c].wait_recv()
        where_row = c * QB + lax.broadcasted_iota(jnp.int32, (QB, dim), 0)
        arrived = (where_row >= first) & (where_row < last)
        r = jnp.where(arrived, rbuf[rows, :].astype(jnp.float32), rloc_ref[rows, :].astype(jnp.float32))
        h = norm_rows(r, gain)
        cos_t = cos_s[rows, :]
        sin_t = sin_s[rows, :]
        q = dot_t(h, wq_s[...])
        for p in range(n_pairs):
            qp = rope_pair(q[:, 128 * p:128 * (p + 1)], cos_t, sin_t, first_half)
            q_s[p] = (qp.astype(jnp.bfloat16) * 0.125).astype(jnp.bfloat16)
        k = rope_pair(dot_t(h, wk_s[...]), cos_t, sin_t, first_half)
        v = dot_t(h, wv_s[...])
        for s, x in ((k_s, k), (v_s, v)):
            other = pltpu.roll(x, 64, 1)
            s[0, rows, :] = jnp.where(low, x, other).astype(jnp.bfloat16)
            s[1, rows, :] = jnp.where(low, other, x).astype(jnp.bfloat16)

        def scores(p, half, dst):
            qp = q_s[p]
            qh = jnp.where(low if half == 0 else ~low, qp, jnp.zeros_like(qp))
            s = jnp.minimum(dot_t(qh, k_s[(2 * p + half) // 7, :length, :]), bias[:, :length])
            dst[:, :length] = s
            return jnp.max(s, axis=1, keepdims=True)

        def soft(p, half, src, top):
            e = jnp.exp(src[:, :length] - top)
            total = jnp.sum(e, axis=1, keepdims=True)
            return dot_n(e.astype(jnp.bfloat16), v_s[(2 * p + half) // 7, :length, :]) / total

        def pair(p, top_a):
            top_b = scores(p, 1, sb)
            out_a = soft(p, 0, sa, top_a)
            top_a = scores(jnp.minimum(p + 1, n_pairs - 1), 0, sa)
            out_b = soft(p, 1, sb, top_b)
            o_s[:, pl.ds(pl.multiple_of(p * 128, 128), 128)] = jnp.where(low, out_a, out_b).astype(jnp.bfloat16)
            return top_a

        lax.fori_loop(0, n_pairs, pair, scores(0, 0, sa))

        attn = dot_n(o_s[...], wo_s[...]).astype(jnp.bfloat16)
        r = jnp.where(arrived, rbuf[rows, :].astype(jnp.float32), rloc_ref[rows, :].astype(jnp.float32))
        out_ref[rows, :] = (r + attn.astype(jnp.float32)).astype(jnp.bfloat16)

    for c in range(n_blk):
        moves[c].wait_send()


def attention(span, outgo, rloc, positions, g_attn, w_q, w_k, w_v, w_o):
    n_rows, dim = rloc.shape
    head_dim = w_q.shape[2]
    half_dim = head_dim // 2
    exponent = -2.0 * np.arange(half_dim, dtype=np.float32) / np.float32(head_dim)
    inv_freq = np.power(np.float32(ROPE_BASE), exponent).astype(np.float32)
    freq = jnp.asarray(np.tile(inv_freq, 128 // half_dim)[None, :])
    wq_t = jnp.transpose(w_q, (1, 2, 0)).reshape(dim, dim)
    wk_t = jnp.transpose(w_k, (1, 2, 0)).reshape(128, dim)
    wv_t = jnp.transpose(w_v, (1, 2, 0)).reshape(128, dim)
    wo_t = w_o.reshape(dim, dim)
    bf = jnp.bfloat16
    n_blk = n_rows // QB
    return pl.pallas_call(
        attn_kernel,
        out_shape=jax.ShapeDtypeStruct((n_rows, dim), bf),
        in_specs=[SM, ANY] + [VM] * 4 + [ANY] * 4,
        out_specs=VM,
        scratch_shapes=[
            pltpu.VMEM((n_rows, dim), bf), pltpu.VMEM((dim // 128, QB, 128), bf), pltpu.VMEM((2, n_rows, 128), bf), pltpu.VMEM((2, n_rows, 128), bf),
            pltpu.VMEM((QB, dim), bf),
            pltpu.VMEM((QB, n_rows), jnp.float32), pltpu.VMEM((QB, n_rows), jnp.float32), pltpu.VMEM((QB, n_rows), jnp.float32),
            pltpu.VMEM((n_rows, 128), jnp.float32), pltpu.VMEM((n_rows, 128), jnp.float32), pltpu.VMEM((n_rows, 128), jnp.int32),
            pltpu.VMEM((dim, dim), bf), pltpu.VMEM((128, dim), bf), pltpu.VMEM((128, dim), bf), pltpu.VMEM((dim, dim), bf),
            pltpu.SemaphoreType.DMA((4,)), pltpu.SemaphoreType.DMA((n_blk,)), pltpu.SemaphoreType.DMA((n_blk,))],
        compiler_params=pltpu.CompilerParams(collective_id=1, has_side_effects=True, vmem_limit_bytes=66000000),
        name="attention",
    )(span, outgo, rloc, positions.reshape(-1, 128), freq, g_attn, wq_t, wk_t, wv_t, wo_t)


CHUNK = 128
MESH_ID = pl.DeviceIdType.MESH
ANY = pl.BlockSpec(memory_space=pl.ANY)
VM = pl.BlockSpec(memory_space=pltpu.VMEM)
SM = pl.BlockSpec(memory_space=pltpu.SMEM)


def meet(devices):
    barrier = pltpu.get_barrier_semaphore()
    for dev in devices:
        pl.semaphore_signal(barrier, inc=1, device_id={"sp": dev}, device_id_type=MESH_ID)
    pl.semaphore_wait(barrier, len(devices))


def push(src, dst, send_sem, recv_sem, dev):
    return pltpu.make_async_remote_copy(src_ref=src, dst_ref=dst, send_sem=send_sem, recv_sem=recv_sem,
                                        device_id={"sp": dev}, device_id_type=MESH_ID)


def share_kernel(n_split, *refs):
    n = (len(refs) - 2) // 2
    ins, outs, send_sems, recv_sems = refs[:n], refs[n:2 * n], refs[-2], refs[-1]
    me = lax.axis_index("sp")
    sib = me + 1 - 2 * lax.rem(me, 2)
    meet([sib])
    copies = []
    for a, b in zip(ins, outs):
        parts = n_split if a.ndim == 2 else 1
        step = a.shape[0] // parts
        for p in range(parts):
            rows = pl.ds(p * step, step)
            copies.append((a.at[rows], b.at[rows]) if parts > 1 else (a, b))
    started = []
    for i, (a, b) in enumerate(copies):
        cp = push(a, b, send_sems.at[i], recv_sems.at[i], sib)
        cp.start()
        started.append(cp)
    for cp in started:
        cp.wait()


def share(arrays, collective_id):
    return pl.pallas_call(
        functools.partial(share_kernel, 4),
        out_shape=[jax.ShapeDtypeStruct(a.shape, a.dtype) for a in arrays],
        in_specs=[ANY] * len(arrays), out_specs=[ANY] * len(arrays),
        scratch_shapes=[pltpu.SemaphoreType.DMA((16,)), pltpu.SemaphoreType.DMA((16,))],
        compiler_params=pltpu.CompilerParams(collective_id=collective_id, has_side_effects=True),
        name="share",
    )(*arrays)


LOAD = 512


def load_table(parts, tab, stage, sems):
    jobs = []
    for ref, blocks in parts:
        for i in range(ref.shape[0] // LOAD):
            n = len(jobs)
            copy = pltpu.make_async_copy(ref.at[pl.ds(i * LOAD, LOAD)], stage.at[pl.ds(n * LOAD, LOAD)], sems.at[n])
            jobs.append((copy, None if blocks is None else i < blocks))
    for copy, cond in jobs:
        if cond is None:
            copy.start()
        else:
            pl.when(cond)(copy.start)
    for n, (copy, cond) in enumerate(jobs):
        def fill(n=n, copy=copy):
            copy.wait()
            fill_table(stage, n * LOAD, tab, n * LOAD)
        if cond is None:
            fill()
        else:
            pl.when(cond)(fill)


def fill_table(stage, at, tab, base):
    @pl.loop(0, LOAD // 64)
    def _blk(i):
        rows = pl.ds(pl.multiple_of(at + i * 64, 64), 64)
        first = pl.multiple_of((base + i * 64) * 8, 8)
        for j in range(stage.shape[1] // 128):
            tab[pl.ds(first + j, 64, stride=8), :] = stage[rows, 128 * j:128 * (j + 1)].astype(jnp.float32)


UNROLL = 16


def slab(k):
    return pl.ds(pl.multiple_of(k * 8, 8), 8)


def copy_rows(n_rows, move):
    @pl.loop(0, n_rows // UNROLL)
    def _grp(i):
        for k in range(UNROLL):
            move(i * UNROLL + k)


def rows_out(n_rows, src3, dst):
    @pl.loop(0, n_rows // CHUNK)
    def _blk(i):
        rows = pl.ds(pl.multiple_of(i * CHUNK, CHUNK), CHUNK)
        for j in range(dst.shape[1] // 128):
            dst[rows, 128 * j:128 * (j + 1)] = src3[pl.ds(pl.multiple_of(i * CHUNK * 8, 8) + j, CHUNK, stride=8), :].astype(dst.dtype)


def move_run(n, one):
    whole = n // UNROLL

    @pl.loop(0, whole)
    def _grp(i):
        for k in range(UNROLL):
            one(i * UNROLL + k)

    @pl.loop(whole * UNROLL, n)
    def _one(i):
        one(i)


def pick_kernel(perm, so, sl, ro, rl, perm_b, so_b, sl_b, ro_b, rl_b, own, sib, outgo, rloc, span, tab, out3, stage, sems):
    cap = rloc.shape[0]
    n_tok = own.shape[0]
    me = lax.axis_index("sp")
    core = lax.rem(me, 2)
    chip = me // 2
    mate = me + 1 - 2 * core
    near, far = 2 * chip, 2 * (1 - chip)
    load_table([(own, None), (sib, None)], tab, stage, sems)
    n_in = rl[far] + rl[far + 1]
    span[0] = (1 - chip) * (cap - n_in)
    span[1] = (1 - chip) * (cap - n_in) + n_in

    def run(dst_row, src, table_row, at, n):
        def one(t):
            out3[slab(dst_row + t), :] = tab[slab(table_row + src[at + t]), :]
        move_run(n, one)

    goal = far + core
    row = chip * (cap - sl[goal] - sl_b[goal])
    run(row + core * sl_b[goal], perm, 0, so[goal], sl[goal])
    run(row + (1 - core) * sl[goal], perm_b, n_tok, so_b[goal], sl_b[goal])
    rows_out(cap, out3, outgo)
    run(ro[me], perm, 0, so[me], sl[me])
    run(ro[mate], perm_b, n_tok, so_b[me], sl_b[me])
    rows_out(cap, out3, rloc)


def back_place_kernel(perm, so, sl, ro, rl, perm_b, so_b, sl_b, ro_b, rl_b, own, sib, stream, out, tab, out3, stage, sems):
    cap = own.shape[0]
    n_tok = out.shape[0]
    me = lax.axis_index("sp")
    core = lax.rem(me, 2)
    chip = me // 2
    mate = me + 1 - 2 * core
    far = 2 * (1 - chip)
    load_table([(own, None), (sib, None), (stream, None)], tab, stage, sems)

    def run(goal, row):
        def one(t):
            out3[slab(perm[so[goal] + t]), :] = tab[slab(row + t), :]
        move_run(sl[goal], one)

    run(me, ro[me])
    run(mate, cap + ro_b[me])
    for goal, base in ((far + core, 2 * cap), (far + 1 - core, 3 * cap)):
        run(goal, base + chip * (cap - sl[goal] - sl_b[goal]) + core * sl_b[goal])
    sent = so[3] + sl[3]

    def blank(t):
        out3[slab(perm[sent + t]), :] = jnp.zeros((8, 128), jnp.float32)

    move_run(n_tok - sent, blank)
    rows_out(n_tok, out3, out)


GROUP = 256
END = 128
PIECE = 5 * FT


def mlp_kernel(z_ref, gm_ref, wg_h, wu_h, wd_h, own, sib_out, far, obuf, m_s, wg_s, wu_s, wd_s, w_sems, own_sem, ps, pr, ss, sr, fs, fr):
    cap, dim = z_ref.shape
    ff = wg_s.shape[1]
    n_grp = (cap - 2 * END) // GROUP + 2
    ENDS = (0, n_grp - 1)
    me = lax.axis_index("sp")
    core = lax.rem(me, 2)
    chip = me // 2
    sib = me + 1 - 2 * core
    peer = lax.rem(me + 2, 4)
    piece = [slice(at, min(at + PIECE, ff)) for at in range(0, ff, PIECE)]
    loads = []
    for n, cols in enumerate(piece):
        for x, y in ((wg_h, wg_s), (wu_h, wu_s)):
            loads.append(pltpu.make_async_copy(x.at[:, cols], y.at[:, cols], w_sems.at[len(loads)]))
    loads.append(pltpu.make_async_copy(wd_h, wd_s, w_sems.at[len(loads)]))
    for c in loads:
        c.start()
    meet([sib, peer])
    gain = gm_ref[...].astype(jnp.float32).reshape(1, dim)

    def rows_of(i, at_chip):
        size = END if isinstance(i, int) and i in ENDS else GROUP
        at = 0 if isinstance(i, int) and i == 0 else END + GROUP * (i - 1)
        return pl.ds(pl.multiple_of(at_chip * at + (1 - at_chip) * (cap - size - at), END), size)

    def to_peer(i):
        rows = rows_of(i, chip)
        return push(own.at[rows], far.at[rows], ps.at[i], pr.at[i], peer)

    def to_sib(i):
        rows = rows_of(i, chip)
        return push(own.at[rows], sib_out.at[rows], ss.at[i], sr.at[i], sib)

    def forward(i):
        rows = rows_of(i, 1 - chip)
        return push(far.at[rows], far.at[pl.ds(pl.multiple_of(cap + rows.start, END), rows.size)], fs.at[i], fr.at[i], sib)

    def keep(i):
        rows = rows_of(i, chip)
        return pltpu.make_async_copy(obuf.at[lax.rem(i, 2), pl.ds(0, rows.size)], own.at[rows], own_sem.at[i])

    def send(i):
        keep(i).wait()
        to_peer(i).start()
        to_sib(i).start()

    def relay(i):
        to_peer(i).wait_recv()
        forward(i).start()

    def group(i, arriving, before):
        rows = rows_of(i, chip)
        z = z_ref[rows, :].astype(jnp.float32)
        h = norm_rows(z, gain)
        before()
        mid = pl.ds(0, rows.size)
        for t in range(ff // FT):
            cols = slice(t * FT, (t + 1) * FT)
            if arriving and t * FT % PIECE == 0:
                loads[2 * (t * FT // PIECE)].wait()
                loads[2 * (t * FT // PIECE) + 1].wait()
            gate = 0.5 * dot_n(h, wg_s[:, cols])
            up = dot_n(h, wu_s[:, cols])
            m_s[mid, cols] = ((gate + gate * jnp.tanh(gate)) * up).astype(jnp.bfloat16)
        if arriving:
            loads[-1].wait()
        down = dot_n(m_s[mid, :], wd_s[...]).astype(jnp.bfloat16)
        obuf[lax.rem(i, 2), mid, :] = (z + down.astype(jnp.float32)).astype(jnp.bfloat16)
        keep(i).start()

    last = n_grp - 1
    group(0, True, lambda: None)
    group(1, False, lambda: send(0))

    @pl.loop(2, last)
    def _group(i):
        def before():
            send(i - 1)

            @pl.when(i >= 4)
            def _fwd():
                relay(i - 3)

        group(i, False, before)

    def ending():
        send(last - 1)
        relay(0)
        relay(last - 3)

    group(last, False, ending)
    send(last)
    for i in range(last - 2, n_grp):
        relay(i)
    for i in range(n_grp):
        to_sib(i).wait()
        to_peer(i).wait_send()
        forward(i).wait()


def mlp(z, g_mlp, w_gate, w_up, w_down):
    cap, dim = z.shape
    ff = w_gate.shape[1]
    bf = jnp.bfloat16
    n_grp = (cap - 2 * END) // GROUP + 2
    dma = pltpu.SemaphoreType.DMA
    rows = jax.ShapeDtypeStruct((cap, dim), bf)
    return pl.pallas_call(
        mlp_kernel,
        out_shape=[rows, rows, jax.ShapeDtypeStruct((2 * cap, dim), bf)],
        in_specs=[VM, VM, ANY, ANY, ANY], out_specs=[ANY] * 3,
        scratch_shapes=[
            pltpu.VMEM((2, GROUP, dim), bf), pltpu.VMEM((GROUP, ff), bf),
            pltpu.VMEM((dim, ff), bf), pltpu.VMEM((dim, ff), bf), pltpu.VMEM((ff, dim), bf),
            dma((2 * -(-ff // PIECE) + 1,))] + [dma((n_grp,))] * 7,
        compiler_params=pltpu.CompilerParams(collective_id=2, has_side_effects=True, vmem_limit_bytes=66000000),
        name="mlp",
    )(z, g_mlp, w_gate, w_up, w_down)


def local_call(body, out_shapes, out_specs, n_any, tab_rows, out_rows, dim, name):
    return pl.pallas_call(
        body,
        out_shape=out_shapes,
        in_specs=[SM] * 10 + [ANY] * n_any,
        out_specs=out_specs,
        scratch_shapes=[pltpu.VMEM((tab_rows * 8, 128), jnp.float32), pltpu.VMEM((out_rows * 8, 128), jnp.float32),
                        pltpu.VMEM((tab_rows, dim), jnp.bfloat16), pltpu.SemaphoreType.DMA((tab_rows // LOAD,))],
        compiler_params=pltpu.CompilerParams(vmem_limit_bytes=66000000),
        name=name,
    )


def solution(mesh):
    row_spec = P(('dp', 'sp'), None)
    vec_spec = P(('dp', 'sp'))
    rep_spec = P()

    def per_device(hidden, tok_perm, send_off, send_len, recv_off, recv_len, recv_doc, recv_pos, g_attn, w_q, w_k, w_v, w_o, g_mlp, w_gate, w_up, w_down):
        n_tok, dim = hidden.shape
        cap = recv_doc.shape[0]
        plan = [tok_perm, send_off, send_len, recv_off, recv_len]
        sib_hidden, *sib_plan = share([hidden] + plan, 0)
        rows_bf = jax.ShapeDtypeStruct((cap, dim), hidden.dtype)
        outs = [rows_bf, rows_bf, jax.ShapeDtypeStruct((2,), jnp.int32)]
        outgo, rloc, span = local_call(pick_kernel, outs, [VM, VM, SM], 2, 2 * n_tok, cap, dim, "pick")(*plan, *sib_plan, hidden, sib_hidden)
        z = attention(span, outgo, rloc, recv_pos, g_attn, w_q, w_k, w_v, w_o)
        done, sib_done, returned = mlp(z, g_mlp, w_gate, w_up, w_down)
        out = jax.ShapeDtypeStruct((n_tok, dim), hidden.dtype)
        return local_call(back_place_kernel, out, VM, 3, 4 * cap, n_tok, dim, "back_place")(*plan, *sib_plan, done, sib_done, returned)

    return jax.shard_map(per_device, mesh=mesh, in_specs=(row_spec,) + (vec_spec,) * 7 + (rep_spec,) * 9, out_specs=row_spec, check_vma=False)
```

```python
import functools

import jax
import jax.numpy as jnp
import numpy as np
from jax import lax
from jax.experimental import pallas as pl
from jax.experimental.pallas import tpu as pltpu
from jax.sharding import PartitionSpec as P

ROPE_BASE = 500000.0
NORM_EPS = 1e-5
ROWS = 512
QB = 256
FT = 256


def norm_rows(rows_f, gain):
    inv = lax.rsqrt(jnp.mean(rows_f * rows_f, axis=-1, keepdims=True) + NORM_EPS)
    return (rows_f * inv * gain).astype(jnp.bfloat16)


def rope_pair(x, cos_t, sin_t, first_half):
    swapped = jnp.where(first_half, pltpu.roll(x, 96, 1), pltpu.roll(x, 32, 1))
    return x * cos_t + swapped * sin_t


def dot_t(a, b):
    return lax.dot_general(a, b, (((1,), (1,)), ((), ())), preferred_element_type=jnp.float32)


def dot_n(a, b):
    return jnp.dot(a, b, preferred_element_type=jnp.float32)


def layer_kernel(span_ref, outgo, rloc_ref, pos_ref, freq_ref, ga_ref, gm_ref, wq_h, wk_h, wv_h, wo_h, wg_h, wu_h, wd_h, own, sib_out, far,
                 rbuf, r_s, q_s, k_s, v_s, o_s, m_s, obuf, sa, sb, bias, cos_s, sin_s, start_s, wq_s, wk_s, wv_s, wo_s, wg_s, wu_s, wd_s, sems,
                 as_, ar, ps, pr, ss, sr, fs, fr, own_sem):
    n_rows, dim = rloc_ref.shape
    n_pairs = dim // 128
    n_blk = n_rows // QB
    ff = wg_s.shape[1]
    me = lax.axis_index("sp")
    sib = me + 1 - 2 * lax.rem(me, 2)
    peer = lax.rem(me + 2, 4)
    loads = [pltpu.make_async_copy(a, b, sems.at[i]) for i, (a, b) in enumerate(
        [(wq_h, wq_s), (wk_h, wk_s), (wv_h, wv_s), (wo_h, wo_s), (wg_h, wg_s), (wu_h, wu_s), (wd_h, wd_s)])]
    meet([sib, peer])

    def rows_at(c):
        return pl.ds(pl.multiple_of(c * QB, QB), QB)

    def arrive(c):
        return push(outgo.at[rows_at(c)], rbuf.at[rows_at(c)], as_.at[c], ar.at[c], peer)

    def to_peer(c):
        return push(own.at[rows_at(c)], far.at[rows_at(c)], ps.at[c], pr.at[c], peer)

    def to_sib(c):
        return push(own.at[rows_at(c)], sib_out.at[rows_at(c)], ss.at[c], sr.at[c], sib)

    def forward(c):
        return push(far.at[rows_at(c)], far.at[pl.ds(pl.multiple_of(n_rows + c * QB, QB), QB)], fs.at[c], fr.at[c], sib)

    def keep(c):
        return pltpu.make_async_copy(obuf.at[lax.rem(c, 2)], own.at[rows_at(c)], own_sem.at[c])

    def send(c):
        keep(c).wait()
        to_peer(c).start()
        to_sib(c).start()

    def relay(c):
        to_peer(c).wait_recv()
        forward(c).start()

    for c in range(n_blk):
        arrive(c).start()
    for c in loads:
        c.start()
    gain_a = ga_ref[...].astype(jnp.float32).reshape(1, dim)
    gain_m = gm_ref[...].astype(jnp.float32).reshape(1, dim)
    first, last = span_ref[0], span_ref[1]
    tile_lane = lax.broadcasted_iota(jnp.int32, (128, 128), 1)
    tile_row = lax.broadcasted_iota(jnp.int32, (128, 128), 0)
    sign = jnp.where(tile_lane % 64 < 32, -1.0, 1.0)
    for t in range(n_rows // 128):
        rows = slice(128 * t, 128 * (t + 1))
        pos = jnp.transpose(jnp.broadcast_to(pos_ref[t:t + 1, :].astype(jnp.float32), (128, 128)))
        angle = pos * freq_ref[...]
        cos_s[rows, :] = jnp.cos(angle)
        sin_s[rows, :] = jnp.sin(angle) * sign
        start_s[rows, :] = 128 * t + tile_row - pos.astype(jnp.int32)
    for c in loads[:4]:
        c.wait()

    lane = lax.broadcasted_iota(jnp.int32, (QB, 128), 1)
    first_half = lane % 64 < 32
    low = lane < 64

    def attend(c):
        length = (c + 1) * QB
        start = start_s[c * QB:(c + 1) * QB, :]
        row = c * QB + lax.broadcasted_iota(jnp.int32, (QB, 128), 0)
        for t in range(length // 128):
            col = 128 * t + lane
            bias[:, 128 * t:128 * (t + 1)] = jnp.where((col >= start) & (col <= row), 3e38, -1e30)

        def scores(p, half, dst):
            qp = q_s[p]
            qh = jnp.where(low if half == 0 else ~low, qp, jnp.zeros_like(qp))
            s = jnp.minimum(dot_t(qh, k_s[(2 * p + half) // 7, :length, :]), bias[:, :length])
            dst[:, :length] = s
            return jnp.max(s, axis=1, keepdims=True)

        def soft(p, half, src, top):
            e = jnp.exp(src[:, :length] - top)
            total = jnp.sum(e, axis=1, keepdims=True)
            return dot_n(e.astype(jnp.bfloat16), v_s[(2 * p + half) // 7, :length, :]) / total

        def pair(p, top_a):
            top_b = scores(p, 1, sb)
            out_a = soft(p, 0, sa, top_a)
            top_a = scores(jnp.minimum(p + 1, n_pairs - 1), 0, sa)
            out_b = soft(p, 1, sb, top_b)
            o_s[:, pl.ds(pl.multiple_of(p * 128, 128), 128)] = jnp.where(low, out_a, out_b).astype(jnp.bfloat16)
            return top_a

        lax.fori_loop(0, n_pairs, pair, scores(0, 0, sa))

    @pl.loop(0, n_blk)
    def _block(c):
        rows = rows_at(c)
        arrive(c).wait_recv()
        where_row = c * QB + lax.broadcasted_iota(jnp.int32, (QB, dim), 0)
        arrived = (where_row >= first) & (where_row < last)
        r = jnp.where(arrived, rbuf[rows, :].astype(jnp.float32), rloc_ref[rows, :].astype(jnp.float32))
        r_s[...] = r
        h = norm_rows(r, gain_a)
        cos_t = cos_s[rows, :]
        sin_t = sin_s[rows, :]
        q = dot_t(h, wq_s[...])
        for p in range(n_pairs):
            qp = rope_pair(q[:, 128 * p:128 * (p + 1)], cos_t, sin_t, first_half)
            q_s[p] = (qp.astype(jnp.bfloat16) * 0.125).astype(jnp.bfloat16)
        k = rope_pair(dot_t(h, wk_s[...]), cos_t, sin_t, first_half)
        v = dot_t(h, wv_s[...])
        for s, x in ((k_s, k), (v_s, v)):
            other = pltpu.roll(x, 64, 1)
            s[0, rows, :] = jnp.where(low, x, other).astype(jnp.bfloat16)
            s[1, rows, :] = jnp.where(low, other, x).astype(jnp.bfloat16)

        for at in range(n_blk):
            pl.when(c == at)(functools.partial(attend, at))

        @pl.when(c >= 1)
        def _send():
            send(c - 1)

        @pl.when(c >= 4)
        def _relay():
            relay(c - 4)

        @pl.when(c == 0)
        def _weights():
            for x in loads[4:]:
                x.wait()

        attn = dot_n(o_s[...], wo_s[...]).astype(jnp.bfloat16)
        z = (r_s[...] + attn.astype(jnp.float32)).astype(jnp.bfloat16).astype(jnp.float32)
        r_s[...] = z
        h = norm_rows(z, gain_m)
        for t in range(ff // FT):
            cols = slice(t * FT, (t + 1) * FT)
            gate = 0.5 * dot_n(h, wg_s[:, cols])
            up = dot_n(h, wu_s[:, cols])
            m_s[:, cols] = ((gate + gate * jnp.tanh(gate)) * up).astype(jnp.bfloat16)
        down = dot_n(m_s[...], wd_s[...]).astype(jnp.bfloat16)
        obuf[lax.rem(c, 2)] = (r_s[...] + down.astype(jnp.float32)).astype(jnp.bfloat16)
        keep(c).start()

    send(n_blk - 1)
    for c in range(n_blk - 4, n_blk):
        relay(c)
    for c in range(n_blk):
        arrive(c).wait_send()
        to_sib(c).wait()
        to_peer(c).wait_send()
        forward(c).wait()


def layer(span, outgo, rloc, positions, g_attn, w_q, w_k, w_v, w_o, g_mlp, w_gate, w_up, w_down):
    n_rows, dim = rloc.shape
    head_dim = w_q.shape[2]
    half_dim = head_dim // 2
    exponent = -2.0 * np.arange(half_dim, dtype=np.float32) / np.float32(head_dim)
    inv_freq = np.power(np.float32(ROPE_BASE), exponent).astype(np.float32)
    freq = jnp.asarray(np.tile(inv_freq, 128 // half_dim)[None, :])
    wq_t = jnp.transpose(w_q, (1, 2, 0)).reshape(dim, dim)
    wk_t = jnp.transpose(w_k, (1, 2, 0)).reshape(128, dim)
    wv_t = jnp.transpose(w_v, (1, 2, 0)).reshape(128, dim)
    wo_t = w_o.reshape(dim, dim)
    bf, f32 = jnp.bfloat16, jnp.float32
    n_blk = n_rows // QB
    ff = w_gate.shape[1]
    rows = jax.ShapeDtypeStruct((n_rows, dim), bf)
    dma = pltpu.SemaphoreType.DMA
    return pl.pallas_call(
        layer_kernel,
        out_shape=[rows, rows, jax.ShapeDtypeStruct((2 * n_rows, dim), bf)],
        in_specs=[SM, ANY] + [VM] * 5 + [ANY] * 7,
        out_specs=[ANY] * 3,
        scratch_shapes=[
            pltpu.VMEM((n_rows, dim), bf), pltpu.VMEM((QB, dim), f32), pltpu.VMEM((dim // 128, QB, 128), bf),
            pltpu.VMEM((2, n_rows, 128), bf), pltpu.VMEM((2, n_rows, 128), bf), pltpu.VMEM((QB, dim), bf),
            pltpu.VMEM((QB, ff), bf), pltpu.VMEM((2, QB, dim), bf)]
            + [pltpu.VMEM((QB, n_rows), f32)] * 3
            + [pltpu.VMEM((n_rows, 128), f32), pltpu.VMEM((n_rows, 128), f32), pltpu.VMEM((n_rows, 128), jnp.int32),
               pltpu.VMEM((dim, dim), bf), pltpu.VMEM((128, dim), bf), pltpu.VMEM((128, dim), bf), pltpu.VMEM((dim, dim), bf),
               pltpu.VMEM((dim, ff), bf), pltpu.VMEM((dim, ff), bf), pltpu.VMEM((ff, dim), bf), dma((7,))] + [dma((n_blk,))] * 9,
        compiler_params=pltpu.CompilerParams(collective_id=1, has_side_effects=True, vmem_limit_bytes=67000000),
        name="layer",
    )(span, outgo, rloc, positions.reshape(-1, 128), freq, g_attn, g_mlp, wq_t, wk_t, wv_t, wo_t, w_gate, w_up, w_down)


CHUNK = 128
MESH_ID = pl.DeviceIdType.MESH
ANY = pl.BlockSpec(memory_space=pl.ANY)
VM = pl.BlockSpec(memory_space=pltpu.VMEM)
SM = pl.BlockSpec(memory_space=pltpu.SMEM)


def meet(devices):
    barrier = pltpu.get_barrier_semaphore()
    for dev in devices:
        pl.semaphore_signal(barrier, inc=1, device_id={"sp": dev}, device_id_type=MESH_ID)
    pl.semaphore_wait(barrier, len(devices))


def push(src, dst, send_sem, recv_sem, dev):
    return pltpu.make_async_remote_copy(src_ref=src, dst_ref=dst, send_sem=send_sem, recv_sem=recv_sem,
                                        device_id={"sp": dev}, device_id_type=MESH_ID)


def share_kernel(n_split, *refs):
    n = (len(refs) - 2) // 2
    ins, outs, send_sems, recv_sems = refs[:n], refs[n:2 * n], refs[-2], refs[-1]
    me = lax.axis_index("sp")
    sib = me + 1 - 2 * lax.rem(me, 2)
    meet([sib])
    copies = []
    for a, b in zip(ins, outs):
        parts = n_split if a.ndim == 2 else 1
        step = a.shape[0] // parts
        for p in range(parts):
            rows = pl.ds(p * step, step)
            copies.append((a.at[rows], b.at[rows]) if parts > 1 else (a, b))
    started = []
    for i, (a, b) in enumerate(copies):
        cp = push(a, b, send_sems.at[i], recv_sems.at[i], sib)
        cp.start()
        started.append(cp)
    for cp in started:
        cp.wait()


def share(arrays, collective_id):
    return pl.pallas_call(
        functools.partial(share_kernel, 4),
        out_shape=[jax.ShapeDtypeStruct(a.shape, a.dtype) for a in arrays],
        in_specs=[ANY] * len(arrays), out_specs=[ANY] * len(arrays),
        scratch_shapes=[pltpu.SemaphoreType.DMA((16,)), pltpu.SemaphoreType.DMA((16,))],
        compiler_params=pltpu.CompilerParams(collective_id=collective_id, has_side_effects=True),
        name="share",
    )(*arrays)


LOAD = 512


def load_table(parts, tab, stage, sems):
    jobs = []
    for ref, blocks in parts:
        for i in range(ref.shape[0] // LOAD):
            n = len(jobs)
            copy = pltpu.make_async_copy(ref.at[pl.ds(i * LOAD, LOAD)], stage.at[pl.ds(n * LOAD, LOAD)], sems.at[n])
            jobs.append((copy, None if blocks is None else i < blocks))
    for copy, cond in jobs:
        if cond is None:
            copy.start()
        else:
            pl.when(cond)(copy.start)
    for n, (copy, cond) in enumerate(jobs):
        def fill(n=n, copy=copy):
            copy.wait()
            fill_table(stage, n * LOAD, tab, n * LOAD)
        if cond is None:
            fill()
        else:
            pl.when(cond)(fill)


def fill_table(stage, at, tab, base):
    @pl.loop(0, LOAD // 64)
    def _blk(i):
        rows = pl.ds(pl.multiple_of(at + i * 64, 64), 64)
        first = pl.multiple_of((base + i * 64) * 8, 8)
        for j in range(stage.shape[1] // 128):
            tab[pl.ds(first + j, 64, stride=8), :] = stage[rows, 128 * j:128 * (j + 1)].astype(jnp.float32)


UNROLL = 16


def slab(k):
    return pl.ds(pl.multiple_of(k * 8, 8), 8)


def copy_rows(n_rows, move):
    @pl.loop(0, n_rows // UNROLL)
    def _grp(i):
        for k in range(UNROLL):
            move(i * UNROLL + k)


def rows_out(n_rows, src3, dst):
    @pl.loop(0, n_rows // CHUNK)
    def _blk(i):
        rows = pl.ds(pl.multiple_of(i * CHUNK, CHUNK), CHUNK)
        for j in range(dst.shape[1] // 128):
            dst[rows, 128 * j:128 * (j + 1)] = src3[pl.ds(pl.multiple_of(i * CHUNK * 8, 8) + j, CHUNK, stride=8), :].astype(dst.dtype)


def move_run(n, one):
    whole = n // UNROLL

    @pl.loop(0, whole)
    def _grp(i):
        for k in range(UNROLL):
            one(i * UNROLL + k)

    @pl.loop(whole * UNROLL, n)
    def _one(i):
        one(i)


def pick_kernel(perm, so, sl, ro, rl, perm_b, so_b, sl_b, ro_b, rl_b, own, sib, outgo, rloc, span, tab, out3, stage, sems):
    cap = rloc.shape[0]
    n_tok = own.shape[0]
    me = lax.axis_index("sp")
    core = lax.rem(me, 2)
    chip = me // 2
    mate = me + 1 - 2 * core
    near, far = 2 * chip, 2 * (1 - chip)
    load_table([(own, None), (sib, None)], tab, stage, sems)
    n_in = rl[far] + rl[far + 1]
    span[0] = (1 - chip) * (cap - n_in)
    span[1] = (1 - chip) * (cap - n_in) + n_in

    def run(dst_row, src, table_row, at, n):
        def one(t):
            out3[slab(dst_row + t), :] = tab[slab(table_row + src[at + t]), :]
        move_run(n, one)

    goal = far + core
    row = chip * (cap - sl[goal] - sl_b[goal])
    run(row + core * sl_b[goal], perm, 0, so[goal], sl[goal])
    run(row + (1 - core) * sl[goal], perm_b, n_tok, so_b[goal], sl_b[goal])
    rows_out(cap, out3, outgo)
    run(ro[me], perm, 0, so[me], sl[me])
    run(ro[mate], perm_b, n_tok, so_b[me], sl_b[me])
    rows_out(cap, out3, rloc)


def back_place_kernel(perm, so, sl, ro, rl, perm_b, so_b, sl_b, ro_b, rl_b, own, sib, stream, out, tab, out3, stage, sems):
    cap = own.shape[0]
    n_tok = out.shape[0]
    me = lax.axis_index("sp")
    core = lax.rem(me, 2)
    chip = me // 2
    mate = me + 1 - 2 * core
    far = 2 * (1 - chip)
    load_table([(own, None), (sib, None), (stream, None)], tab, stage, sems)

    def run(goal, row):
        def one(t):
            out3[slab(perm[so[goal] + t]), :] = tab[slab(row + t), :]
        move_run(sl[goal], one)

    run(me, ro[me])
    run(mate, cap + ro_b[me])
    for goal, base in ((far + core, 2 * cap), (far + 1 - core, 3 * cap)):
        run(goal, base + chip * (cap - sl[goal] - sl_b[goal]) + core * sl_b[goal])
    sent = so[3] + sl[3]

    def blank(t):
        out3[slab(perm[sent + t]), :] = jnp.zeros((8, 128), jnp.float32)

    move_run(n_tok - sent, blank)
    rows_out(n_tok, out3, out)


def local_call(body, out_shapes, out_specs, n_any, tab_rows, out_rows, dim, name):
    return pl.pallas_call(
        body,
        out_shape=out_shapes,
        in_specs=[SM] * 10 + [ANY] * n_any,
        out_specs=out_specs,
        scratch_shapes=[pltpu.VMEM((tab_rows * 8, 128), jnp.float32), pltpu.VMEM((out_rows * 8, 128), jnp.float32),
                        pltpu.VMEM((tab_rows, dim), jnp.bfloat16), pltpu.SemaphoreType.DMA((tab_rows // LOAD,))],
        compiler_params=pltpu.CompilerParams(vmem_limit_bytes=66000000),
        name=name,
    )


def solution(mesh):
    row_spec = P(('dp', 'sp'), None)
    vec_spec = P(('dp', 'sp'))
    rep_spec = P()

    def per_device(hidden, tok_perm, send_off, send_len, recv_off, recv_len, recv_doc, recv_pos, g_attn, w_q, w_k, w_v, w_o, g_mlp, w_gate, w_up, w_down):
        n_tok, dim = hidden.shape
        cap = recv_doc.shape[0]
        plan = [tok_perm, send_off, send_len, recv_off, recv_len]
        sib_hidden, *sib_plan = share([hidden] + plan, 0)
        rows_bf = jax.ShapeDtypeStruct((cap, dim), hidden.dtype)
        outs = [rows_bf, rows_bf, jax.ShapeDtypeStruct((2,), jnp.int32)]
        outgo, rloc, span = local_call(pick_kernel, outs, [VM, VM, SM], 2, 2 * n_tok, cap, dim, "pick")(*plan, *sib_plan, hidden, sib_hidden)
        done, sib_done, returned = layer(span, outgo, rloc, recv_pos, g_attn, w_q, w_k, w_v, w_o, g_mlp, w_gate, w_up, w_down)
        out = jax.ShapeDtypeStruct((n_tok, dim), hidden.dtype)
        return local_call(back_place_kernel, out, VM, 3, 4 * cap, n_tok, dim, "back_place")(*plan, *sib_plan, done, sib_done, returned)

    return jax.shard_map(per_device, mesh=mesh, in_specs=(row_spec,) + (vec_spec,) * 7 + (rep_spec,) * 9, out_specs=row_spec, check_vma=False)
```

```python
import functools

import jax
import jax.numpy as jnp
import numpy as np
from jax import lax
from jax.experimental import pallas as pl
from jax.experimental.pallas import tpu as pltpu
from jax.sharding import PartitionSpec as P

ROPE_BASE = 500000.0
NORM_EPS = 1e-5
ROWS = 512
QB = 256
FT = 256


def norm_rows(rows_f, gain):
    inv = lax.rsqrt(jnp.mean(rows_f * rows_f, axis=-1, keepdims=True) + NORM_EPS)
    return (rows_f * inv * gain).astype(jnp.bfloat16)


def rope_pair(x, cos_t, sin_t, first_half):
    swapped = jnp.where(first_half, pltpu.roll(x, 96, 1), pltpu.roll(x, 32, 1))
    return x * cos_t + swapped * sin_t


def dot_t(a, b):
    return lax.dot_general(a, b, (((1,), (1,)), ((), ())), preferred_element_type=jnp.float32)


def dot_n(a, b):
    return jnp.dot(a, b, preferred_element_type=jnp.float32)


def layer_kernel(span_ref, outgo, rloc_ref, pos_ref, freq_ref, ga_ref, gm_ref, wq_h, wk_h, wv_h, wo_h, wg_h, wu_h, wd_h, own, sib_out, far,
                 rbuf, r_s, q_s, k_s, v_s, o_s, m_s, obuf, sa, sb, bias, cos_s, sin_s, start_s, wq_s, wk_s, wv_s, wo_s, wg_s, wu_s, wd_s, sems,
                 as_, ar, ps, pr, ss, sr, fs, fr, own_sem):
    n_rows, dim = rloc_ref.shape
    n_pairs = dim // 128
    n_blk = n_rows // QB
    ff = wg_s.shape[1]
    me = lax.axis_index("sp")
    sib = me + 1 - 2 * lax.rem(me, 2)
    peer = lax.rem(me + 2, 4)
    loads = [pltpu.make_async_copy(a, b, sems.at[i]) for i, (a, b) in enumerate(
        [(wq_h, wq_s), (wk_h, wk_s), (wv_h, wv_s), (wo_h, wo_s), (wg_h, wg_s), (wu_h, wu_s), (wd_h, wd_s)])]
    meet([sib, peer])

    def rows_at(c):
        return pl.ds(pl.multiple_of(c * QB, QB), QB)

    def arrive(c):
        return push(outgo.at[rows_at(c)], rbuf.at[rows_at(c)], as_.at[c], ar.at[c], peer)

    def to_peer(c):
        return push(own.at[rows_at(c)], far.at[rows_at(c)], ps.at[c], pr.at[c], peer)

    def to_sib(c):
        return push(own.at[rows_at(c)], sib_out.at[rows_at(c)], ss.at[c], sr.at[c], sib)

    def forward(c):
        return push(far.at[rows_at(c)], far.at[pl.ds(pl.multiple_of(n_rows + c * QB, QB), QB)], fs.at[c], fr.at[c], sib)

    def keep(c):
        return pltpu.make_async_copy(obuf.at[lax.rem(c, 2)], own.at[rows_at(c)], own_sem.at[c])

    def send(c):
        keep(c).wait()
        to_peer(c).start()
        to_sib(c).start()

    def relay(c):
        to_peer(c).wait_recv()
        forward(c).start()

    for c in range(n_blk):
        arrive(c).start()
    for c in loads:
        c.start()
    gain_a = ga_ref[...].astype(jnp.float32).reshape(1, dim)
    gain_m = gm_ref[...].astype(jnp.float32).reshape(1, dim)
    first, last = span_ref[0], span_ref[1]
    tile_lane = lax.broadcasted_iota(jnp.int32, (128, 128), 1)
    tile_row = lax.broadcasted_iota(jnp.int32, (128, 128), 0)
    sign = jnp.where(tile_lane % 64 < 32, -1.0, 1.0)
    for t in range(n_rows // 128):
        rows = slice(128 * t, 128 * (t + 1))
        pos = jnp.transpose(jnp.broadcast_to(pos_ref[t:t + 1, :].astype(jnp.float32), (128, 128)))
        angle = pos * freq_ref[...]
        cos_s[rows, :] = jnp.cos(angle)
        sin_s[rows, :] = jnp.sin(angle) * sign
        start_s[rows, :] = 128 * t + tile_row - pos.astype(jnp.int32)
    for c in loads[:4]:
        c.wait()

    lane = lax.broadcasted_iota(jnp.int32, (QB, 128), 1)
    first_half = lane % 64 < 32
    low = lane < 64

    def attend(c):
        length = (c + 1) * QB
        start = start_s[c * QB:(c + 1) * QB, :]
        row = c * QB + lax.broadcasted_iota(jnp.int32, (QB, 128), 0)
        for t in range(length // 128):
            col = 128 * t + lane
            bias[:, 128 * t:128 * (t + 1)] = jnp.where((col >= start) & (col <= row), 3e38, -1e30)

        def scores(p, half, dst):
            qp = q_s[p]
            qh = jnp.where(low if half == 0 else ~low, qp, jnp.zeros_like(qp))
            s = jnp.minimum(dot_t(qh, k_s[(2 * p + half) // 7, :length, :]), bias[:, :length])
            dst[:, :length] = s
            return jnp.max(s, axis=1, keepdims=True)

        def soft(p, half, src, top):
            e = jnp.exp(src[:, :length] - top)
            total = jnp.sum(e, axis=1, keepdims=True)
            return dot_n(e.astype(jnp.bfloat16), v_s[(2 * p + half) // 7, :length, :]) / total

        def pair(p, top_a):
            top_b = scores(p, 1, sb)
            out_a = soft(p, 0, sa, top_a)
            top_a = scores(jnp.minimum(p + 1, n_pairs - 1), 0, sa)
            out_b = soft(p, 1, sb, top_b)
            o_s[:, pl.ds(pl.multiple_of(p * 128, 128), 128)] = jnp.where(low, out_a, out_b).astype(jnp.bfloat16)
            return top_a

        lax.fori_loop(0, n_pairs, pair, scores(0, 0, sa))

    @pl.loop(0, n_blk)
    def _block(c):
        rows = rows_at(c)
        arrive(c).wait_recv()
        where_row = c * QB + lax.broadcasted_iota(jnp.int32, (QB, dim), 0)
        arrived = (where_row >= first) & (where_row < last)
        r = jnp.where(arrived, rbuf[rows, :].astype(jnp.float32), rloc_ref[rows, :].astype(jnp.float32))
        r_s[...] = r
        h = norm_rows(r, gain_a)
        cos_t = cos_s[rows, :]
        sin_t = sin_s[rows, :]
        q = dot_t(h, wq_s[...])
        for p in range(n_pairs):
            qp = rope_pair(q[:, 128 * p:128 * (p + 1)], cos_t, sin_t, first_half)
            q_s[p] = (qp.astype(jnp.bfloat16) * 0.125).astype(jnp.bfloat16)
        k = rope_pair(dot_t(h, wk_s[...]), cos_t, sin_t, first_half)
        v = dot_t(h, wv_s[...])
        for s, x in ((k_s, k), (v_s, v)):
            other = pltpu.roll(x, 64, 1)
            s[0, rows, :] = jnp.where(low, x, other).astype(jnp.bfloat16)
            s[1, rows, :] = jnp.where(low, other, x).astype(jnp.bfloat16)

        for at in range(n_blk):
            pl.when(c == at)(functools.partial(attend, at))

        @pl.when(c >= 1)
        def _send():
            send(c - 1)

        @pl.when(c >= 4)
        def _relay():
            relay(c - 4)

        @pl.when(c == 0)
        def _weights():
            for x in loads[4:]:
                x.wait()

        attn = dot_n(o_s[...], wo_s[...]).astype(jnp.bfloat16)
        z = (r_s[...] + attn.astype(jnp.float32)).astype(jnp.bfloat16).astype(jnp.float32)
        r_s[...] = z
        h = norm_rows(z, gain_m)
        for t in range(ff // FT):
            cols = slice(t * FT, (t + 1) * FT)
            gate = 0.5 * dot_n(h, wg_s[:, cols])
            up = dot_n(h, wu_s[:, cols])
            m_s[:, cols] = ((gate + gate * jnp.tanh(gate)) * up).astype(jnp.bfloat16)
        down = dot_n(m_s[...], wd_s[...]).astype(jnp.bfloat16)
        obuf[lax.rem(c, 2)] = (r_s[...] + down.astype(jnp.float32)).astype(jnp.bfloat16)
        keep(c).start()

    send(n_blk - 1)
    for c in range(n_blk - 4, n_blk):
        relay(c)
    for c in range(n_blk):
        arrive(c).wait_send()
        to_sib(c).wait()
        to_peer(c).wait_send()
        forward(c).wait()


def layer(span, outgo, rloc, positions, g_attn, w_q, w_k, w_v, w_o, g_mlp, w_gate, w_up, w_down):
    n_rows, dim = rloc.shape
    head_dim = w_q.shape[2]
    half_dim = head_dim // 2
    exponent = -2.0 * np.arange(half_dim, dtype=np.float32) / np.float32(head_dim)
    inv_freq = np.power(np.float32(ROPE_BASE), exponent).astype(np.float32)
    freq = jnp.asarray(np.tile(inv_freq, 128 // half_dim)[None, :])
    wq_t = jnp.transpose(w_q, (1, 2, 0)).reshape(dim, dim)
    wk_t = jnp.transpose(w_k, (1, 2, 0)).reshape(128, dim)
    wv_t = jnp.transpose(w_v, (1, 2, 0)).reshape(128, dim)
    wo_t = w_o.reshape(dim, dim)
    bf, f32 = jnp.bfloat16, jnp.float32
    n_blk = n_rows // QB
    ff = w_gate.shape[1]
    rows = jax.ShapeDtypeStruct((n_rows, dim), bf)
    dma = pltpu.SemaphoreType.DMA
    return pl.pallas_call(
        layer_kernel,
        out_shape=[rows, rows, jax.ShapeDtypeStruct((2 * n_rows, dim), bf)],
        in_specs=[SM, ANY] + [VM] * 5 + [ANY] * 7,
        out_specs=[ANY] * 3,
        scratch_shapes=[
            pltpu.VMEM((n_rows, dim), bf), pltpu.VMEM((QB, dim), f32), pltpu.VMEM((dim // 128, QB, 128), bf),
            pltpu.VMEM((2, n_rows, 128), bf), pltpu.VMEM((2, n_rows, 128), bf), pltpu.VMEM((QB, dim), bf),
            pltpu.VMEM((QB, ff), bf), pltpu.VMEM((2, QB, dim), bf)]
            + [pltpu.VMEM((QB, n_rows), f32)] * 3
            + [pltpu.VMEM((n_rows, 128), f32), pltpu.VMEM((n_rows, 128), f32), pltpu.VMEM((n_rows, 128), jnp.int32),
               pltpu.VMEM((dim, dim), bf), pltpu.VMEM((128, dim), bf), pltpu.VMEM((128, dim), bf), pltpu.VMEM((dim, dim), bf),
               pltpu.VMEM((dim, ff), bf), pltpu.VMEM((dim, ff), bf), pltpu.VMEM((ff, dim), bf), dma((7,))] + [dma((n_blk,))] * 9,
        compiler_params=pltpu.CompilerParams(collective_id=1, has_side_effects=True, vmem_limit_bytes=67000000),
        name="layer",
    )(span, outgo, rloc, positions.reshape(-1, 128), freq, g_attn, g_mlp, wq_t, wk_t, wv_t, wo_t, w_gate, w_up, w_down)


CHUNK = 128
MESH_ID = pl.DeviceIdType.MESH
ANY = pl.BlockSpec(memory_space=pl.ANY)
VM = pl.BlockSpec(memory_space=pltpu.VMEM)
SM = pl.BlockSpec(memory_space=pltpu.SMEM)


def meet(devices):
    barrier = pltpu.get_barrier_semaphore()
    for dev in devices:
        pl.semaphore_signal(barrier, inc=1, device_id={"sp": dev}, device_id_type=MESH_ID)
    pl.semaphore_wait(barrier, len(devices))


def push(src, dst, send_sem, recv_sem, dev):
    return pltpu.make_async_remote_copy(src_ref=src, dst_ref=dst, send_sem=send_sem, recv_sem=recv_sem,
                                        device_id={"sp": dev}, device_id_type=MESH_ID)


def share_kernel(n_split, *refs):
    n = (len(refs) - 2) // 2
    ins, outs, send_sems, recv_sems = refs[:n], refs[n:2 * n], refs[-2], refs[-1]
    me = lax.axis_index("sp")
    sib = me + 1 - 2 * lax.rem(me, 2)
    meet([sib])
    copies = []
    for a, b in zip(ins, outs):
        parts = n_split if a.ndim == 2 else 1
        step = a.shape[0] // parts
        for p in range(parts):
            rows = pl.ds(p * step, step)
            copies.append((a.at[rows], b.at[rows]) if parts > 1 else (a, b))
    started = []
    for i, (a, b) in enumerate(copies):
        cp = push(a, b, send_sems.at[i], recv_sems.at[i], sib)
        cp.start()
        started.append(cp)
    for cp in started:
        cp.wait()


def share(arrays, collective_id):
    return pl.pallas_call(
        functools.partial(share_kernel, 4),
        out_shape=[jax.ShapeDtypeStruct(a.shape, a.dtype) for a in arrays],
        in_specs=[ANY] * len(arrays), out_specs=[ANY] * len(arrays),
        scratch_shapes=[pltpu.SemaphoreType.DMA((16,)), pltpu.SemaphoreType.DMA((16,))],
        compiler_params=pltpu.CompilerParams(collective_id=collective_id, has_side_effects=True),
        name="share",
    )(*arrays)


LOAD = 512
FILL = 64
PITCH = 9


def load_table(parts, tab, stage, sems):
    jobs = []
    for ref, lo, hi in parts:
        for i in range(ref.shape[0] // LOAD):
            n = len(jobs)
            copy = pltpu.make_async_copy(ref.at[pl.ds(i * LOAD, LOAD)], stage.at[pl.ds(n * LOAD, LOAD)], sems.at[n])
            if lo is None:
                jobs.append((copy, None, 0, LOAD // FILL))
            else:
                low, high = jnp.maximum(lo - i * LOAD, 0), jnp.minimum(hi - i * LOAD, LOAD)
                jobs.append((copy, low < high, low // FILL, (high + FILL - 1) // FILL))
    for copy, cond, _, _ in jobs:
        if cond is None:
            copy.start()
        else:
            pl.when(cond)(copy.start)
    for n, (copy, cond, low, high) in enumerate(jobs):
        def fill(n=n, copy=copy, low=low, high=high):
            copy.wait()

            @pl.loop(low, high)
            def _blk(i):
                rows = pl.ds(pl.multiple_of(n * LOAD + i * FILL, FILL), FILL)
                first = (n * LOAD + i * FILL) * PITCH
                for j in range(stage.shape[1] // 128):
                    tab[pl.ds(first + j, FILL, stride=PITCH), :] = stage[rows, 128 * j:128 * (j + 1)].astype(jnp.float32)
        if cond is None:
            fill()
        else:
            pl.when(cond)(fill)


UNROLL = 16


def slab(k):
    return pl.ds(pl.multiple_of(k * 8, 8), 8)


def rows_out(lo, hi, src3, stage, base, dst, sem):
    first, last = lo // CHUNK, (hi + CHUNK - 1) // CHUNK

    def copy(i):
        rows = pl.multiple_of(i * CHUNK, CHUNK)
        return pltpu.make_async_copy(stage.at[pl.ds(base + rows, CHUNK)], dst.at[pl.ds(rows, CHUNK)], sem)

    @pl.loop(first, last)
    def _blk(i):
        rows = pl.ds(pl.multiple_of(base + i * CHUNK, CHUNK), CHUNK)
        for j in range(dst.shape[1] // 128):
            stage[rows, 128 * j:128 * (j + 1)] = src3[pl.ds(i * CHUNK * PITCH + j, CHUNK, stride=PITCH), :].astype(stage.dtype)
        copy(i).start()

    def finish():
        pl.loop(first, last)(lambda i: copy(i).wait())

    return finish


def slab(k):
    return pl.ds(k * PITCH, 8)


def move_run(n, one):
    whole = n // UNROLL

    @pl.loop(0, whole)
    def _grp(i):
        for k in range(UNROLL):
            one(i * UNROLL + k)

    @pl.loop(whole * UNROLL, n)
    def _one(i):
        one(i)


def pick_kernel(perm, so, sl, ro, rl, perm_b, so_b, sl_b, ro_b, rl_b, own, sib, outgo, rloc, span, tab, out3, stage, sems, out_sems):
    cap = rloc.shape[0]
    n_tok = own.shape[0]
    me = lax.axis_index("sp")
    core = lax.rem(me, 2)
    chip = me // 2
    mate = me + 1 - 2 * core
    far = 2 * (1 - chip)
    load_table([(own, None, None), (sib, None, None)], tab, stage, sems)
    n_in = rl[far] + rl[far + 1]
    span[0] = (1 - chip) * (cap - n_in)
    span[1] = (1 - chip) * (cap - n_in) + n_in

    def run(dst_row, src, table_row, at, n):
        def one(t):
            out3[slab(dst_row + t), :] = tab[slab(table_row + src[at + t]), :]
        move_run(n, one)

    goal = far + core
    n_out = sl[goal] + sl_b[goal]
    row = chip * (cap - n_out)
    run(row + core * sl_b[goal], perm, 0, so[goal], sl[goal])
    run(row + (1 - core) * sl[goal], perm_b, n_tok, so_b[goal], sl_b[goal])
    finish_out = rows_out(row, row + n_out, out3, stage, 0, outgo, out_sems.at[0])
    near = chip * n_in
    run(ro[me], perm, 0, so[me], sl[me])
    run(ro[mate], perm_b, n_tok, so_b[me], sl_b[me])
    finish_loc = rows_out(near, near + cap - n_in, out3, stage, cap, rloc, out_sems.at[1])
    finish_out()
    finish_loc()


def back_place_kernel(perm, so, sl, ro, rl, perm_b, so_b, sl_b, ro_b, rl_b, own, sib, stream, out, tab, out3, stage, sems, out_sems):
    cap = own.shape[0]
    n_tok = out.shape[0]
    me = lax.axis_index("sp")
    core = lax.rem(me, 2)
    chip = me // 2
    mate = me + 1 - 2 * core
    far = 2 * (1 - chip)

    def far_row(goal):
        return chip * (cap - sl[goal] - sl_b[goal]) + core * sl_b[goal]

    runs = [(me, own, ro[me]), (mate, sib, ro_b[me]),
            (far + core, stream.at[pl.ds(0, cap)], far_row(far + core)), (far + 1 - core, stream.at[pl.ds(cap, cap)], far_row(far + 1 - core))]
    load_table([(ref, row, row + sl[goal]) for goal, ref, row in runs], tab, stage, sems)
    for n, (goal, _, row) in enumerate(runs):
        def one(t, goal=goal, row=n * cap + row):
            out3[slab(perm[so[goal] + t]), :] = tab[slab(row + t), :]
        move_run(sl[goal], one)
    sent = so[3] + sl[3]

    def blank(t):
        out3[slab(perm[sent + t]), :] = jnp.zeros((8, 128), jnp.float32)

    move_run(n_tok - sent, blank)
    rows_out(0, n_tok, out3, stage, 0, out, out_sems.at[0])()


def local_call(body, out_shapes, out_specs, n_any, tab_rows, out_rows, dim, name):
    return pl.pallas_call(
        body,
        out_shape=out_shapes,
        in_specs=[SM] * 10 + [ANY] * n_any,
        out_specs=out_specs,
        scratch_shapes=[pltpu.VMEM((tab_rows * PITCH, 128), jnp.float32), pltpu.VMEM((out_rows * PITCH, 128), jnp.float32),
                        pltpu.VMEM((tab_rows, dim), jnp.bfloat16), pltpu.SemaphoreType.DMA((tab_rows // LOAD,)), pltpu.SemaphoreType.DMA((2,))],
        compiler_params=pltpu.CompilerParams(vmem_limit_bytes=66000000),
        name=name,
    )


def solution(mesh):
    row_spec = P(('dp', 'sp'), None)
    vec_spec = P(('dp', 'sp'))
    rep_spec = P()

    def per_device(hidden, tok_perm, send_off, send_len, recv_off, recv_len, recv_doc, recv_pos, g_attn, w_q, w_k, w_v, w_o, g_mlp, w_gate, w_up, w_down):
        n_tok, dim = hidden.shape
        cap = recv_doc.shape[0]
        plan = [tok_perm, send_off, send_len, recv_off, recv_len]
        sib_hidden, *sib_plan = share([hidden] + plan, 0)
        rows_bf = jax.ShapeDtypeStruct((cap, dim), hidden.dtype)
        outs = [rows_bf, rows_bf, jax.ShapeDtypeStruct((2,), jnp.int32)]
        outgo, rloc, span = local_call(pick_kernel, outs, [ANY, ANY, SM], 2, 2 * n_tok, cap, dim, "pick")(*plan, *sib_plan, hidden, sib_hidden)
        done, sib_done, returned = layer(span, outgo, rloc, recv_pos, g_attn, w_q, w_k, w_v, w_o, g_mlp, w_gate, w_up, w_down)
        out = jax.ShapeDtypeStruct((n_tok, dim), hidden.dtype)
        return local_call(back_place_kernel, out, ANY, 3, 4 * cap, n_tok, dim, "back_place")(*plan, *sib_plan, done, sib_done, returned)

    return jax.shard_map(per_device, mesh=mesh, in_specs=(row_spec,) + (vec_spec,) * 7 + (rep_spec,) * 9, out_specs=row_spec, check_vma=False)
```

```python
import functools

import jax
import jax.numpy as jnp
import numpy as np
from jax import lax
from jax.experimental import pallas as pl
from jax.experimental.pallas import tpu as pltpu
from jax.sharding import PartitionSpec as P

ROPE_BASE = 500000.0
NORM_EPS = 1e-5
ROWS = 512
QB = 256
FT = 256


def norm_rows(rows_f, gain):
    inv = lax.rsqrt(jnp.mean(rows_f * rows_f, axis=-1, keepdims=True) + NORM_EPS)
    return (rows_f * inv * gain).astype(jnp.bfloat16)


def rope_pair(x, cos_t, sin_t, first_half):
    swapped = jnp.where(first_half, pltpu.roll(x, 96, 1), pltpu.roll(x, 32, 1))
    return x * cos_t + swapped * sin_t


def dot_t(a, b):
    return lax.dot_general(a, b, (((1,), (1,)), ((), ())), preferred_element_type=jnp.float32)


def dot_n(a, b):
    return jnp.dot(a, b, preferred_element_type=jnp.float32)


def layer_kernel(span_ref, out_a, out_b, loc_a, loc_b, pos_ref, freq_ref, ga_ref, gm_ref, wq_h, wk_h, wv_h, wo_h, wg_h, wu_h, wd_h, own, sib_out, far,
                 rbuf, oa, ob, la, lb, r_s, q_s, k_s, v_s, o_s, m_s, obuf, sa, sb, bias, cos_s, sin_s, start_s, wq_s, wk_s, wv_s, wo_s, wg_s, wu_s, wd_s, sems,
                 as_, ar, ps, pr, ss, sr, fs, fr, own_sem, oas, obs, obr, las, lbs, lbr):
    n_rows, dim = loc_a.shape
    n_pairs = dim // 128
    n_blk = n_rows // QB
    ff = wg_s.shape[1]
    me = lax.axis_index("sp")
    sib = me + 1 - 2 * lax.rem(me, 2)
    peer = lax.rem(me + 2, 4)
    loads = [pltpu.make_async_copy(a, b, sems.at[i]) for i, (a, b) in enumerate(
        [(wq_h, wq_s), (wk_h, wk_s), (wv_h, wv_s), (wo_h, wo_s), (wg_h, wg_s), (wu_h, wu_s), (wd_h, wd_s)])]
    meet([sib, peer])

    def rows_at(c):
        return pl.ds(pl.multiple_of(c * QB, QB), QB)

    def arrive(c):
        return push(ob.at[rows_at(c)], rbuf.at[rows_at(c)], as_.at[c], ar.at[c], peer)

    def to_peer(c):
        return push(own.at[rows_at(c)], far.at[rows_at(c)], ps.at[c], pr.at[c], peer)

    def to_sib(c):
        return push(own.at[rows_at(c)], sib_out.at[rows_at(c)], ss.at[c], sr.at[c], sib)

    def forward(c):
        return push(far.at[rows_at(c)], far.at[pl.ds(pl.multiple_of(n_rows + c * QB, QB), QB)], fs.at[c], fr.at[c], sib)

    def keep(c):
        return pltpu.make_async_copy(obuf.at[lax.rem(c, 2)], own.at[rows_at(c)], own_sem.at[c])

    def send(c):
        keep(c).wait()
        to_peer(c).start()
        to_sib(c).start()

    def relay(c):
        to_peer(c).wait_recv()
        forward(c).start()

    def fetch(c, src, dst, sem):
        return pltpu.make_async_copy(src.at[rows_at(c)], dst.at[rows_at(c)], sem.at[c])

    def trade(c, src, dst, send_sem, recv_sem):
        return push(src.at[rows_at(c)], dst.at[rows_at(c)], send_sem.at[c], recv_sem.at[c], sib)

    def select(c, lo, hi, yes, no):
        row = c * QB + lax.broadcasted_iota(jnp.int32, (QB, dim), 0)
        return jnp.where((row >= lo) & (row < hi), yes.astype(jnp.float32), no.astype(jnp.float32))

    for c in range(n_blk):
        trade(c, out_b, ob, obs, obr).start()
        fetch(c, out_a, oa, oas).start()
    for c in range(n_blk):
        trade(c, loc_b, lb, lbs, lbr).start()
        fetch(c, loc_a, la, las).start()
    for c in loads:
        c.start()
    for c in range(n_blk):
        trade(c, out_b, ob, obs, obr).wait_recv()
        fetch(c, out_a, oa, oas).wait()
        rows = rows_at(c)
        ob[rows, :] = select(c, span_ref[2], span_ref[3], oa[rows, :], ob[rows, :]).astype(jnp.bfloat16)
        if c:
            arrive(c - 1).start()
    gain_a = ga_ref[...].astype(jnp.float32).reshape(1, dim)
    gain_m = gm_ref[...].astype(jnp.float32).reshape(1, dim)
    first, last = span_ref[0], span_ref[1]
    tile_lane = lax.broadcasted_iota(jnp.int32, (128, 128), 1)
    tile_row = lax.broadcasted_iota(jnp.int32, (128, 128), 0)
    sign = jnp.where(tile_lane % 64 < 32, -1.0, 1.0)
    for t in range(n_rows // 128):
        rows = slice(128 * t, 128 * (t + 1))
        pos = jnp.transpose(jnp.broadcast_to(pos_ref[t:t + 1, :].astype(jnp.float32), (128, 128)))
        angle = pos * freq_ref[...]
        cos_s[rows, :] = jnp.cos(angle)
        sin_s[rows, :] = jnp.sin(angle) * sign
        start_s[rows, :] = 128 * t + tile_row - pos.astype(jnp.int32)
        if t == 0:
            arrive(n_blk - 1).start()
    for c in loads[:4]:
        c.wait()

    lane = lax.broadcasted_iota(jnp.int32, (QB, 128), 1)
    first_half = lane % 64 < 32
    low = lane < 64

    def attend(c):
        length = (c + 1) * QB
        start = start_s[c * QB:(c + 1) * QB, :]
        row = c * QB + lax.broadcasted_iota(jnp.int32, (QB, 128), 0)
        for t in range(length // 128):
            col = 128 * t + lane
            bias[:, 128 * t:128 * (t + 1)] = jnp.where((col >= start) & (col <= row), 3e38, -1e30)

        def scores(p, half, dst):
            qp = q_s[p]
            qh = jnp.where(low if half == 0 else ~low, qp, jnp.zeros_like(qp))
            s = jnp.minimum(dot_t(qh, k_s[(2 * p + half) // 7, :length, :]), bias[:, :length])
            dst[:, :length] = s
            return jnp.max(s, axis=1, keepdims=True)

        def soft(p, half, src, top):
            e = jnp.exp(src[:, :length] - top)
            total = jnp.sum(e, axis=1, keepdims=True)
            return dot_n(e.astype(jnp.bfloat16), v_s[(2 * p + half) // 7, :length, :]) / total

        def pair(p, top_a):
            top_b = scores(p, 1, sb)
            out_a = soft(p, 0, sa, top_a)
            top_a = scores(jnp.minimum(p + 1, n_pairs - 1), 0, sa)
            out_b = soft(p, 1, sb, top_b)
            o_s[:, pl.ds(pl.multiple_of(p * 128, 128), 128)] = jnp.where(low, out_a, out_b).astype(jnp.bfloat16)
            return top_a

        lax.fori_loop(0, n_pairs, pair, scores(0, 0, sa))

    @pl.loop(0, n_blk)
    def _block(c):
        rows = rows_at(c)
        arrive(c).wait_recv()
        trade(c, loc_b, lb, lbs, lbr).wait_recv()
        fetch(c, loc_a, la, las).wait()
        r = select(c, first, last, rbuf[rows, :], select(c, span_ref[4], span_ref[5], la[rows, :], lb[rows, :]))
        r_s[...] = r
        h = norm_rows(r, gain_a)
        cos_t = cos_s[rows, :]
        sin_t = sin_s[rows, :]
        q = dot_t(h, wq_s[...])
        for p in range(n_pairs):
            qp = rope_pair(q[:, 128 * p:128 * (p + 1)], cos_t, sin_t, first_half)
            q_s[p] = (qp.astype(jnp.bfloat16) * 0.125).astype(jnp.bfloat16)
        k = rope_pair(dot_t(h, wk_s[...]), cos_t, sin_t, first_half)
        v = dot_t(h, wv_s[...])
        for s, x in ((k_s, k), (v_s, v)):
            other = pltpu.roll(x, 64, 1)
            s[0, rows, :] = jnp.where(low, x, other).astype(jnp.bfloat16)
            s[1, rows, :] = jnp.where(low, other, x).astype(jnp.bfloat16)

        for at in range(n_blk):
            pl.when(c == at)(functools.partial(attend, at))

        @pl.when(c >= 1)
        def _send():
            send(c - 1)

        @pl.when(c >= 4)
        def _relay():
            relay(c - 4)

        @pl.when(c == 0)
        def _weights():
            for x in loads[4:]:
                x.wait()

        attn = dot_n(o_s[...], wo_s[...]).astype(jnp.bfloat16)
        z = (r_s[...] + attn.astype(jnp.float32)).astype(jnp.bfloat16).astype(jnp.float32)
        r_s[...] = z
        h = norm_rows(z, gain_m)
        for t in range(ff // FT):
            cols = slice(t * FT, (t + 1) * FT)
            gate = 0.5 * dot_n(h, wg_s[:, cols])
            up = dot_n(h, wu_s[:, cols])
            m_s[:, cols] = ((gate + gate * jnp.tanh(gate)) * up).astype(jnp.bfloat16)
        down = dot_n(m_s[...], wd_s[...]).astype(jnp.bfloat16)
        obuf[lax.rem(c, 2)] = (r_s[...] + down.astype(jnp.float32)).astype(jnp.bfloat16)
        keep(c).start()

    send(n_blk - 1)
    for c in range(n_blk - 4, n_blk):
        relay(c)
    for c in range(n_blk):
        arrive(c).wait_send()
        trade(c, out_b, ob, obs, obr).wait_send()
        trade(c, loc_b, lb, lbs, lbr).wait_send()
        to_sib(c).wait()
        to_peer(c).wait_send()
        forward(c).wait()


def layer(span, sends, positions, g_attn, w_q, w_k, w_v, w_o, g_mlp, w_gate, w_up, w_down):
    n_rows, dim = sends[0].shape
    head_dim = w_q.shape[2]
    half_dim = head_dim // 2
    exponent = -2.0 * np.arange(half_dim, dtype=np.float32) / np.float32(head_dim)
    inv_freq = np.power(np.float32(ROPE_BASE), exponent).astype(np.float32)
    freq = jnp.asarray(np.tile(inv_freq, 128 // half_dim)[None, :])
    wq_t = jnp.transpose(w_q, (1, 2, 0)).reshape(dim, dim)
    wk_t = jnp.transpose(w_k, (1, 2, 0)).reshape(128, dim)
    wv_t = jnp.transpose(w_v, (1, 2, 0)).reshape(128, dim)
    wo_t = w_o.reshape(dim, dim)
    bf, f32 = jnp.bfloat16, jnp.float32
    n_blk = n_rows // QB
    ff = w_gate.shape[1]
    rows = jax.ShapeDtypeStruct((n_rows, dim), bf)
    dma = pltpu.SemaphoreType.DMA
    return pl.pallas_call(
        layer_kernel,
        out_shape=[rows, rows, jax.ShapeDtypeStruct((2 * n_rows, dim), bf)],
        in_specs=[SM] + [ANY] * 4 + [VM] * 4 + [ANY] * 7,
        out_specs=[ANY] * 3,
        scratch_shapes=[
            *[pltpu.VMEM((n_rows, dim), bf)] * 5, pltpu.VMEM((QB, dim), f32), pltpu.VMEM((dim // 128, QB, 128), bf),
            pltpu.VMEM((2, n_rows, 128), bf), pltpu.VMEM((2, n_rows, 128), bf), pltpu.VMEM((QB, dim), bf),
            pltpu.VMEM((QB, ff), bf), pltpu.VMEM((2, QB, dim), bf)]
            + [pltpu.VMEM((QB, n_rows), f32)] * 3
            + [pltpu.VMEM((n_rows, 128), f32), pltpu.VMEM((n_rows, 128), f32), pltpu.VMEM((n_rows, 128), jnp.int32),
               pltpu.VMEM((dim, dim), bf), pltpu.VMEM((128, dim), bf), pltpu.VMEM((128, dim), bf), pltpu.VMEM((dim, dim), bf),
               pltpu.VMEM((dim, ff), bf), pltpu.VMEM((dim, ff), bf), pltpu.VMEM((ff, dim), bf), dma((7,))] + [dma((n_blk,))] * 15,
        compiler_params=pltpu.CompilerParams(collective_id=1, has_side_effects=True, vmem_limit_bytes=67000000),
        name="layer",
    )(span, *sends, positions.reshape(-1, 128), freq, g_attn, g_mlp, wq_t, wk_t, wv_t, wo_t, w_gate, w_up, w_down)


CHUNK = 128
MESH_ID = pl.DeviceIdType.MESH
ANY = pl.BlockSpec(memory_space=pl.ANY)
VM = pl.BlockSpec(memory_space=pltpu.VMEM)
SM = pl.BlockSpec(memory_space=pltpu.SMEM)


def meet(devices):
    barrier = pltpu.get_barrier_semaphore()
    for dev in devices:
        pl.semaphore_signal(barrier, inc=1, device_id={"sp": dev}, device_id_type=MESH_ID)
    pl.semaphore_wait(barrier, len(devices))


def push(src, dst, send_sem, recv_sem, dev):
    return pltpu.make_async_remote_copy(src_ref=src, dst_ref=dst, send_sem=send_sem, recv_sem=recv_sem,
                                        device_id={"sp": dev}, device_id_type=MESH_ID)


def share_kernel(n_split, *refs):
    n = (len(refs) - 2) // 2
    ins, outs, send_sems, recv_sems = refs[:n], refs[n:2 * n], refs[-2], refs[-1]
    me = lax.axis_index("sp")
    sib = me + 1 - 2 * lax.rem(me, 2)
    meet([sib])
    copies = []
    for a, b in zip(ins, outs):
        parts = n_split if a.ndim == 2 else 1
        step = a.shape[0] // parts
        for p in range(parts):
            rows = pl.ds(p * step, step)
            copies.append((a.at[rows], b.at[rows]) if parts > 1 else (a, b))
    started = []
    for i, (a, b) in enumerate(copies):
        cp = push(a, b, send_sems.at[i], recv_sems.at[i], sib)
        cp.start()
        started.append(cp)
    for cp in started:
        cp.wait()


def share(arrays, collective_id):
    return pl.pallas_call(
        functools.partial(share_kernel, 4),
        out_shape=[jax.ShapeDtypeStruct(a.shape, a.dtype) for a in arrays],
        in_specs=[ANY] * len(arrays), out_specs=[ANY] * len(arrays),
        scratch_shapes=[pltpu.SemaphoreType.DMA((16,)), pltpu.SemaphoreType.DMA((16,))],
        compiler_params=pltpu.CompilerParams(collective_id=collective_id, has_side_effects=True),
        name="share",
    )(*arrays)


LOAD = 512
FILL = 64
PITCH = 9


def load_table(parts, tab, stage, sems):
    jobs = []
    for ref, lo, hi in parts:
        for i in range(ref.shape[0] // LOAD):
            n = len(jobs)
            copy = pltpu.make_async_copy(ref.at[pl.ds(i * LOAD, LOAD)], stage.at[pl.ds(n * LOAD, LOAD)], sems.at[n])
            if lo is None:
                jobs.append((copy, None, 0, LOAD // FILL))
            else:
                low, high = jnp.maximum(lo - i * LOAD, 0), jnp.minimum(hi - i * LOAD, LOAD)
                jobs.append((copy, low < high, low // FILL, (high + FILL - 1) // FILL))
    for copy, cond, _, _ in jobs:
        if cond is None:
            copy.start()
        else:
            pl.when(cond)(copy.start)
    for n, (copy, cond, low, high) in enumerate(jobs):
        def fill(n=n, copy=copy, low=low, high=high):
            copy.wait()

            @pl.loop(low, high)
            def _blk(i):
                rows = pl.ds(pl.multiple_of(n * LOAD + i * FILL, FILL), FILL)
                first = (n * LOAD + i * FILL) * PITCH
                for j in range(stage.shape[1] // 128):
                    tab[pl.ds(first + j, FILL, stride=PITCH), :] = stage[rows, 128 * j:128 * (j + 1)].astype(jnp.float32)
        if cond is None:
            fill()
        else:
            pl.when(cond)(fill)


UNROLL = 16


def slab(k):
    return pl.ds(pl.multiple_of(k * 8, 8), 8)


def rows_out(lo, hi, src3, stage, base, dst, sem):
    first, last = lo // CHUNK, jnp.where(hi > lo, (hi + CHUNK - 1) // CHUNK, 0)

    def copy(i):
        rows = pl.multiple_of(i * CHUNK, CHUNK)
        return pltpu.make_async_copy(stage.at[pl.ds(base + rows, CHUNK)], dst.at[pl.ds(rows, CHUNK)], sem)

    @pl.loop(first, last)
    def _blk(i):
        rows = pl.ds(pl.multiple_of(base + i * CHUNK, CHUNK), CHUNK)
        for j in range(dst.shape[1] // 128):
            stage[rows, 128 * j:128 * (j + 1)] = src3[pl.ds(i * CHUNK * PITCH + j, CHUNK, stride=PITCH), :].astype(stage.dtype)
        copy(i).start()

    def finish():
        pl.loop(first, last)(lambda i: copy(i).wait())

    return finish


def slab(k):
    return pl.ds(k * PITCH, 8)


def move_run(n, one):
    whole = n // UNROLL

    @pl.loop(0, whole)
    def _grp(i):
        for k in range(UNROLL):
            one(i * UNROLL + k)

    @pl.loop(whole * UNROLL, n)
    def _one(i):
        one(i)


def pick_kernel(perm, so, sl, ro, rl, sl_b, ro_b, own, out_a, out_b, loc_a, loc_b, span, tab, out3, stage, sems, out_sems):
    cap = loc_a.shape[0]
    me = lax.axis_index("sp")
    core = lax.rem(me, 2)
    chip = me // 2
    mate = me + 1 - 2 * core
    far = 2 * (1 - chip)
    load_table([(own, None, None)], tab, stage, sems)
    n_in = rl[far] + rl[far + 1]
    span[0] = (1 - chip) * (cap - n_in)
    span[1] = (1 - chip) * (cap - n_in) + n_in

    def far_row(goal):
        return chip * (cap - sl[goal] - sl_b[goal]) + core * sl_b[goal]

    span[2] = far_row(far + core)
    span[3] = far_row(far + core) + sl[far + core]
    span[4] = ro[me]
    span[5] = ro[me] + sl[me]
    ends = []
    for n, (goal, row, dst) in enumerate([(far + 1 - core, far_row(far + 1 - core), out_b), (far + core, far_row(far + core), out_a),
                                          (mate, ro_b[me], loc_b), (me, ro[me], loc_a)]):
        def one(t, goal=goal, row=row):
            out3[slab(row + t), :] = tab[slab(perm[so[goal] + t]), :]
        move_run(sl[goal], one)
        ends.append(rows_out(row, row + sl[goal], out3, stage, n * cap, dst, out_sems.at[n]))
    for end in ends:
        end()


def back_place_kernel(perm, so, sl, ro, rl, sl_b, ro_b, own, sib, stream, out, tab, out3, stage, sems, out_sems):
    cap = own.shape[0]
    n_tok = out.shape[0]
    me = lax.axis_index("sp")
    core = lax.rem(me, 2)
    chip = me // 2
    mate = me + 1 - 2 * core
    far = 2 * (1 - chip)

    def far_row(goal):
        return chip * (cap - sl[goal] - sl_b[goal]) + core * sl_b[goal]

    runs = [(me, own, ro[me]), (mate, sib, ro_b[me]),
            (far + core, stream.at[pl.ds(0, cap)], far_row(far + core)), (far + 1 - core, stream.at[pl.ds(cap, cap)], far_row(far + 1 - core))]
    load_table([(ref, row, row + sl[goal]) for goal, ref, row in runs], tab, stage, sems)
    for n, (goal, _, row) in enumerate(runs):
        def one(t, goal=goal, row=n * cap + row):
            out3[slab(perm[so[goal] + t]), :] = tab[slab(row + t), :]
        move_run(sl[goal], one)
    sent = so[3] + sl[3]

    def blank(t):
        out3[slab(perm[sent + t]), :] = jnp.zeros((8, 128), jnp.float32)

    move_run(n_tok - sent, blank)
    rows_out(0, n_tok, out3, stage, 0, out, out_sems.at[0])()


def local_call(body, out_shapes, out_specs, n_any, tab_rows, out_rows, stage_rows, dim, name):
    return pl.pallas_call(
        body,
        out_shape=out_shapes,
        in_specs=[SM] * 7 + [ANY] * n_any,
        out_specs=out_specs,
        scratch_shapes=[pltpu.VMEM((tab_rows * PITCH, 128), jnp.float32), pltpu.VMEM((out_rows * PITCH, 128), jnp.float32),
                        pltpu.VMEM((stage_rows, dim), jnp.bfloat16), pltpu.SemaphoreType.DMA((tab_rows // LOAD,)), pltpu.SemaphoreType.DMA((4,))],
        compiler_params=pltpu.CompilerParams(vmem_limit_bytes=66000000),
        name=name,
    )


def solution(mesh):
    row_spec = P(('dp', 'sp'), None)
    vec_spec = P(('dp', 'sp'))
    rep_spec = P()

    def per_device(hidden, tok_perm, send_off, send_len, recv_off, recv_len, recv_doc, recv_pos, g_attn, w_q, w_k, w_v, w_o, g_mlp, w_gate, w_up, w_down):
        n_tok, dim = hidden.shape
        cap = recv_doc.shape[0]
        plan = [tok_perm, send_off, send_len, recv_off, recv_len]
        plan += share([send_len, recv_off], 0)
        rows_bf = jax.ShapeDtypeStruct((cap, dim), hidden.dtype)
        outs = [rows_bf] * 4 + [jax.ShapeDtypeStruct((6,), jnp.int32)]
        out_a, out_b, loc_a, loc_b, span = local_call(pick_kernel, outs, [ANY] * 4 + [SM], 1, n_tok, cap, 4 * cap, dim, "pick")(*plan, hidden)
        done, sib_done, returned = layer(span, (out_a, out_b, loc_a, loc_b), recv_pos, g_attn, w_q, w_k, w_v, w_o, g_mlp, w_gate, w_up, w_down)
        out = jax.ShapeDtypeStruct((n_tok, dim), hidden.dtype)
        return local_call(back_place_kernel, out, ANY, 3, 4 * cap, n_tok, 4 * cap, dim, "back_place")(*plan, done, sib_done, returned)

    return jax.shard_map(per_device, mesh=mesh, in_specs=(row_spec,) + (vec_spec,) * 7 + (rep_spec,) * 9, out_specs=row_spec, check_vma=False)
```

```python
import functools

import jax
import jax.numpy as jnp
import numpy as np
from jax import lax
from jax.experimental import pallas as pl
from jax.experimental.pallas import tpu as pltpu
from jax.sharding import PartitionSpec as P

ROPE_BASE = 500000.0
NORM_EPS = 1e-5
ROWS = 512
QB = 256
END = 128
FT = 256


def norm_rows(rows_f, gain):
    inv = lax.rsqrt(jnp.mean(rows_f * rows_f, axis=-1, keepdims=True) + NORM_EPS)
    return (rows_f * inv * gain).astype(jnp.bfloat16)


def rope_pair(x, cos_t, sin_t, first_half):
    swapped = jnp.where(first_half, pltpu.roll(x, 96, 1), pltpu.roll(x, 32, 1))
    return x * cos_t + swapped * sin_t


def dot_t(a, b):
    return lax.dot_general(a, b, (((1,), (1,)), ((), ())), preferred_element_type=jnp.float32)


def dot_n(a, b):
    return jnp.dot(a, b, preferred_element_type=jnp.float32)


def layer_kernel(span_ref, out_a, out_b, loc_a, loc_b, pos_ref, freq_ref, ga_ref, gm_ref, wq_h, wk_h, wv_h, wo_h, wg_h, wu_h, wd_h, own, sib_out, far,
                 rbuf, oa, ob, la, lb, r_s, q_s, k_s, v_s, o_s, m_s, obuf, sa, sb, bias, cos_s, sin_s, start_s, wq_s, wk_s, wv_s, wo_s, wg_s, wu_s, wd_s, sems,
                 as_, ar, ps, pr, ss, sr, fs, fr, own_sem, oas, obs, obr, las, lbs, lbr):
    n_rows, dim = loc_a.shape
    n_pairs = dim // 128
    n_blk = (n_rows - 2 * END) // QB + 2
    final = n_blk - 1
    ff = wg_s.shape[1]
    me = lax.axis_index("sp")
    sib = me + 1 - 2 * lax.rem(me, 2)
    peer = lax.rem(me + 2, 4)
    loads = [pltpu.make_async_copy(a, b, sems.at[i]) for i, (a, b) in enumerate(
        [(wq_h, wq_s), (wk_h, wk_s), (wv_h, wv_s), (wo_h, wo_s), (wg_h, wg_s), (wu_h, wu_s), (wd_h, wd_s)])]
    meet([sib, peer])

    def rows_at(c):
        if isinstance(c, int) and c in (0, final):
            return pl.ds(0 if c == 0 else n_rows - END, END)
        return pl.ds(pl.multiple_of(END + (c - 1) * QB, END), QB)

    def arrive(c):
        return push(ob.at[rows_at(c)], rbuf.at[rows_at(c)], as_.at[c], ar.at[c], peer)

    def to_peer(c):
        return push(own.at[rows_at(c)], far.at[rows_at(c)], ps.at[c], pr.at[c], peer)

    def to_sib(c):
        return push(own.at[rows_at(c)], sib_out.at[rows_at(c)], ss.at[c], sr.at[c], sib)

    def forward(c):
        rows = rows_at(c)
        return push(far.at[rows], far.at[pl.ds(pl.multiple_of(n_rows + rows.start, END), rows.size)], fs.at[c], fr.at[c], sib)

    def keep(c):
        rows = rows_at(c)
        return pltpu.make_async_copy(obuf.at[lax.rem(c, 2), pl.ds(0, rows.size)], own.at[rows], own_sem.at[c])

    def send(c):
        keep(c).wait()
        to_peer(c).start()
        to_sib(c).start()

    def relay(c):
        to_peer(c).wait_recv()
        forward(c).start()

    def fetch(c, src, dst, sem):
        return pltpu.make_async_copy(src.at[rows_at(c)], dst.at[rows_at(c)], sem.at[c])

    def trade(c, src, dst, send_sem, recv_sem):
        return push(src.at[rows_at(c)], dst.at[rows_at(c)], send_sem.at[c], recv_sem.at[c], sib)

    def select(c, lo, hi, yes, no):
        rows = rows_at(c)
        row = rows.start + lax.broadcasted_iota(jnp.int32, (rows.size, dim), 0)
        return jnp.where((row >= lo) & (row < hi), yes.astype(jnp.float32), no.astype(jnp.float32))

    for c in range(n_blk):
        trade(c, out_b, ob, obs, obr).start()
        fetch(c, out_a, oa, oas).start()
    for c in range(n_blk):
        trade(c, loc_b, lb, lbs, lbr).start()
        fetch(c, loc_a, la, las).start()
    for c in loads:
        c.start()
    for c in range(n_blk):
        trade(c, out_b, ob, obs, obr).wait_recv()
        fetch(c, out_a, oa, oas).wait()
        rows = rows_at(c)
        ob[rows, :] = select(c, span_ref[2], span_ref[3], oa[rows, :], ob[rows, :]).astype(jnp.bfloat16)
        if c:
            arrive(c - 1).start()
    gain_a = ga_ref[...].astype(jnp.float32).reshape(1, dim)
    gain_m = gm_ref[...].astype(jnp.float32).reshape(1, dim)
    first, last = span_ref[0], span_ref[1]
    tile_lane = lax.broadcasted_iota(jnp.int32, (128, 128), 1)
    tile_row = lax.broadcasted_iota(jnp.int32, (128, 128), 0)
    sign = jnp.where(tile_lane % 64 < 32, -1.0, 1.0)
    for t in range(n_rows // 128):
        rows = slice(128 * t, 128 * (t + 1))
        pos = jnp.transpose(jnp.broadcast_to(pos_ref[t:t + 1, :].astype(jnp.float32), (128, 128)))
        angle = pos * freq_ref[...]
        cos_s[rows, :] = jnp.cos(angle)
        sin_s[rows, :] = jnp.sin(angle) * sign
        start_s[rows, :] = 128 * t + tile_row - pos.astype(jnp.int32)
        if t == 0:
            arrive(n_blk - 1).start()
    for c in loads[:4]:
        c.wait()

    def attend(at, size):
        length = at + size
        mine = pl.ds(0, size)
        lane = lax.broadcasted_iota(jnp.int32, (size, 128), 1)
        low = lane < 64
        start = start_s[at:length, :]
        row = at + lax.broadcasted_iota(jnp.int32, (size, 128), 0)
        for t in range(length // 128):
            col = 128 * t + lane
            bias[mine, 128 * t:128 * (t + 1)] = jnp.where((col >= start) & (col <= row), 3e38, -1e30)

        def scores(p, half, dst):
            qp = q_s[p, mine, :]
            qh = jnp.where(low if half == 0 else ~low, qp, jnp.zeros_like(qp))
            s = jnp.minimum(dot_t(qh, k_s[(2 * p + half) // 7, :length, :]), bias[mine, :length])
            dst[mine, :length] = s
            return jnp.max(s, axis=1, keepdims=True)

        def soft(p, half, src, top):
            e = jnp.exp(src[mine, :length] - top)
            total = jnp.sum(e, axis=1, keepdims=True)
            return dot_n(e.astype(jnp.bfloat16), v_s[(2 * p + half) // 7, :length, :]) / total

        def pair(p, top_a):
            top_b = scores(p, 1, sb)
            out_a = soft(p, 0, sa, top_a)
            top_a = scores(jnp.minimum(p + 1, n_pairs - 1), 0, sa)
            out_b = soft(p, 1, sb, top_b)
            o_s[mine, pl.ds(pl.multiple_of(p * 128, 128), 128)] = jnp.where(low, out_a, out_b).astype(jnp.bfloat16)
            return top_a

        lax.fori_loop(0, n_pairs, pair, scores(0, 0, sa))

    def block(c, attention, before_mlp):
        rows = rows_at(c)
        size = rows.size
        mine = pl.ds(0, size)
        lane = lax.broadcasted_iota(jnp.int32, (size, 128), 1)
        first_half = lane % 64 < 32
        low = lane < 64
        trade(c, loc_b, lb, lbs, lbr).wait_recv()
        fetch(c, loc_a, la, las).wait()
        arrive(c).wait_recv()
        r = select(c, first, last, rbuf[rows, :], select(c, span_ref[4], span_ref[5], la[rows, :], lb[rows, :]))
        r_s[mine, :] = r
        h = norm_rows(r, gain_a)
        cos_t = cos_s[rows, :]
        sin_t = sin_s[rows, :]
        q = dot_t(h, wq_s[...])
        for p in range(n_pairs):
            qp = rope_pair(q[:, 128 * p:128 * (p + 1)], cos_t, sin_t, first_half)
            q_s[p, mine, :] = (qp.astype(jnp.bfloat16) * 0.125).astype(jnp.bfloat16)
        k = rope_pair(dot_t(h, wk_s[...]), cos_t, sin_t, first_half)
        v = dot_t(h, wv_s[...])
        for s, x in ((k_s, k), (v_s, v)):
            other = pltpu.roll(x, 64, 1)
            s[0, rows, :] = jnp.where(low, x, other).astype(jnp.bfloat16)
            s[1, rows, :] = jnp.where(low, other, x).astype(jnp.bfloat16)

        attention()
        before_mlp()
        attn = dot_n(o_s[mine, :], wo_s[...]).astype(jnp.bfloat16)
        z = (r_s[mine, :] + attn.astype(jnp.float32)).astype(jnp.bfloat16).astype(jnp.float32)
        r_s[mine, :] = z
        h = norm_rows(z, gain_m)
        for t in range(ff // FT):
            cols = slice(t * FT, (t + 1) * FT)
            gate = 0.5 * dot_n(h, wg_s[:, cols])
            up = dot_n(h, wu_s[:, cols])
            m_s[mine, cols] = ((gate + gate * jnp.tanh(gate)) * up).astype(jnp.bfloat16)
        down = dot_n(m_s[mine, :], wd_s[...]).astype(jnp.bfloat16)
        obuf[lax.rem(c, 2), mine, :] = (r_s[mine, :] + down.astype(jnp.float32)).astype(jnp.bfloat16)
        keep(c).start()

    def weights():
        for x in loads[4:]:
            x.wait()

    def send_before(c):
        @pl.when(c == 1)
        def _first():
            send(0)

        @pl.when(c > 1)
        def _other():
            send(c - 1)

    def ending():
        send(final - 1)
        relay(0)
        relay(1)
        relay(2)

    block(0, lambda: attend(0, END), weights)

    @pl.loop(1, final)
    def _block(c):
        def attention():
            for at in range(1, final):
                pl.when(c == at)(functools.partial(attend, END + (at - 1) * QB, QB))

        block(c, attention, lambda: send_before(c))

    block(final, lambda: attend(n_rows - END, END), ending)
    send(final)
    for c in range(3, n_blk):
        relay(c)
    for c in range(n_blk):
        arrive(c).wait_send()
        trade(c, out_b, ob, obs, obr).wait_send()
        trade(c, loc_b, lb, lbs, lbr).wait_send()
        to_sib(c).wait()
        to_peer(c).wait_send()
        forward(c).wait()


def layer(span, sends, positions, g_attn, w_q, w_k, w_v, w_o, g_mlp, w_gate, w_up, w_down):
    n_rows, dim = sends[0].shape
    head_dim = w_q.shape[2]
    half_dim = head_dim // 2
    exponent = -2.0 * np.arange(half_dim, dtype=np.float32) / np.float32(head_dim)
    inv_freq = np.power(np.float32(ROPE_BASE), exponent).astype(np.float32)
    freq = jnp.asarray(np.tile(inv_freq, 128 // half_dim)[None, :])
    wq_t = jnp.transpose(w_q, (1, 2, 0)).reshape(dim, dim)
    wk_t = jnp.transpose(w_k, (1, 2, 0)).reshape(128, dim)
    wv_t = jnp.transpose(w_v, (1, 2, 0)).reshape(128, dim)
    wo_t = w_o.reshape(dim, dim)
    bf, f32 = jnp.bfloat16, jnp.float32
    n_blk = (n_rows - 2 * END) // QB + 2
    ff = w_gate.shape[1]
    rows = jax.ShapeDtypeStruct((n_rows, dim), bf)
    dma = pltpu.SemaphoreType.DMA
    return pl.pallas_call(
        layer_kernel,
        out_shape=[rows, rows, jax.ShapeDtypeStruct((2 * n_rows, dim), bf)],
        in_specs=[SM] + [ANY] * 4 + [VM] * 4 + [ANY] * 7,
        out_specs=[ANY] * 3,
        scratch_shapes=[
            *[pltpu.VMEM((n_rows, dim), bf)] * 5, pltpu.VMEM((QB, dim), f32), pltpu.VMEM((dim // 128, QB, 128), bf),
            pltpu.VMEM((2, n_rows, 128), bf), pltpu.VMEM((2, n_rows, 128), bf), pltpu.VMEM((QB, dim), bf),
            pltpu.VMEM((QB, ff), bf), pltpu.VMEM((2, QB, dim), bf)]
            + [pltpu.VMEM((QB, n_rows), f32)] * 3
            + [pltpu.VMEM((n_rows, 128), f32), pltpu.VMEM((n_rows, 128), f32), pltpu.VMEM((n_rows, 128), jnp.int32),
               pltpu.VMEM((dim, dim), bf), pltpu.VMEM((128, dim), bf), pltpu.VMEM((128, dim), bf), pltpu.VMEM((dim, dim), bf),
               pltpu.VMEM((dim, ff), bf), pltpu.VMEM((dim, ff), bf), pltpu.VMEM((ff, dim), bf), dma((7,))] + [dma((n_blk,))] * 15,
        compiler_params=pltpu.CompilerParams(collective_id=1, has_side_effects=True, vmem_limit_bytes=67000000),
        name="layer",
    )(span, *sends, positions.reshape(-1, 128), freq, g_attn, g_mlp, wq_t, wk_t, wv_t, wo_t, w_gate, w_up, w_down)


CHUNK = 128
MESH_ID = pl.DeviceIdType.MESH
ANY = pl.BlockSpec(memory_space=pl.ANY)
VM = pl.BlockSpec(memory_space=pltpu.VMEM)
SM = pl.BlockSpec(memory_space=pltpu.SMEM)


def meet(devices):
    barrier = pltpu.get_barrier_semaphore()
    for dev in devices:
        pl.semaphore_signal(barrier, inc=1, device_id={"sp": dev}, device_id_type=MESH_ID)
    pl.semaphore_wait(barrier, len(devices))


def push(src, dst, send_sem, recv_sem, dev):
    return pltpu.make_async_remote_copy(src_ref=src, dst_ref=dst, send_sem=send_sem, recv_sem=recv_sem,
                                        device_id={"sp": dev}, device_id_type=MESH_ID)


def share_kernel(n_split, *refs):
    n = (len(refs) - 2) // 2
    ins, outs, send_sems, recv_sems = refs[:n], refs[n:2 * n], refs[-2], refs[-1]
    me = lax.axis_index("sp")
    sib = me + 1 - 2 * lax.rem(me, 2)
    meet([sib])
    copies = []
    for a, b in zip(ins, outs):
        parts = n_split if a.ndim == 2 else 1
        step = a.shape[0] // parts
        for p in range(parts):
            rows = pl.ds(p * step, step)
            copies.append((a.at[rows], b.at[rows]) if parts > 1 else (a, b))
    started = []
    for i, (a, b) in enumerate(copies):
        cp = push(a, b, send_sems.at[i], recv_sems.at[i], sib)
        cp.start()
        started.append(cp)
    for cp in started:
        cp.wait()


def share(arrays, collective_id):
    return pl.pallas_call(
        functools.partial(share_kernel, 4),
        out_shape=[jax.ShapeDtypeStruct(a.shape, a.dtype) for a in arrays],
        in_specs=[ANY] * len(arrays), out_specs=[ANY] * len(arrays),
        scratch_shapes=[pltpu.SemaphoreType.DMA((16,)), pltpu.SemaphoreType.DMA((16,))],
        compiler_params=pltpu.CompilerParams(collective_id=collective_id, has_side_effects=True),
        name="share",
    )(*arrays)


LOAD = 512
FILL = 64
PITCH = 9


def load_table(parts, tab, stage, sems):
    jobs = []
    for ref, lo, hi in parts:
        for i in range(ref.shape[0] // LOAD):
            n = len(jobs)
            copy = pltpu.make_async_copy(ref.at[pl.ds(i * LOAD, LOAD)], stage.at[pl.ds(n * LOAD, LOAD)], sems.at[n])
            if lo is None:
                jobs.append((copy, None, 0, LOAD // FILL))
            else:
                low, high = jnp.maximum(lo - i * LOAD, 0), jnp.minimum(hi - i * LOAD, LOAD)
                jobs.append((copy, low < high, low // FILL, (high + FILL - 1) // FILL))
    for copy, cond, _, _ in jobs:
        if cond is None:
            copy.start()
        else:
            pl.when(cond)(copy.start)
    for n, (copy, cond, low, high) in enumerate(jobs):
        def fill(n=n, copy=copy, low=low, high=high):
            copy.wait()

            @pl.loop(low, high)
            def _blk(i):
                rows = pl.ds(pl.multiple_of(n * LOAD + i * FILL, FILL), FILL)
                first = (n * LOAD + i * FILL) * PITCH
                for j in range(stage.shape[1] // 128):
                    tab[pl.ds(first + j, FILL, stride=PITCH), :] = stage[rows, 128 * j:128 * (j + 1)].astype(jnp.float32)
        if cond is None:
            fill()
        else:
            pl.when(cond)(fill)


UNROLL = 16


def slab(k):
    return pl.ds(pl.multiple_of(k * 8, 8), 8)


def rows_out(lo, hi, src3, stage, base, dst, sem):
    first, last = lo // CHUNK, jnp.where(hi > lo, (hi + CHUNK - 1) // CHUNK, 0)

    def copy(i):
        rows = pl.multiple_of(i * CHUNK, CHUNK)
        return pltpu.make_async_copy(stage.at[pl.ds(base + rows, CHUNK)], dst.at[pl.ds(rows, CHUNK)], sem)

    @pl.loop(first, last)
    def _blk(i):
        rows = pl.ds(pl.multiple_of(base + i * CHUNK, CHUNK), CHUNK)
        for j in range(dst.shape[1] // 128):
            stage[rows, 128 * j:128 * (j + 1)] = src3[pl.ds(i * CHUNK * PITCH + j, CHUNK, stride=PITCH), :].astype(stage.dtype)
        copy(i).start()

    def finish():
        pl.loop(first, last)(lambda i: copy(i).wait())

    return finish


def slab(k):
    return pl.ds(k * PITCH, 8)


def move_run(n, one):
    whole = n // UNROLL

    @pl.loop(0, whole)
    def _grp(i):
        for k in range(UNROLL):
            one(i * UNROLL + k)

    @pl.loop(whole * UNROLL, n)
    def _one(i):
        one(i)


def pick_kernel(perm, so, sl, ro, rl, sl_b, ro_b, own, out_a, out_b, loc_a, loc_b, span, tab, out3, stage, sems, out_sems):
    cap = loc_a.shape[0]
    me = lax.axis_index("sp")
    core = lax.rem(me, 2)
    chip = me // 2
    mate = me + 1 - 2 * core
    far = 2 * (1 - chip)
    load_table([(own, None, None)], tab, stage, sems)
    n_in = rl[far] + rl[far + 1]
    span[0] = (1 - chip) * (cap - n_in)
    span[1] = (1 - chip) * (cap - n_in) + n_in

    def far_row(goal):
        return chip * (cap - sl[goal] - sl_b[goal]) + core * sl_b[goal]

    span[2] = far_row(far + core)
    span[3] = far_row(far + core) + sl[far + core]
    span[4] = ro[me]
    span[5] = ro[me] + sl[me]
    ends = []
    for n, (goal, row, dst) in enumerate([(far + 1 - core, far_row(far + 1 - core), out_b), (far + core, far_row(far + core), out_a),
                                          (mate, ro_b[me], loc_b), (me, ro[me], loc_a)]):
        def one(t, goal=goal, row=row):
            out3[slab(row + t), :] = tab[slab(perm[so[goal] + t]), :]
        move_run(sl[goal], one)
        ends.append(rows_out(row, row + sl[goal], out3, stage, n * cap, dst, out_sems.at[n]))
    for end in ends:
        end()


def back_place_kernel(perm, so, sl, ro, rl, sl_b, ro_b, own, sib, stream, out, tab, out3, stage, sems, out_sems):
    cap = own.shape[0]
    n_tok = out.shape[0]
    me = lax.axis_index("sp")
    core = lax.rem(me, 2)
    chip = me // 2
    mate = me + 1 - 2 * core
    far = 2 * (1 - chip)

    def far_row(goal):
        return chip * (cap - sl[goal] - sl_b[goal]) + core * sl_b[goal]

    runs = [(me, own, ro[me]), (mate, sib, ro_b[me]),
            (far + core, stream.at[pl.ds(0, cap)], far_row(far + core)), (far + 1 - core, stream.at[pl.ds(cap, cap)], far_row(far + 1 - core))]
    load_table([(ref, row, row + sl[goal]) for goal, ref, row in runs], tab, stage, sems)
    for n, (goal, _, row) in enumerate(runs):
        def one(t, goal=goal, row=n * cap + row):
            out3[slab(perm[so[goal] + t]), :] = tab[slab(row + t), :]
        move_run(sl[goal], one)
    sent = so[3] + sl[3]

    def blank(t):
        out3[slab(perm[sent + t]), :] = jnp.zeros((8, 128), jnp.float32)

    move_run(n_tok - sent, blank)
    rows_out(0, n_tok, out3, stage, 0, out, out_sems.at[0])()


def local_call(body, out_shapes, out_specs, n_any, tab_rows, out_rows, stage_rows, dim, name):
    return pl.pallas_call(
        body,
        out_shape=out_shapes,
        in_specs=[SM] * 7 + [ANY] * n_any,
        out_specs=out_specs,
        scratch_shapes=[pltpu.VMEM((tab_rows * PITCH, 128), jnp.float32), pltpu.VMEM((out_rows * PITCH, 128), jnp.float32),
                        pltpu.VMEM((stage_rows, dim), jnp.bfloat16), pltpu.SemaphoreType.DMA((tab_rows // LOAD,)), pltpu.SemaphoreType.DMA((4,))],
        compiler_params=pltpu.CompilerParams(vmem_limit_bytes=66000000),
        name=name,
    )


def solution(mesh):
    row_spec = P(('dp', 'sp'), None)
    vec_spec = P(('dp', 'sp'))
    rep_spec = P()

    def per_device(hidden, tok_perm, send_off, send_len, recv_off, recv_len, recv_doc, recv_pos, g_attn, w_q, w_k, w_v, w_o, g_mlp, w_gate, w_up, w_down):
        n_tok, dim = hidden.shape
        cap = recv_doc.shape[0]
        plan = [tok_perm, send_off, send_len, recv_off, recv_len]
        plan += share([send_len, recv_off], 0)
        rows_bf = jax.ShapeDtypeStruct((cap, dim), hidden.dtype)
        outs = [rows_bf] * 4 + [jax.ShapeDtypeStruct((6,), jnp.int32)]
        out_a, out_b, loc_a, loc_b, span = local_call(pick_kernel, outs, [ANY] * 4 + [SM], 1, n_tok, cap, 4 * cap, dim, "pick")(*plan, hidden)
        done, sib_done, returned = layer(span, (out_a, out_b, loc_a, loc_b), recv_pos, g_attn, w_q, w_k, w_v, w_o, g_mlp, w_gate, w_up, w_down)
        out = jax.ShapeDtypeStruct((n_tok, dim), hidden.dtype)
        return local_call(back_place_kernel, out, ANY, 3, 4 * cap, n_tok, 4 * cap, dim, "back_place")(*plan, done, sib_done, returned)

    return jax.shard_map(per_device, mesh=mesh, in_specs=(row_spec,) + (vec_spec,) * 7 + (rep_spec,) * 9, out_specs=row_spec, check_vma=False)
```

```python
import functools

import jax
import jax.numpy as jnp
import numpy as np
from jax import lax
from jax.experimental import pallas as pl
from jax.experimental.pallas import tpu as pltpu
from jax.sharding import PartitionSpec as P

ROPE_BASE = 500000.0
NORM_EPS = 1e-5
ROWS = 512
QB = 256
END = 128
WIDE = 256
FT = 256


def norm_rows(rows_f, gain):
    inv = lax.rsqrt(jnp.mean(rows_f * rows_f, axis=-1, keepdims=True) + NORM_EPS)
    return (rows_f * inv * gain).astype(jnp.bfloat16)


def rope_pair(x, cos_t, sin_t, first_half):
    swapped = jnp.where(first_half, pltpu.roll(x, 96, 1), pltpu.roll(x, 32, 1))
    return x * cos_t + swapped * sin_t


def dot_t(a, b):
    return lax.dot_general(a, b, (((1,), (1,)), ((), ())), preferred_element_type=jnp.float32)


def dot_n(a, b):
    return jnp.dot(a, b, preferred_element_type=jnp.float32)


def layer_kernel(span_ref, out_a, out_b, loc_a, loc_b, pos_ref, freq_ref, ga_ref, gm_ref, wq_h, wk_h, wv_h, wo_h, wg_h, wu_h, wd_h, own, sib_out, far,
                 rbuf, oa, ob, la, lb, r_s, q_s, k_s, v_s, o_s, m_s, obuf, sa, sb, bias, cos_s, sin_s, start_s, wq_s, wk_s, wv_s, wo_s, wg_s, wu_s, wd_s, sems,
                 as_, ar, ps, pr, ss, sr, fs, fr, own_sem, oas, obs, obr, las, lbs, lbr):
    n_rows, dim = loc_a.shape
    n_pairs = dim // 128
    n_blk = (n_rows - 2 * END) // QB + 2
    final = n_blk - 1
    ff = wg_s.shape[1]
    me = lax.axis_index("sp")
    sib = me + 1 - 2 * lax.rem(me, 2)
    peer = lax.rem(me + 2, 4)
    loads = [pltpu.make_async_copy(a, b, sems.at[i]) for i, (a, b) in enumerate(
        [(wq_h, wq_s), (wk_h, wk_s), (wv_h, wv_s), (wo_h, wo_s), (wg_h, wg_s), (wu_h, wu_s), (wd_h, wd_s)])]
    meet([sib, peer])

    def rows_at(c):
        if isinstance(c, int) and c in (0, final):
            return pl.ds(0 if c == 0 else n_rows - END, END)
        return pl.ds(pl.multiple_of(END + (c - 1) * QB, END), QB)

    def arrive(c):
        return push(ob.at[rows_at(c)], rbuf.at[rows_at(c)], as_.at[c], ar.at[c], peer)

    def to_peer(c):
        return push(own.at[rows_at(c)], far.at[rows_at(c)], ps.at[c], pr.at[c], peer)

    def to_sib(c):
        return push(own.at[rows_at(c)], sib_out.at[rows_at(c)], ss.at[c], sr.at[c], sib)

    def forward(c):
        rows = rows_at(c)
        return push(far.at[rows], far.at[pl.ds(pl.multiple_of(n_rows + rows.start, END), rows.size)], fs.at[c], fr.at[c], sib)

    def keep(c):
        rows = rows_at(c)
        return pltpu.make_async_copy(obuf.at[lax.rem(c, 2), pl.ds(0, rows.size)], own.at[rows], own_sem.at[c])

    def send(c):
        keep(c).wait()
        to_peer(c).start()
        to_sib(c).start()

    def relay(c):
        to_peer(c).wait_recv()
        forward(c).start()

    def fetch(c, src, dst, sem):
        return pltpu.make_async_copy(src.at[rows_at(c)], dst.at[rows_at(c)], sem.at[c])

    def trade(c, src, dst, send_sem, recv_sem):
        return push(src.at[rows_at(c)], dst.at[rows_at(c)], send_sem.at[c], recv_sem.at[c], sib)

    def select(c, lo, hi, yes, no):
        rows = rows_at(c)
        row = rows.start + lax.broadcasted_iota(jnp.int32, (rows.size, dim), 0)
        return jnp.where((row >= lo) & (row < hi), yes.astype(jnp.float32), no.astype(jnp.float32))

    for c in range(n_blk):
        trade(c, out_b, ob, obs, obr).start()
        fetch(c, out_a, oa, oas).start()
    for c in range(n_blk):
        trade(c, loc_b, lb, lbs, lbr).start()
        fetch(c, loc_a, la, las).start()
    for c in range(n_blk):
        trade(c, out_b, ob, obs, obr).wait_recv()
        fetch(c, out_a, oa, oas).wait()
        rows = rows_at(c)
        ob[rows, :] = select(c, span_ref[2], span_ref[3], oa[rows, :], ob[rows, :]).astype(jnp.bfloat16)
        if c:
            arrive(c - 1).start()
        if c == 1:
            for x in loads:
                x.start()
    gain_a = ga_ref[...].astype(jnp.float32).reshape(1, dim)
    gain_m = gm_ref[...].astype(jnp.float32).reshape(1, dim)
    first, last = span_ref[0], span_ref[1]
    tile_lane = lax.broadcasted_iota(jnp.int32, (128, 128), 1)
    tile_row = lax.broadcasted_iota(jnp.int32, (128, 128), 0)
    sign = jnp.where(tile_lane % 64 < 32, -1.0, 1.0)
    for t in range(n_rows // 128):
        rows = slice(128 * t, 128 * (t + 1))
        pos = jnp.transpose(jnp.broadcast_to(pos_ref[t:t + 1, :].astype(jnp.float32), (128, 128)))
        angle = pos * freq_ref[...]
        cos_s[rows, :] = jnp.cos(angle)
        sin_s[rows, :] = jnp.sin(angle) * sign
        start_s[rows, :] = 128 * t + tile_row - pos.astype(jnp.int32)
        if t == 0:
            arrive(n_blk - 1).start()
    for c in loads[:4]:
        c.wait()

    def attend(at, size):
        length = at + size
        mine = pl.ds(0, size)
        lane = lax.broadcasted_iota(jnp.int32, (size, 128), 1)
        low = lane < 64
        start = start_s[at:length, :]
        row = at + lax.broadcasted_iota(jnp.int32, (size, 128), 0)
        for t in range(length // 128):
            col = 128 * t + lane
            bias[mine, 128 * t:128 * (t + 1)] = jnp.where((col >= start) & (col <= row), 3e38, -1e30)

        def scores(p, half, dst):
            qp = q_s[p, mine, :]
            qh = jnp.where(low if half == 0 else ~low, qp, jnp.zeros_like(qp))
            top = jnp.full((size, 128), -3e38, jnp.float32)
            for lo in range(0, length, WIDE):
                hi = min(lo + WIDE, length)
                s = jnp.minimum(dot_t(qh, k_s[(2 * p + half) // 7, lo:hi, :]), bias[mine, lo:hi])
                dst[mine, lo:hi] = s
                for t in range(0, hi - lo, 128):
                    top = jnp.maximum(top, s[:, t:t + 128])
            return jnp.max(top, axis=1, keepdims=True)

        def soft(p, half, src, top):
            total = jnp.zeros((size, 128), jnp.float32)
            out = jnp.zeros((size, 128), jnp.float32)
            for lo in range(0, length, WIDE):
                hi = min(lo + WIDE, length)
                e = jnp.exp(src[mine, lo:hi] - top)
                for t in range(0, hi - lo, 128):
                    total += e[:, t:t + 128]
                out += dot_n(e.astype(jnp.bfloat16), v_s[(2 * p + half) // 7, lo:hi, :])
            return out / jnp.sum(total, axis=1, keepdims=True)

        def pair(p, top_a):
            top_b = scores(p, 1, sb)
            out_a = soft(p, 0, sa, top_a)
            top_a = scores(jnp.minimum(p + 1, n_pairs - 1), 0, sa)
            out_b = soft(p, 1, sb, top_b)
            o_s[mine, pl.ds(pl.multiple_of(p * 128, 128), 128)] = jnp.where(low, out_a, out_b).astype(jnp.bfloat16)
            return top_a

        lax.fori_loop(0, n_pairs, pair, scores(0, 0, sa))

    def block(c, attention, before_mlp):
        rows = rows_at(c)
        size = rows.size
        mine = pl.ds(0, size)
        lane = lax.broadcasted_iota(jnp.int32, (size, 128), 1)
        first_half = lane % 64 < 32
        low = lane < 64
        trade(c, loc_b, lb, lbs, lbr).wait_recv()
        fetch(c, loc_a, la, las).wait()
        arrive(c).wait_recv()
        r = select(c, first, last, rbuf[rows, :], select(c, span_ref[4], span_ref[5], la[rows, :], lb[rows, :]))
        r_s[mine, :] = r
        h = norm_rows(r, gain_a)
        cos_t = cos_s[rows, :]
        sin_t = sin_s[rows, :]
        q = dot_t(h, wq_s[...])
        for p in range(n_pairs):
            qp = rope_pair(q[:, 128 * p:128 * (p + 1)], cos_t, sin_t, first_half)
            q_s[p, mine, :] = (qp.astype(jnp.bfloat16) * 0.125).astype(jnp.bfloat16)
        k = rope_pair(dot_t(h, wk_s[...]), cos_t, sin_t, first_half)
        v = dot_t(h, wv_s[...])
        for s, x in ((k_s, k), (v_s, v)):
            other = pltpu.roll(x, 64, 1)
            s[0, rows, :] = jnp.where(low, x, other).astype(jnp.bfloat16)
            s[1, rows, :] = jnp.where(low, other, x).astype(jnp.bfloat16)

        attention()
        before_mlp()
        attn = dot_n(o_s[mine, :], wo_s[...]).astype(jnp.bfloat16)
        z = (r_s[mine, :] + attn.astype(jnp.float32)).astype(jnp.bfloat16).astype(jnp.float32)
        r_s[mine, :] = z
        h = norm_rows(z, gain_m)
        for t in range(ff // FT):
            cols = slice(t * FT, (t + 1) * FT)
            gate = 0.5 * dot_n(h, wg_s[:, cols])
            up = dot_n(h, wu_s[:, cols])
            m_s[mine, cols] = ((gate + gate * jnp.tanh(gate)) * up).astype(jnp.bfloat16)
        down = dot_n(m_s[mine, :], wd_s[...]).astype(jnp.bfloat16)
        obuf[lax.rem(c, 2), mine, :] = (r_s[mine, :] + down.astype(jnp.float32)).astype(jnp.bfloat16)
        keep(c).start()

    def weights():
        for x in loads[4:]:
            x.wait()

    def send_before(c):
        @pl.when(c == 1)
        def _first():
            send(0)

        @pl.when(c > 1)
        def _other():
            send(c - 1)

    def ending():
        send(final - 1)
        relay(0)
        relay(1)
        relay(2)

    block(0, lambda: attend(0, END), weights)

    @pl.loop(1, final)
    def _block(c):
        def attention():
            for at in range(1, final):
                pl.when(c == at)(functools.partial(attend, END + (at - 1) * QB, QB))

        block(c, attention, lambda: send_before(c))

    block(final, lambda: attend(n_rows - END, END), ending)
    send(final)
    for c in range(3, n_blk):
        relay(c)
    for c in range(n_blk):
        arrive(c).wait_send()
        trade(c, out_b, ob, obs, obr).wait_send()
        trade(c, loc_b, lb, lbs, lbr).wait_send()
        to_sib(c).wait()
        to_peer(c).wait_send()
        forward(c).wait()


def layer(span, sends, positions, g_attn, w_q, w_k, w_v, w_o, g_mlp, w_gate, w_up, w_down):
    n_rows, dim = sends[0].shape
    head_dim = w_q.shape[2]
    half_dim = head_dim // 2
    exponent = -2.0 * np.arange(half_dim, dtype=np.float32) / np.float32(head_dim)
    inv_freq = np.power(np.float32(ROPE_BASE), exponent).astype(np.float32)
    freq = jnp.asarray(np.tile(inv_freq, 128 // half_dim)[None, :])
    wq_t = jnp.transpose(w_q, (1, 2, 0)).reshape(dim, dim)
    wk_t = jnp.transpose(w_k, (1, 2, 0)).reshape(128, dim)
    wv_t = jnp.transpose(w_v, (1, 2, 0)).reshape(128, dim)
    wo_t = w_o.reshape(dim, dim)
    bf, f32 = jnp.bfloat16, jnp.float32
    n_blk = (n_rows - 2 * END) // QB + 2
    ff = w_gate.shape[1]
    rows = jax.ShapeDtypeStruct((n_rows, dim), bf)
    dma = pltpu.SemaphoreType.DMA
    return pl.pallas_call(
        layer_kernel,
        out_shape=[rows, rows, jax.ShapeDtypeStruct((2 * n_rows, dim), bf)],
        in_specs=[SM] + [ANY] * 4 + [VM] * 4 + [ANY] * 7,
        out_specs=[ANY] * 3,
        scratch_shapes=[
            *[pltpu.VMEM((n_rows, dim), bf)] * 5, pltpu.VMEM((QB, dim), f32), pltpu.VMEM((dim // 128, QB, 128), bf),
            pltpu.VMEM((2, n_rows, 128), bf), pltpu.VMEM((2, n_rows, 128), bf), pltpu.VMEM((QB, dim), bf),
            pltpu.VMEM((QB, ff), bf), pltpu.VMEM((2, QB, dim), bf)]
            + [pltpu.VMEM((QB, n_rows), f32)] * 3
            + [pltpu.VMEM((n_rows, 128), f32), pltpu.VMEM((n_rows, 128), f32), pltpu.VMEM((n_rows, 128), jnp.int32),
               pltpu.VMEM((dim, dim), bf), pltpu.VMEM((128, dim), bf), pltpu.VMEM((128, dim), bf), pltpu.VMEM((dim, dim), bf),
               pltpu.VMEM((dim, ff), bf), pltpu.VMEM((dim, ff), bf), pltpu.VMEM((ff, dim), bf), dma((7,))] + [dma((n_blk,))] * 15,
        compiler_params=pltpu.CompilerParams(collective_id=1, has_side_effects=True, vmem_limit_bytes=67000000),
        name="layer",
    )(span, *sends, positions.reshape(-1, 128), freq, g_attn, g_mlp, wq_t, wk_t, wv_t, wo_t, w_gate, w_up, w_down)


CHUNK = 128
MESH_ID = pl.DeviceIdType.MESH
ANY = pl.BlockSpec(memory_space=pl.ANY)
VM = pl.BlockSpec(memory_space=pltpu.VMEM)
SM = pl.BlockSpec(memory_space=pltpu.SMEM)


def meet(devices):
    barrier = pltpu.get_barrier_semaphore()
    for dev in devices:
        pl.semaphore_signal(barrier, inc=1, device_id={"sp": dev}, device_id_type=MESH_ID)
    pl.semaphore_wait(barrier, len(devices))


def push(src, dst, send_sem, recv_sem, dev):
    return pltpu.make_async_remote_copy(src_ref=src, dst_ref=dst, send_sem=send_sem, recv_sem=recv_sem,
                                        device_id={"sp": dev}, device_id_type=MESH_ID)


def share_kernel(n_split, *refs):
    n = (len(refs) - 2) // 2
    ins, outs, send_sems, recv_sems = refs[:n], refs[n:2 * n], refs[-2], refs[-1]
    me = lax.axis_index("sp")
    sib = me + 1 - 2 * lax.rem(me, 2)
    meet([sib])
    copies = []
    for a, b in zip(ins, outs):
        parts = n_split if a.ndim == 2 else 1
        step = a.shape[0] // parts
        for p in range(parts):
            rows = pl.ds(p * step, step)
            copies.append((a.at[rows], b.at[rows]) if parts > 1 else (a, b))
    started = []
    for i, (a, b) in enumerate(copies):
        cp = push(a, b, send_sems.at[i], recv_sems.at[i], sib)
        cp.start()
        started.append(cp)
    for cp in started:
        cp.wait()


def share(arrays, collective_id):
    return pl.pallas_call(
        functools.partial(share_kernel, 4),
        out_shape=[jax.ShapeDtypeStruct(a.shape, a.dtype) for a in arrays],
        in_specs=[ANY] * len(arrays), out_specs=[ANY] * len(arrays),
        scratch_shapes=[pltpu.SemaphoreType.DMA((16,)), pltpu.SemaphoreType.DMA((16,))],
        compiler_params=pltpu.CompilerParams(collective_id=collective_id, has_side_effects=True),
        name="share",
    )(*arrays)


LOAD = 512
FILL = 64
PITCH = 9


def load_table(parts, tab, stage, sems):
    jobs = []
    for ref, lo, hi in parts:
        for i in range(ref.shape[0] // LOAD):
            n = len(jobs)
            copy = pltpu.make_async_copy(ref.at[pl.ds(i * LOAD, LOAD)], stage.at[pl.ds(n * LOAD, LOAD)], sems.at[n])
            if lo is None:
                jobs.append((copy, None, 0, LOAD // FILL))
            else:
                low, high = jnp.maximum(lo - i * LOAD, 0), jnp.minimum(hi - i * LOAD, LOAD)
                jobs.append((copy, low < high, low // FILL, (high + FILL - 1) // FILL))
    for copy, cond, _, _ in jobs:
        if cond is None:
            copy.start()
        else:
            pl.when(cond)(copy.start)
    for n, (copy, cond, low, high) in enumerate(jobs):
        def fill(n=n, copy=copy, low=low, high=high):
            copy.wait()

            @pl.loop(low, high)
            def _blk(i):
                rows = pl.ds(pl.multiple_of(n * LOAD + i * FILL, FILL), FILL)
                first = (n * LOAD + i * FILL) * PITCH
                for j in range(stage.shape[1] // 128):
                    tab[pl.ds(first + j, FILL, stride=PITCH), :] = stage[rows, 128 * j:128 * (j + 1)].astype(jnp.float32)
        if cond is None:
            fill()
        else:
            pl.when(cond)(fill)


UNROLL = 16


def slab(k):
    return pl.ds(pl.multiple_of(k * 8, 8), 8)


def rows_out(lo, hi, src3, stage, base, dst, sem):
    first, last = lo // CHUNK, jnp.where(hi > lo, (hi + CHUNK - 1) // CHUNK, 0)

    def copy(i):
        rows = pl.multiple_of(i * CHUNK, CHUNK)
        return pltpu.make_async_copy(stage.at[pl.ds(base + rows, CHUNK)], dst.at[pl.ds(rows, CHUNK)], sem)

    @pl.loop(first, last)
    def _blk(i):
        rows = pl.ds(pl.multiple_of(base + i * CHUNK, CHUNK), CHUNK)
        for j in range(dst.shape[1] // 128):
            stage[rows, 128 * j:128 * (j + 1)] = src3[pl.ds(i * CHUNK * PITCH + j, CHUNK, stride=PITCH), :].astype(stage.dtype)
        copy(i).start()

    def finish():
        pl.loop(first, last)(lambda i: copy(i).wait())

    return finish


def slab(k):
    return pl.ds(k * PITCH, 8)


def move_run(n, one):
    whole = n // UNROLL

    @pl.loop(0, whole)
    def _grp(i):
        for k in range(UNROLL):
            one(i * UNROLL + k)

    @pl.loop(whole * UNROLL, n)
    def _one(i):
        one(i)


def pick_kernel(perm, so, sl, ro, rl, sl_b, ro_b, own, out_a, out_b, loc_a, loc_b, span, tab, out3, stage, sems, out_sems):
    cap = loc_a.shape[0]
    me = lax.axis_index("sp")
    core = lax.rem(me, 2)
    chip = me // 2
    mate = me + 1 - 2 * core
    far = 2 * (1 - chip)
    load_table([(own, None, None)], tab, stage, sems)
    n_in = rl[far] + rl[far + 1]
    span[0] = (1 - chip) * (cap - n_in)
    span[1] = (1 - chip) * (cap - n_in) + n_in

    def far_row(goal):
        return chip * (cap - sl[goal] - sl_b[goal]) + core * sl_b[goal]

    span[2] = far_row(far + core)
    span[3] = far_row(far + core) + sl[far + core]
    span[4] = ro[me]
    span[5] = ro[me] + sl[me]
    ends = []
    for n, (goal, row, dst) in enumerate([(far + 1 - core, far_row(far + 1 - core), out_b), (far + core, far_row(far + core), out_a),
                                          (mate, ro_b[me], loc_b), (me, ro[me], loc_a)]):
        def one(t, goal=goal, row=row):
            out3[slab(row + t), :] = tab[slab(perm[so[goal] + t]), :]
        move_run(sl[goal], one)
        ends.append(rows_out(row, row + sl[goal], out3, stage, n * cap, dst, out_sems.at[n]))
    for end in ends:
        end()


def back_place_kernel(perm, so, sl, ro, rl, sl_b, ro_b, own, sib, stream, out, tab, out3, stage, sems, out_sems):
    cap = own.shape[0]
    n_tok = out.shape[0]
    me = lax.axis_index("sp")
    core = lax.rem(me, 2)
    chip = me // 2
    mate = me + 1 - 2 * core
    far = 2 * (1 - chip)

    def far_row(goal):
        return chip * (cap - sl[goal] - sl_b[goal]) + core * sl_b[goal]

    runs = [(me, own, ro[me]), (mate, sib, ro_b[me]),
            (far + core, stream.at[pl.ds(0, cap)], far_row(far + core)), (far + 1 - core, stream.at[pl.ds(cap, cap)], far_row(far + 1 - core))]
    load_table([(ref, row, row + sl[goal]) for goal, ref, row in runs], tab, stage, sems)
    for n, (goal, _, row) in enumerate(runs):
        def one(t, goal=goal, row=n * cap + row):
            out3[slab(perm[so[goal] + t]), :] = tab[slab(row + t), :]
        move_run(sl[goal], one)
    sent = so[3] + sl[3]

    def blank(t):
        out3[slab(perm[sent + t]), :] = jnp.zeros((8, 128), jnp.float32)

    move_run(n_tok - sent, blank)
    rows_out(0, n_tok, out3, stage, 0, out, out_sems.at[0])()


def local_call(body, out_shapes, out_specs, n_any, tab_rows, out_rows, stage_rows, dim, name):
    return pl.pallas_call(
        body,
        out_shape=out_shapes,
        in_specs=[SM] * 7 + [ANY] * n_any,
        out_specs=out_specs,
        scratch_shapes=[pltpu.VMEM((tab_rows * PITCH, 128), jnp.float32), pltpu.VMEM((out_rows * PITCH, 128), jnp.float32),
                        pltpu.VMEM((stage_rows, dim), jnp.bfloat16), pltpu.SemaphoreType.DMA((tab_rows // LOAD,)), pltpu.SemaphoreType.DMA((4,))],
        compiler_params=pltpu.CompilerParams(vmem_limit_bytes=66000000),
        name=name,
    )


def solution(mesh):
    row_spec = P(('dp', 'sp'), None)
    vec_spec = P(('dp', 'sp'))
    rep_spec = P()

    def per_device(hidden, tok_perm, send_off, send_len, recv_off, recv_len, recv_doc, recv_pos, g_attn, w_q, w_k, w_v, w_o, g_mlp, w_gate, w_up, w_down):
        n_tok, dim = hidden.shape
        cap = recv_doc.shape[0]
        plan = [tok_perm, send_off, send_len, recv_off, recv_len]
        plan += share([send_len, recv_off], 0)
        rows_bf = jax.ShapeDtypeStruct((cap, dim), hidden.dtype)
        outs = [rows_bf] * 4 + [jax.ShapeDtypeStruct((6,), jnp.int32)]
        out_a, out_b, loc_a, loc_b, span = local_call(pick_kernel, outs, [ANY] * 4 + [SM], 1, n_tok, cap, 4 * cap, dim, "pick")(*plan, hidden)
        done, sib_done, returned = layer(span, (out_a, out_b, loc_a, loc_b), recv_pos, g_attn, w_q, w_k, w_v, w_o, g_mlp, w_gate, w_up, w_down)
        out = jax.ShapeDtypeStruct((n_tok, dim), hidden.dtype)
        return local_call(back_place_kernel, out, ANY, 3, 4 * cap, n_tok, 4 * cap, dim, "back_place")(*plan, done, sib_done, returned)

    return jax.shard_map(per_device, mesh=mesh, in_specs=(row_spec,) + (vec_spec,) * 7 + (rep_spec,) * 9, out_specs=row_spec, check_vma=False)
```
